32 devices in a mesh: tm: 32 (over z, y, x, core).
Axes of the slice: x: 2, y: 2, z: 4, core: 2. Of those that a mesh axis runs over, the one named last changes fastest.
Arguments:
- field: bfloat16 [10752, 2048], P('tm'), may hold values from -52 to 52
- index: float32 [10752, 10], P('tm'), may hold values from -13 to 13
- lag_list: int32 [61], replicated, may hold values from -30 to 30, as said below
- index_offset: int32 [10], replicated, may hold values from 0 to 14, as said below
- sea_mask: int32 [2048], P('tm'), may hold values 0 or 1
Outputs:
- corr_maps: float32 [2048, 10, 61], P('tm')
The draws below stay inside these ranges and needn't reach their ends.
Inputs may be any that keep to these rules, and one draw needn't show every extreme that they name: `lag_list`: each whole number of -30 to 30 appears once. `index_offset`: some index has the extra lead 14.
All inputs are finite; a program needn't handle non-finite values. No bound on the sum of `sea_mask` on one device may be relied on, other than what follows from the above.
Results may differ from the reference program's by a relative error of at most 0.00051.
Values may be sent and summed in bfloat16 or wider, within the bound.
A program may use at most 256 MiB of HBM per device.

```python
import jax
import jax.numpy as jnp
from jax import lax

T_DEV = 336
INDEX_COUNT = 10
MAXLAG = 30
MAXOFF = 14
LAGS = 61
TDAYS = 10752
CELLS = 2048
N_TM = 32


def index_base(key):
    keys = jax.random.split(jax.random.fold_in(key, 11), 2)
    times = jnp.arange(TDAYS, dtype=jnp.float32)[:, None]
    envelope = 1.0 + 2.0 * times / (TDAYS - 1.0)
    noise = jax.random.truncated_normal(keys[0], -4.0, 4.0, (TDAYS, INDEX_COUNT), jnp.float32)
    offset_means = jax.random.uniform(keys[1], (INDEX_COUNT,), jnp.float32, -0.5, 0.5)
    return envelope * noise + offset_means[None, :]


def draw_index(key, part):
    return index_base(key)


def draw_field(key, part):
    series = index_base(key)
    keys = jax.random.split(jax.random.fold_in(key, 23), 6)
    linked = jax.random.randint(keys[0], (CELLS,), 0, INDEX_COUNT)
    delays = jax.random.randint(keys[1], (CELLS,), -MAXLAG, MAXLAG + MAXOFF + 1)
    weights = jax.random.uniform(keys[2], (CELLS,), jnp.float32, 0.3, 1.0) * jnp.where(jax.random.randint(keys[3], (CELLS,), 0, 2) == 0, -1.0, 1.0)
    scales = jnp.exp(jax.random.uniform(keys[4], (CELLS,), jnp.float32, jnp.log(0.3), jnp.log(3.0)))
    times = jnp.arange(TDAYS, dtype=jnp.int32)[:, None]
    source = jnp.clip(times - delays[None, :], 0, TDAYS - 1)
    signal = series[source, linked[None, :]]
    noise = jax.random.truncated_normal(keys[5], -4.0, 4.0, (TDAYS, CELLS), jnp.float32)
    cell_means = 0.5 * weights
    return (scales[None, :] * (weights[None, :] * signal + noise + cell_means[None, :])).astype(jnp.bfloat16)


def draw_lag_list(key, part):
    order = jax.random.permutation(jax.random.fold_in(key, 31), LAGS)
    return (order - MAXLAG).astype(jnp.int32)


def draw_index_offset(key, part):
    keys = jax.random.split(jax.random.fold_in(key, 37), 2)
    series_values = jax.random.randint(keys[0], (INDEX_COUNT,), 0, MAXOFF + 1)
    chosen = jax.random.randint(keys[1], (), 0, INDEX_COUNT)
    return series_values.at[chosen].set(MAXOFF).astype(jnp.int32)


def place_ends(drawn, stream_key, smallest, high):
    dims = drawn.shape
    index_at = [jax.random.randint(jax.random.fold_in(stream_key, axis), (), 0, dims[axis]) for axis in range(len(dims))]
    drawn = drawn.at[tuple(index_at)].set(smallest)
    longest = dims.index(max(dims))
    index_at[longest] = (index_at[longest] + 1) % dims[longest]
    return drawn.at[tuple(index_at)].set(high)


def setup_inputs(seed: int = 0) -> dict:
    streams_of = jax.random.split(jax.random.key(seed), 6)
    field = draw_field(jax.random.fold_in(streams_of[5], 71), 0)
    index = draw_index(jax.random.fold_in(streams_of[5], 71), 0)
    lag_list = draw_lag_list(jax.random.fold_in(streams_of[5], 71), 0)
    index_offset = draw_index_offset(jax.random.fold_in(streams_of[5], 71), 0)
    sea_mask = place_ends((jax.random.randint(streams_of[4], (CELLS,), 0, 10) < 7).astype(jnp.int32), jax.random.fold_in(streams_of[4], 1), 0, 1)
    return dict(field=field, index=index, lag_list=lag_list, index_offset=index_offset, sea_mask=sea_mask)


def build_window_sums(padded, begin, length, reach, lag_low):
    count = reach + lag_low + 1
    piece = lax.dynamic_slice_in_dim(padded, begin, length + reach + lag_low, 0)
    windows = jnp.stack([piece[reach + lag_low - j:reach + lag_low - j + length] for j in range(count)], 1)
    return windows.reshape(length, count * padded.shape[1])

def lag_selector(shifts, reach, lag_low):
    count = reach + lag_low + 1
    places = jnp.arange(count, dtype=jnp.int32)
    return (places[None, :, None] == (shifts + lag_low)[:, None, :]).astype(jnp.float32)

def pick_lags(accum, selector):
    kcount, count, lcount = selector.shape
    spread = accum.reshape(accum.shape[0], count, kcount)
    chosen = jnp.einsum('cjk,kjl->ckl', spread, selector, precision=lax.Precision.HIGHEST)
    return chosen.reshape(accum.shape[0], kcount * lcount)

def reference(field, index, lag_list, index_offset, sea_mask):
    reach = MAXLAG + MAXOFF
    count = reach + MAXLAG + 1
    total_days = TDAYS * 1.0
    mean_i = lax.optimization_barrier(jnp.sum(index, 0)) / total_days
    var_i = lax.optimization_barrier(jnp.sum(index * index, 0)) / total_days - mean_i * mean_i
    centered = (index - mean_i).astype(jnp.bfloat16)
    shifts = (lag_list[None, :] + index_offset[:, None]).astype(jnp.int32)
    padded = jnp.pad(centered, ((reach, reach), (0, 0)))
    running_total = jnp.concatenate([jnp.zeros((1, INDEX_COUNT), jnp.float32), jnp.cumsum(padded.astype(jnp.float32), 0)], 0)
    upper_bound = (TDAYS - shifts + reach).astype(jnp.int32)
    lower_bound = (reach - shifts).astype(jnp.int32)
    series_number = jnp.arange(INDEX_COUNT, dtype=jnp.int32)[:, None]
    prefix_totals = running_total[upper_bound, series_number] - running_total[lower_bound, series_number]
    selector = lag_selector(shifts, reach, MAXLAG)
    block_rows = 8 * T_DEV
    turns = N_TM // 8

    def one_block(carry, turn):
        accum, first_sum, second_sum = carry
        begin = (turn * block_rows).astype(jnp.int32)
        rows = lax.dynamic_slice_in_dim(field, begin, block_rows, 0)
        windows = build_window_sums(padded, begin, block_rows, reach, MAXLAG)
        accum = accum + lax.dot_general(rows, windows, (((0,), (0,)), ((), ())), preferred_element_type=jnp.float32)
        wide = rows.astype(jnp.float32)
        return ((accum, first_sum + lax.optimization_barrier(jnp.sum(wide, 0)), second_sum + lax.optimization_barrier(jnp.sum(wide * wide, 0))), None)
    start_carry = (jnp.zeros((CELLS, count * INDEX_COUNT), jnp.float32), jnp.zeros((CELLS,), jnp.float32), jnp.zeros((CELLS,), jnp.float32))
    (accum, first_sum, second_sum), unused = lax.scan(one_block, start_carry, jnp.arange(turns, dtype=jnp.int32))
    products = pick_lags(accum, selector)
    mean_x = first_sum / total_days
    var_x = second_sum / total_days - mean_x * mean_x
    numer = products.reshape(CELLS, INDEX_COUNT, LAGS) - mean_x[:, None, None] * prefix_totals[None]
    scale = total_days * jnp.sqrt(var_x + 1e-06)[:, None, None] * jnp.sqrt(var_i + 1e-06)[None, :, None]
    return numer / scale * sea_mask.astype(jnp.float32)[:, None, None]
```

```python
import functools

import jax
import jax.numpy as jnp
from jax import lax
from jax.experimental import pallas as pl
from jax.experimental.pallas import tpu as pltpu
from jax.sharding import PartitionSpec as P

MAXLAG = 30
MAXOFF = 14
REACH = 64
ROWS = 64
EXTRA = 8
TOP = 32767.0
GROUPS = 4
MESH = pl.DeviceIdType.MESH


def round_up(value, unit):
    return -(-value // unit) * unit


def kernel(
    sizes,
    field_hbm,
    index_ref,
    lag_ref,
    offset_ref,
    mask_ref,
    out_ref,
    field_ref,
    idx_ref,
    idx_all,
    zmsg,
    zin,
    recv,
    win,
    acc,
    other,
    partner_in,
    sent,
    sent_extra,
    got,
    got_extra,
    small,
    tot_ref,
    raw_send,
    raw_recv,
    idx_send,
    idx_recv,
    relay_sem,
    z_send,
    z_recv,
    swap_send,
    swap_recv,
    sum_send,
    sum_recv,
    own_sem,
    round_sem,
):
    devices, t_dev, kcount, groups, g = sizes
    lanes = idx_ref.shape[1]
    wide = lanes + 128
    half_k = kcount // 2
    count = half_k * ROWS
    cells = 128
    me = lax.axis_index("tm")
    core = lax.rem(me, 2)
    chip = lax.div(me, 2)
    h = lax.div(chip, g)
    m = lax.rem(chip, g)
    partner = chip * 2 + (1 - core)
    f32 = jnp.float32
    total_days = devices * t_dev * 1.0

    def across(step):
        other_m, bit = 0, 1
        while bit < g:
            flip = lax.rem(lax.div(m, bit) + lax.div(step, bit), 2)
            other_m, bit = other_m + flip * bit, bit * 2
        return other_m

    def device_of(group, member):
        return (group * g + member) * 2 + core

    def remote(src, dst, send, recv_s, device):
        return pltpu.make_async_remote_copy(
            src_ref=src,
            dst_ref=dst,
            send_sem=send,
            recv_sem=recv_s,
            device_id=(device,),
            device_id_type=MESH,
        )

    def block(at):
        return field_ref.at[:, pl.ds(pl.multiple_of(at * cells, cells), cells)]

    def plane_of(piece):
        return lax.rem(h + 1 + piece, groups)

    def raw_copy(piece, step):
        to = across(step)
        return remote(
            block(plane_of(piece) * g + to),
            recv.at[piece, step],
            raw_send.at[piece, step],
            raw_recv.at[piece, step],
            device_of(h, to),
        )

    def own_copy(piece):
        return pltpu.make_async_copy(
            block(plane_of(piece) * g + m), recv.at[piece, 0], own_sem.at[piece]
        )

    def idx_copy(step):
        return remote(
            idx_ref,
            idx_all.at[core * g + m],
            idx_send.at[step],
            idx_recv.at[step],
            device_of(h, across(step)),
        )

    def relay_copy():
        part = idx_all.at[pl.ds(core * g, g)]
        return remote(part, part, relay_sem.at[0], relay_sem.at[1], partner)

    def z_copy(step):
        return remote(
            zmsg,
            zin.at[step],
            z_send.at[step],
            z_recv.at[step],
            device_of(lax.rem(h + step, groups), m),
        )

    def swap_copy(piece):
        return remote(
            other.at[piece],
            partner_in.at[piece],
            swap_send.at[piece],
            swap_recv.at[piece],
            partner,
        )

    def sum_copy(piece):
        return remote(
            sent.at[piece],
            got.at[piece],
            sum_send.at[0, piece],
            sum_recv.at[0, piece],
            device_of(plane_of(piece), m),
        )

    def extra_copy(piece):
        return remote(
            sent_extra.at[piece],
            got_extra.at[piece],
            sum_send.at[1, piece],
            sum_recv.at[1, piece],
            device_of(plane_of(piece), m),
        )

    def each(low_step, high_step, act):
        def body(step, carry):
            act(step)
            return carry

        lax.fori_loop(low_step, high_step, body, 0)

    load = pltpu.make_async_copy(field_hbm, field_ref, own_sem.at[groups])
    load.start()
    barrier = pltpu.get_barrier_semaphore()

    def tell(sem, device):
        pl.semaphore_signal(sem, inc=1, device_id=(device,), device_id_type=MESH)

    def tell_line(sem):
        @pl.when(h > 0)
        def _():
            tell(sem, device_of(h - 1, m))

        @pl.when(h < groups - 1)
        def _():
            tell(sem, device_of(h + 1, m))

    beside = jnp.where(h > 0, 1, 0) + jnp.where(h < groups - 1, 1, 0)

    tell(barrier, partner)
    tell_line(barrier)
    each(1, g, lambda s: tell(barrier, device_of(h, across(s))))
    idx_ref[...] = jnp.zeros_like(idx_ref)
    idx_ref[0:kcount, 0:t_dev] = index_ref[...]
    small[...] = jnp.zeros_like(small)
    small[0:1, 0 : cells // 2] = mask_ref[...].astype(f32)
    zmsg[...] = jnp.zeros_like(zmsg)
    pl.semaphore_wait(barrier, g + beside)

    each(1, g, lambda s: idx_copy(s).start())
    load.wait()
    for piece in range(groups):
        own_copy(piece).start()
        each(1, g, lambda s, piece=piece: raw_copy(piece, s).start())
    for turn in range(groups - 2):
        tell_line(round_sem.at[turn])
        pl.semaphore_wait(round_sem.at[turn], beside)
    idx_all[core * g + m] = idx_ref[...]
    each(1, g, lambda s: idx_copy(s).wait())
    relay_copy().start()
    relay_copy().wait()

    def sum_body(at, carry):
        first, second = carry
        value = idx_all[at]
        return first + value, second + value * value

    zero = jnp.zeros((kcount, lanes), f32)
    first, second = lax.fori_loop(0, 2 * g, sum_body, (zero, zero))
    first = jnp.sum(first, 1, keepdims=True)
    second = jnp.sum(second, 1, keepdims=True)
    lane = lax.broadcasted_iota(jnp.int32, (kcount, 128), 1)
    zmsg[0:kcount, :] = jnp.where(lane < 64, first, second)
    ending = pltpu.roll(idx_all[2 * g - 1], (64 - (t_dev - 64)) % lanes, 1)
    zmsg[16 : 16 + kcount, :] = jnp.where(lane < 64, idx_all[0][:, :128], ending[:, :128])
    each(1, groups, lambda s: z_copy(s).start())
    each(1, groups, lambda s: z_copy(s).wait())
    for s in range(1, groups):
        stats = zin[s, 0:kcount, :]
        first = first + stats[:, 0:1]
        second = second + stats[:, 64:65]
    mean = first / total_days
    var = second / total_days - mean * mean
    outer = 1.0 / jnp.sqrt(var + 1e-06)

    place = lax.broadcasted_iota(jnp.int32, (kcount, lanes), 1)

    def centered(value, valid):
        value = (value - mean).astype(jnp.bfloat16).astype(f32)
        return jnp.where(valid, value, 0.0)

    def center_body(at, carry):
        value = centered(idx_all[at], place < t_dev)
        idx_all[at] = value
        return carry + value

    group_sum = jnp.sum(lax.fori_loop(0, 2 * g, center_body, zero), 1, keepdims=True)
    tail = jnp.zeros((kcount, lanes - 128), f32)

    def edge(slot):
        return jnp.concatenate([zin[slot, 16 : 16 + kcount, :], tail], 1)

    before_at, after_at = 2 * g, 2 * g + 1
    ahead = pltpu.roll(edge(1), t_dev - 128, 1)
    idx_all[before_at] = centered(
        ahead, (place >= t_dev - 64) & (place < t_dev) & (h > 0)
    )
    idx_all[after_at] = centered(edge(groups - 1), (place < 64) & (h < groups - 1))

    def slot_at(order):
        inside = lax.rem(order, 2) * g + lax.div(order, 2)
        inside = jnp.where(order < 0, before_at, inside)
        return jnp.where(order >= 2 * g, after_at, inside)

    spot = lax.broadcasted_iota(jnp.int32, (kcount, wide), 1)
    wing = jnp.zeros((kcount, 128), f32)

    def window_body(step, carry):
        order = across(step) * 2 + core
        here = jnp.concatenate([idx_all[slot_at(order)], wing], 1)
        before = jnp.concatenate([idx_all[slot_at(order - 1)], wing], 1)
        after = jnp.concatenate([idx_all[slot_at(order + 1)], wing], 1)
        left = pltpu.roll(before, (REACH - t_dev) % wide, 1)
        mid = pltpu.roll(here, REACH, 1)
        right = pltpu.roll(after, REACH + t_dev, 1)
        ext = jnp.where(spot < REACH, left, jnp.where(spot < REACH + t_dev, mid, right))
        for k in range(kcount):
            line = pltpu.roll(ext[k : k + 1], wide - REACH - MAXLAG + offset_ref[k], 1)
            line = jnp.broadcast_to(line, (ROWS, wide))
            turned = pltpu.roll(line, 0, 1, stride=1, stride_axis=0)
            win[step, k * ROWS : (k + 1) * ROWS, :] = turned[:, :lanes].astype(jnp.bfloat16)
        return carry

    lax.fori_loop(0, g, window_body, 0)

    day = lax.broadcasted_iota(jnp.int32, (lanes, 128), 0)
    shift = lax.broadcasted_iota(jnp.int32, (lanes, 128), 1) - MAXLAG
    late = jnp.where((day >= t_dev - shift) & (day < t_dev), 1.0, 0.0).astype(jnp.bfloat16)
    early = jnp.where(day < -shift, 1.0, 0.0).astype(jnp.bfloat16)

    def part(at, sel):
        return jnp.dot(idx_all[at].astype(jnp.bfloat16), sel, preferred_element_type=f32)

    by_shift = group_sum + (part(before_at, late) - part(2 * g - 1, late)) + (
        part(after_at, early) - part(0, early)
    )
    tot_ref[...] = jnp.zeros_like(tot_ref)
    for k in range(kcount):
        tot_ref[k : k + 1, :] = pltpu.roll(
            by_shift[k : k + 1], lax.rem(128 - offset_ref[k], 128), 1
        )
    own_tot = tot_ref[...]
    own_cols = jnp.transpose(own_tot)

    low = lax.broadcasted_iota(jnp.int32, (ROWS, 128), 1) < 64
    low_row = lax.broadcasted_iota(jnp.int32, (1, 128), 1) < 64

    def pair_cols(cols, k):
        return jnp.where(low, cols[0:ROWS, k : k + 1], cols[0:ROWS, k + half_k : k + half_k + 1])

    def halves(first_half, second_half, is_low):
        turned_first = pltpu.roll(first_half, 64, 1)
        turned_second = pltpu.roll(second_half, 64, 1)
        zeroth = jnp.where(is_low, first_half, turned_second)
        oneth = jnp.where(is_low, turned_first, second_half)
        mine = jnp.where(core == 0, zeroth, oneth)
        theirs = jnp.where(core == 0, oneth, zeroth)
        return mine, theirs

    group_days = 2 * g * t_dev * 1.0
    mine_at = acc.shape[0] - EXTRA

    def products(piece):
        own_copy(piece).wait()

        def add(step, first_time):
            value = recv[piece, step]
            wide_value = value.astype(f32)
            sums = jnp.sum(wide_value, 0, keepdims=True)
            squares = jnp.sum(wide_value * wide_value, 0, keepdims=True)
            found = jnp.dot(win[step, :, :t_dev], value, preferred_element_type=f32)
            if first_time:
                acc[0 : 2 * count, :] = found
                acc[mine_at : mine_at + 1, :] = sums
                acc[mine_at + 1 : mine_at + 2, :] = squares
            else:
                acc[0 : 2 * count, :] += found
                acc[mine_at : mine_at + 1, :] += sums
                acc[mine_at + 1 : mine_at + 2, :] += squares

        add(0, True)

        def body(step, carry):
            raw_copy(piece, step).wait()
            add(step, False)
            return carry

        lax.fori_loop(1, g, body, 0)
        for k in range(half_k):
            at = k * ROWS
            mine, theirs = halves(
                acc[at : at + ROWS, :], acc[count + at : count + at + ROWS, :], low
            )
            acc[at : at + ROWS, :] = mine
            other[piece, at : at + ROWS, :] = theirs
        for row in range(2):
            value = acc[mine_at + row : mine_at + row + 1, :]
            mine, theirs = halves(value, value, low_row)
            acc[mine_at + row : mine_at + row + 1, :] = mine
            other[piece, count + row : count + row + 1, :] = theirs
        swap_copy(piece).start()
        swap_copy(piece).wait()

    def joined(piece, k):
        at = k * ROWS
        return acc[at : at + ROWS, :] + partner_in[piece, at : at + ROWS, :]

    def joined_row(piece, row):
        return (
            acc[mine_at + row : mine_at + row + 1, :]
            + partner_in[piece, count + row : count + row + 1, :]
        )

    other[...] = jnp.zeros_like(other)
    sent_extra[...] = jnp.zeros_like(sent_extra)
    for piece in range(groups - 1):
        products(piece)
        sx = joined_row(piece, 0)
        sent_extra[piece, 0:1, :] = sx
        sent_extra[piece, 1:2, :] = joined_row(piece, 1)
        local_mean = sx / group_days
        for k in range(half_k):
            value = joined(piece, k) - local_mean * pair_cols(own_cols, k)
            top = jnp.max(jnp.abs(value), 0, keepdims=True)
            sent_extra[piece, 2 + k : 3 + k, :] = top
            scaled = value * (TOP / jnp.maximum(top, 1e-30))
            sent[piece, k * ROWS : (k + 1) * ROWS, :] = (
                jnp.round(scaled).astype(jnp.int32).astype(jnp.int16)
            )
        sent_extra[piece, EXTRA:, :] = own_tot
        sum_copy(piece).start()
        extra_copy(piece).start()

    last = groups - 1
    products(last)
    sx = joined_row(last, 0)
    sq = joined_row(last, 1)
    for piece in range(groups - 1):
        extra_copy(piece).wait()
        sum_copy(piece).wait()
        sx = sx + got_extra[piece, 0:1, :]
        sq = sq + got_extra[piece, 1:2, :]
    mean_x = sx / total_days
    var_x = sq / total_days - mean_x * mean_x
    mask = small[0:1, :]
    mask = mask + pltpu.roll(mask, 64, 1)
    inner = mask / (total_days * jnp.sqrt(var_x + 1e-06))
    far_cols = [
        jnp.transpose(got_extra[piece, EXTRA : EXTRA + 16, :]) for piece in range(groups - 1)
    ]
    far_mean = [
        got_extra[piece, 0:1, :] / group_days - mean_x for piece in range(groups - 1)
    ]
    small_int = lag_ref[...] + MAXLAG

    def normal(k):
        value = joined(last, k) - mean_x * pair_cols(own_cols, k)
        for piece in range(groups - 1):
            coded = got[piece, k * ROWS : (k + 1) * ROWS, :].astype(jnp.int32).astype(f32)
            value = value + coded * (got_extra[piece, 2 + k : 3 + k, :] * (1.0 / TOP))
            value = value + far_mean[piece] * pair_cols(far_cols[piece], k)
        scale = jnp.where(low_row, outer[k : k + 1], outer[k + half_k : k + half_k + 1])
        return value * (inner * scale)

    small[0:1, 0 : lag_ref.shape[1]] = small_int.astype(f32)
    chosen = jnp.broadcast_to(small[0:1, :].astype(jnp.int32), (64, 128))
    kept = lag_ref.shape[1]
    for k in range(0, half_k, 2):
        upper = normal(k)
        under = normal(k + 1) if k + 1 < half_k else upper
        flat = jnp.transpose(jnp.concatenate([upper, under], 0))
        for side in range(2):
            rows = flat[side * 64 : (side + 1) * 64, :]
            out_ref[k + side * half_k] = jnp.take_along_axis(rows, chosen, axis=1)[:, :kept]
            if k + 1 < half_k:
                out_ref[k + 1 + side * half_k] = jnp.take_along_axis(
                    rows, chosen + 64, axis=1
                )[:, :kept]


def shards(field, index, lag_list, index_offset, sea_mask):
    t_dev, cells_all = field.shape
    devices = lax.axis_size("tm")
    kcount = index.shape[1]
    lanes = round_up(t_dev, 128)
    groups = GROUPS
    g = devices // 2 // groups
    rows = kcount * ROWS
    half = rows // 2
    sizes = (devices, t_dev, kcount, groups, g)
    dma = pltpu.SemaphoreType.DMA
    f32 = jnp.float32
    vmem = pl.BlockSpec(memory_space=pltpu.VMEM)
    maps = pl.pallas_call(
        functools.partial(kernel, sizes),
        out_shape=jax.ShapeDtypeStruct((kcount, 64, lag_list.shape[0]), f32),
        in_specs=[
            pl.BlockSpec(memory_space=pl.ANY),
            vmem,
            vmem,
            pl.BlockSpec(memory_space=pltpu.SMEM),
            vmem,
        ],
        out_specs=vmem,
        scratch_shapes=[
            pltpu.VMEM((t_dev, cells_all), jnp.bfloat16),
            pltpu.VMEM((kcount, lanes), f32),
            pltpu.VMEM((2 * g + 2, kcount, lanes), f32),
            pltpu.VMEM((32, 128), f32),
            pltpu.VMEM((groups, 32, 128), f32),
            pltpu.VMEM((groups, g, t_dev, 128), jnp.bfloat16),
            pltpu.VMEM((g, rows, lanes), jnp.bfloat16),
            pltpu.VMEM((rows + EXTRA, 128), f32),
            pltpu.VMEM((groups, half + EXTRA, 128), f32),
            pltpu.VMEM((groups, half + EXTRA, 128), f32),
            pltpu.VMEM((groups, half, 128), jnp.int16),
            pltpu.VMEM((groups, EXTRA + 16, 128), f32),
            pltpu.VMEM((groups, half, 128), jnp.int16),
            pltpu.VMEM((groups, EXTRA + 16, 128), f32),
            pltpu.VMEM((8, 128), f32),
            pltpu.VMEM((16, 128), f32),
            dma((groups, g)),
            dma((groups, g)),
            dma((g,)),
            dma((g,)),
            dma((2,)),
            dma((groups,)),
            dma((groups,)),
            dma((groups,)),
            dma((groups,)),
            dma((2, groups)),
            dma((2, groups)),
            dma((groups + 1,)),
            pltpu.SemaphoreType.REGULAR((groups,)),
        ],
        compiler_params=pltpu.CompilerParams(
            collective_id=0, has_side_effects=True, vmem_limit_bytes=60 * 1024 * 1024
        ),
    )(field, index.T, lag_list[None, :], index_offset, sea_mask[None, :])
    return jnp.transpose(maps, (1, 0, 2))


def solution(mesh):
    return jax.shard_map(
        shards,
        mesh=mesh,
        in_specs=(P("tm", None), P("tm", None), P(), P(), P("tm")),
        out_specs=P("tm", None, None),
        check_vma=False,
    )
```

```python
import functools

import jax
import jax.numpy as jnp
from jax import lax
from jax.experimental import pallas as pl
from jax.experimental.pallas import tpu as pltpu
from jax.sharding import PartitionSpec as P

MAXLAG = 30
MAXOFF = 14
REACH = 64
ROWS = 64
EXTRA = 8
TOP = 32767.0
FAR = 1e30
NEAR = 1e29
GROUPS = 4
MESH = pl.DeviceIdType.MESH


def round_up(value, unit):
    return -(-value // unit) * unit


def kernel(
    sizes,
    field_hbm,
    index_ref,
    lag_ref,
    offset_ref,
    mask_ref,
    out_ref,
    field_ref,
    idx_ref,
    idx_all,
    tiles,
    zmsg,
    zin,
    recv,
    raw_win,
    win,
    acc,
    other,
    partner_in,
    sent,
    sent_extra,
    got,
    got_extra,
    far,
    small,
    tot_part,
    tot_in,
    raw_send,
    raw_recv,
    idx_send,
    idx_recv,
    tile_send,
    tile_recv,
    lone_sem,
    z_send,
    z_recv,
    swap_send,
    swap_recv,
    sum_send,
    sum_recv,
    own_sem,
    round_sem,
):
    devices, t_dev, kcount, groups, g = sizes
    lanes = idx_ref.shape[1]
    wide = lanes + 128
    half_k = kcount // 2
    count = half_k * ROWS
    cells = 128
    me = lax.axis_index("tm")
    core = lax.rem(me, 2)
    chip = lax.div(me, 2)
    h = lax.div(chip, g)
    m = lax.rem(chip, g)
    partner = chip * 2 + (1 - core)
    edge_peer = ((h + 2 * core - 1) * g + m) * 2 + (1 - core)
    has_edge = jnp.where(core == 0, h > 0, h < groups - 1)
    f32 = jnp.float32
    total_days = devices * t_dev * 1.0

    def flipped(value, step, size):
        found, bit = 0, 1
        while bit < size:
            flip = lax.rem(lax.div(value, bit) + lax.div(step, bit), 2)
            found, bit = found + flip * bit, bit * 2
        return found

    def across(step):
        return flipped(m, step, g)

    def device_of(group, member):
        return (group * g + member) * 2 + core

    def remote(src, dst, send, recv_s, device):
        return pltpu.make_async_remote_copy(
            src_ref=src,
            dst_ref=dst,
            send_sem=send,
            recv_sem=recv_s,
            device_id=(device,),
            device_id_type=MESH,
        )

    def block(at):
        return field_ref.at[:, pl.ds(pl.multiple_of(at * cells, cells), cells)]

    def plane_of(piece):
        return flipped(h, groups - 1 - piece, groups)

    def raw_copy(piece, step):
        to = across(step)
        return remote(
            block(plane_of(piece) * g + to),
            recv.at[piece, step],
            raw_send.at[piece, step],
            raw_recv.at[piece, step],
            device_of(h, to),
        )

    def own_copy(piece):
        return pltpu.make_async_copy(
            block(plane_of(piece) * g + m), recv.at[piece, 0], own_sem.at[piece]
        )

    def idx_copy(step):
        return remote(
            idx_ref,
            idx_all.at[m],
            idx_send.at[step],
            idx_recv.at[step],
            device_of(h, across(step)),
        )

    def tile_copy(side, step):
        to = (h * g + across(step)) * 2 + (core if side == 0 else 1 - core)
        mine = tiles.at[core * g + m]
        return remote(
            mine, mine, tile_send.at[side, step], tile_recv.at[side, step], to
        )

    def edge_copy():
        return remote(
            tiles.at[jnp.where(core == 0, 0, 2 * g - 1)],
            tiles.at[2 * g],
            lone_sem.at[0],
            lone_sem.at[1],
            edge_peer,
        )

    def total_copy():
        return remote(tot_part, tot_in, lone_sem.at[2], lone_sem.at[3], partner)

    def z_copy(step):
        return remote(
            zmsg,
            zin.at[step],
            z_send.at[step],
            z_recv.at[step],
            device_of(flipped(h, step, groups), m),
        )

    def swap_copy(piece):
        return remote(
            other.at[piece],
            partner_in.at[piece],
            swap_send.at[piece],
            swap_recv.at[piece],
            partner,
        )

    def sum_copy(piece):
        return remote(
            sent.at[piece],
            got.at[piece],
            sum_send.at[0, piece],
            sum_recv.at[0, piece],
            device_of(plane_of(piece), m),
        )

    def extra_copy(piece):
        return remote(
            sent_extra.at[piece],
            got_extra.at[piece],
            sum_send.at[1, piece],
            sum_recv.at[1, piece],
            device_of(plane_of(piece), m),
        )

    def each(low_step, high_step, act):
        def body(step, carry):
            act(step)
            return carry

        lax.fori_loop(low_step, high_step, body, 0)

    load = pltpu.make_async_copy(field_hbm, field_ref, own_sem.at[groups])
    load.start()
    barrier = pltpu.get_barrier_semaphore()

    def tell(sem, device):
        pl.semaphore_signal(sem, inc=1, device_id=(device,), device_id_type=MESH)

    def tell_line(sem):
        @pl.when(h > 0)
        def _():
            tell(sem, device_of(h - 1, m))

        @pl.when(h < groups - 1)
        def _():
            tell(sem, device_of(h + 1, m))

    beside = jnp.where(h > 0, 1, 0) + jnp.where(h < groups - 1, 1, 0)
    tell_line(barrier)

    @pl.when(has_edge)
    def _():
        tell(barrier, edge_peer)

    each(1, 2 * g, lambda s: tell(barrier, (h * g + across(lax.div(s, 2))) * 2 + lax.rem(core + s, 2)))
    idx_ref[...] = jnp.zeros_like(idx_ref)
    idx_ref[0:kcount, 0:t_dev] = index_ref[...]
    lane = lax.broadcasted_iota(jnp.int32, (kcount, 128), 1)
    series = idx_ref[...]
    tile = jnp.where(
        lane < 64, series[:, :128], pltpu.roll(series, (128 - t_dev) % lanes, 1)[:, :128]
    )
    tile = jnp.where(lane == 62, jnp.sum(series, 1, keepdims=True), tile)
    tile = jnp.where(lane == 63, jnp.sum(series * series, 1, keepdims=True), tile)
    tiles[core * g + m] = tile
    idx_all[m] = series
    small[...] = jnp.zeros_like(small)
    small[0:1, 0 : cells // 2] = mask_ref[...].astype(f32)

    @pl.when(jnp.logical_not(has_edge))
    def _():
        tiles[2 * g] = jnp.full((kcount, 128), FAR, f32)

    pl.semaphore_wait(barrier, 2 * g - 1 + beside + jnp.where(has_edge, 1, 0))

    for side in range(2):
        each(1 - side, g, lambda s, side=side: tile_copy(side, s).start())
    each(1, g, lambda s: idx_copy(s).start())
    load.wait()
    for piece in range(groups):
        own_copy(piece).start()
        each(1, g, lambda s, piece=piece: raw_copy(piece, s).start())
    for turn in range(groups - 2):
        tell_line(round_sem.at[turn])
        pl.semaphore_wait(round_sem.at[turn], beside)
    for side in range(2):
        each(1 - side, g, lambda s, side=side: tile_copy(side, s).wait())

    @pl.when(has_edge)
    def _():
        edge_copy().start()

    zero_tile = jnp.zeros((kcount, 128), f32)
    zmsg[...] = lax.fori_loop(0, 2 * g, lambda at, carry: carry + tiles[at], zero_tile)
    each(1, groups, lambda s: z_copy(s).start())
    each(1, g, lambda s: idx_copy(s).wait())

    spot = lax.broadcasted_iota(jnp.int32, (kcount, wide), 1)
    wing = jnp.zeros((kcount, 128), f32)
    tail = jnp.zeros((kcount, wide - 128), f32)

    def tile_at(order):
        inside = lax.rem(order, 2) * g + lax.div(order, 2)
        outside = jnp.logical_or(order < 0, order >= 2 * g)
        return tiles[jnp.where(outside, 2 * g, inside)]

    def window(member):
        order = member * 2 + core
        step = flipped(m, member, g)
        here = jnp.concatenate([idx_all[member], wing], 1)
        before = jnp.concatenate([tile_at(order - 1), tail], 1)
        after = jnp.concatenate([tile_at(order + 1), tail], 1)
        left = pltpu.roll(before, wide - REACH, 1)
        mid = pltpu.roll(here, REACH, 1)
        right = pltpu.roll(after, REACH + t_dev, 1)
        ext = jnp.where(spot < REACH, left, jnp.where(spot < REACH + t_dev, mid, right))
        for k in range(kcount):
            line = pltpu.roll(ext[k : k + 1], wide - REACH - MAXLAG + offset_ref[k], 1)
            line = jnp.broadcast_to(line, (ROWS, wide))
            turned = pltpu.roll(line, 0, 1, stride=1, stride_axis=0)
            raw_win[step, k * ROWS : (k + 1) * ROWS, :] = turned[:, :lanes]

    each(0, g - 1, lambda at: window(jnp.where(core == 0, g - 1 - at, at)))

    @pl.when(has_edge)
    def _():
        edge_copy().wait()

    window(jnp.where(core == 0, 0, g - 1))
    each(1, groups, lambda s: z_copy(s).wait())
    stats = zmsg[...]
    for s in range(1, groups):
        stats = stats + zin[s]
    mean = stats[:, 62:63] / total_days
    var = stats[:, 63:64] / total_days - mean * mean
    outer = 1.0 / jnp.sqrt(var + 1e-06)

    def center_window(step):
        for k in range(kcount):
            value = raw_win[step, k * ROWS : (k + 1) * ROWS, :]
            value = jnp.where(value < NEAR, value - mean[k : k + 1], 0.0)
            win[step, k * ROWS : (k + 1) * ROWS, :] = value.astype(jnp.bfloat16)

    each(0, g, center_window)

    place = lax.broadcasted_iota(jnp.int32, (kcount, lanes), 1)
    day = lax.broadcasted_iota(jnp.int32, (lanes, 128), 0)
    shift = lax.broadcasted_iota(jnp.int32, (lanes, 128), 1) - MAXLAG
    late = jnp.where((day >= t_dev - shift) & (day < t_dev), 1.0, 0.0)
    early = jnp.where(day < -shift, 1.0, 0.0)

    def centered(value, valid):
        return jnp.where(valid, (value - mean).astype(jnp.bfloat16).astype(f32), 0.0)

    def center_body(at, carry):
        return carry + centered(idx_all[at], place < t_dev)

    core_sum = lax.fori_loop(0, g, center_body, jnp.zeros((kcount, lanes), f32))
    inner_block = centered(idx_all[jnp.where(core == 0, 0, g - 1)], place < t_dev)
    edge = jnp.concatenate([tiles[2 * g], tail[:, : lanes - 128]], 1)
    edge = jnp.where(core == 0, pltpu.roll(edge, t_dev - 128, 1), edge)
    opens = jnp.where(core == 0, t_dev - 64, 0)
    closes = jnp.where(core == 0, t_dev, 62)
    outer_block = centered(edge, (place >= opens) & (place < closes) & (edge < NEAR))

    def part(value, sel):
        return jnp.dot(
            value.astype(jnp.bfloat16), sel.astype(jnp.bfloat16), preferred_element_type=f32
        )

    by_shift = (
        jnp.sum(core_sum, 1, keepdims=True)
        + part(outer_block, jnp.where(core == 0, late, early))
        - part(inner_block, jnp.where(core == 0, early, late))
    )
    tot_part[...] = jnp.zeros_like(tot_part)
    for k in range(kcount):
        tot_part[k : k + 1, :] = pltpu.roll(
            by_shift[k : k + 1], lax.rem(128 - offset_ref[k], 128), 1
        )
    total_copy().start()

    low = lax.broadcasted_iota(jnp.int32, (ROWS, 128), 1) < 64
    low_row = lax.broadcasted_iota(jnp.int32, (1, 128), 1) < 64

    def pair_cols(cols, k):
        return jnp.where(low, cols[0:ROWS, k : k + 1], cols[0:ROWS, k + half_k : k + half_k + 1])

    def halves(first_half, second_half, is_low):
        turned_first = pltpu.roll(first_half, 64, 1)
        turned_second = pltpu.roll(second_half, 64, 1)
        zeroth = jnp.where(is_low, first_half, turned_second)
        oneth = jnp.where(is_low, turned_first, second_half)
        mine = jnp.where(core == 0, zeroth, oneth)
        theirs = jnp.where(core == 0, oneth, zeroth)
        return mine, theirs

    group_days = 2 * g * t_dev * 1.0
    mine_at = acc.shape[0] - EXTRA

    def products(piece):
        own_copy(piece).wait()

        def add(step, first_time):
            value = recv[piece, step]
            wide_value = value.astype(f32)
            sums = jnp.sum(wide_value, 0, keepdims=True)
            squares = jnp.sum(wide_value * wide_value, 0, keepdims=True)
            found = jnp.dot(win[step, :, :t_dev], value, preferred_element_type=f32)
            if first_time:
                acc[0 : 2 * count, :] = found
                acc[mine_at : mine_at + 1, :] = sums
                acc[mine_at + 1 : mine_at + 2, :] = squares
            else:
                acc[0 : 2 * count, :] += found
                acc[mine_at : mine_at + 1, :] += sums
                acc[mine_at + 1 : mine_at + 2, :] += squares

        add(0, True)

        def body(step, carry):
            raw_copy(piece, step).wait()
            add(step, False)
            return carry

        lax.fori_loop(1, g, body, 0)
        for k in range(half_k):
            at = k * ROWS
            mine, theirs = halves(
                acc[at : at + ROWS, :], acc[count + at : count + at + ROWS, :], low
            )
            acc[at : at + ROWS, :] = mine
            other[piece, at : at + ROWS, :] = theirs
        for row in range(2):
            value = acc[mine_at + row : mine_at + row + 1, :]
            mine, theirs = halves(value, value, low_row)
            acc[mine_at + row : mine_at + row + 1, :] = mine
            other[piece, count + row : count + row + 1, :] = theirs
        swap_copy(piece).start()
        swap_copy(piece).wait()

    def joined(piece, k):
        at = k * ROWS
        return acc[at : at + ROWS, :] + partner_in[piece, at : at + ROWS, :]

    def joined_row(piece, row):
        return (
            acc[mine_at + row : mine_at + row + 1, :]
            + partner_in[piece, count + row : count + row + 1, :]
        )

    other[...] = jnp.zeros_like(other)
    far[...] = jnp.zeros_like(far)
    sent_extra[...] = jnp.zeros_like(sent_extra)
    for piece in range(groups - 1):
        products(piece)
        if piece == 0:
            total_copy().wait()
            own_tot = tot_part[...] + tot_in[...]
            own_cols = jnp.transpose(own_tot)
        sx = joined_row(piece, 0)
        sent_extra[piece, 0:1, :] = sx
        sent_extra[piece, 1:2, :] = joined_row(piece, 1)
        local_mean = sx / group_days
        for k in range(half_k):
            value = joined(piece, k) - local_mean * pair_cols(own_cols, k)
            top = jnp.max(jnp.abs(value), 0, keepdims=True)
            sent_extra[piece, 2 + k : 3 + k, :] = top
            scaled = value * (TOP / jnp.maximum(top, 1e-30))
            sent[piece, k * ROWS : (k + 1) * ROWS, :] = (
                jnp.round(scaled).astype(jnp.int32).astype(jnp.int16)
            )
        sent_extra[piece, EXTRA:, :] = own_tot
        sum_copy(piece).start()
        extra_copy(piece).start()

    last = groups - 1
    products(last)
    sx = joined_row(last, 0)
    sq = joined_row(last, 1)
    all_cols = own_cols
    for piece in range(groups - 1):
        extra_copy(piece).wait()
        sum_copy(piece).wait()
        far_x = got_extra[piece, 0:1, :]
        sx = sx + far_x
        sq = sq + got_extra[piece, 1:2, :]
        far_mean = far_x / group_days
        far_cols = jnp.transpose(got_extra[piece, EXTRA:, :])
        all_cols = all_cols + far_cols
        for k in range(half_k):
            at = k * ROWS
            coded = got[piece, at : at + ROWS, :].astype(jnp.int32).astype(f32)
            far[at : at + ROWS, :] += coded * (
                got_extra[piece, 2 + k : 3 + k, :] * (1.0 / TOP)
            ) + far_mean * pair_cols(far_cols, k)
    mean_x = sx / total_days
    var_x = sq / total_days - mean_x * mean_x
    mask = small[0:1, :]
    mask = mask + pltpu.roll(mask, 64, 1)
    inner = mask / (total_days * jnp.sqrt(var_x + 1e-06))

    def normal(k):
        value = joined(last, k) + far[k * ROWS : (k + 1) * ROWS, :]
        value = value - mean_x * pair_cols(all_cols, k)
        scale = jnp.where(low_row, outer[k : k + 1], outer[k + half_k : k + half_k + 1])
        return value * (inner * scale)

    small_int = lag_ref[...] + MAXLAG
    small[0:1, 0 : lag_ref.shape[1]] = small_int.astype(f32)
    chosen = jnp.broadcast_to(small[0:1, :].astype(jnp.int32), (64, 128))
    kept = lag_ref.shape[1]
    for k in range(0, half_k, 2):
        upper = normal(k)
        under = normal(k + 1) if k + 1 < half_k else upper
        flat = jnp.transpose(jnp.concatenate([upper, under], 0))
        for side in range(2):
            rows = flat[side * 64 : (side + 1) * 64, :]
            out_ref[k + side * half_k] = jnp.take_along_axis(rows, chosen, axis=1)[:, :kept]
            if k + 1 < half_k:
                out_ref[k + 1 + side * half_k] = jnp.take_along_axis(
                    rows, chosen + 64, axis=1
                )[:, :kept]


def shards(field, index, lag_list, index_offset, sea_mask):
    t_dev, cells_all = field.shape
    devices = lax.axis_size("tm")
    kcount = index.shape[1]
    lanes = round_up(t_dev, 128)
    groups = GROUPS
    g = devices // 2 // groups
    rows = kcount * ROWS
    half = rows // 2
    sizes = (devices, t_dev, kcount, groups, g)
    dma = pltpu.SemaphoreType.DMA
    f32 = jnp.float32
    vmem = pl.BlockSpec(memory_space=pltpu.VMEM)
    maps = pl.pallas_call(
        functools.partial(kernel, sizes),
        out_shape=jax.ShapeDtypeStruct((kcount, 64, lag_list.shape[0]), f32),
        in_specs=[
            pl.BlockSpec(memory_space=pl.ANY),
            vmem,
            vmem,
            pl.BlockSpec(memory_space=pltpu.SMEM),
            vmem,
        ],
        out_specs=vmem,
        scratch_shapes=[
            pltpu.VMEM((t_dev, cells_all), jnp.bfloat16),
            pltpu.VMEM((kcount, lanes), f32),
            pltpu.VMEM((g, kcount, lanes), f32),
            pltpu.VMEM((2 * g + 1, kcount, 128), f32),
            pltpu.VMEM((kcount, 128), f32),
            pltpu.VMEM((groups, kcount, 128), f32),
            pltpu.VMEM((groups, g, t_dev, 128), jnp.bfloat16),
            pltpu.VMEM((g, rows, lanes), f32),
            pltpu.VMEM((g, rows, lanes), jnp.bfloat16),
            pltpu.VMEM((rows + EXTRA, 128), f32),
            pltpu.VMEM((groups, half + EXTRA, 128), f32),
            pltpu.VMEM((groups, half + EXTRA, 128), f32),
            pltpu.VMEM((groups, half, 128), jnp.int16),
            pltpu.VMEM((groups, EXTRA + 16, 128), f32),
            pltpu.VMEM((groups, half, 128), jnp.int16),
            pltpu.VMEM((groups, EXTRA + 16, 128), f32),
            pltpu.VMEM((half, 128), f32),
            pltpu.VMEM((8, 128), f32),
            pltpu.VMEM((16, 128), f32),
            pltpu.VMEM((16, 128), f32),
            dma((groups, g)),
            dma((groups, g)),
            dma((g,)),
            dma((g,)),
            dma((2, g)),
            dma((2, g)),
            dma((4,)),
            dma((groups,)),
            dma((groups,)),
            dma((groups,)),
            dma((groups,)),
            dma((2, groups)),
            dma((2, groups)),
            dma((groups + 1,)),
            pltpu.SemaphoreType.REGULAR((groups,)),
        ],
        compiler_params=pltpu.CompilerParams(
            collective_id=0, has_side_effects=True, vmem_limit_bytes=60 * 1024 * 1024
        ),
    )(field, index.T, lag_list[None, :], index_offset, sea_mask[None, :])
    return jnp.transpose(maps, (1, 0, 2))


def solution(mesh):
    return jax.shard_map(
        shards,
        mesh=mesh,
        in_specs=(P("tm", None), P("tm", None), P(), P(), P("tm")),
        out_specs=P("tm", None, None),
        check_vma=False,
    )
```

```python
import functools

import jax
import jax.numpy as jnp
from jax import lax
from jax.experimental import pallas as pl
from jax.experimental.pallas import tpu as pltpu
from jax.sharding import PartitionSpec as P

MAXLAG = 30
MAXOFF = 14
REACH = 64
ROWS = 64
BASE = 16
EXTRA = 8
TOP = 32767.0
FAR = 1e30
NEAR = 1e29
GROUPS = 4
MESH = pl.DeviceIdType.MESH


def round_up(value, unit):
    return -(-value // unit) * unit


def kernel(
    sizes,
    field_hbm,
    index_ref,
    lag_ref,
    offset_ref,
    mask_ref,
    out_ref,
    field_ref,
    idx_ref,
    idx_all,
    tiles,
    zmsg,
    zin,
    recv,
    raw_win,
    win,
    acc,
    mine,
    other,
    partner_in,
    sent,
    sent_extra,
    got,
    got_extra,
    far,
    small,
    tot_part,
    tot_in,
    raw_send,
    raw_recv,
    idx_send,
    idx_recv,
    tile_send,
    tile_recv,
    lone_sem,
    z_send,
    z_recv,
    swap_send,
    swap_recv,
    sum_send,
    sum_recv,
    own_sem,
    round_sem,
):
    devices, t_dev, kcount, groups, g = sizes
    lanes = idx_ref.shape[1]
    wide = lanes + 128
    half_k = kcount // 2
    count = half_k * ROWS
    cells = 128
    me = lax.axis_index("tm")
    core = lax.rem(me, 2)
    chip = lax.div(me, 2)
    h = lax.div(chip, g)
    m = lax.rem(chip, g)
    partner = chip * 2 + (1 - core)
    edge_peer = ((h + 2 * core - 1) * g + m) * 2 + (1 - core)
    has_edge = jnp.where(core == 0, h > 0, h < groups - 1)
    f32 = jnp.float32
    total_days = devices * t_dev * 1.0

    def flipped(value, step, size):
        found, bit = 0, 1
        while bit < size:
            flip = lax.rem(lax.div(value, bit) + lax.div(step, bit), 2)
            found, bit = found + flip * bit, bit * 2
        return found

    def across(step):
        return flipped(m, step, g)

    def device_of(group, member):
        return (group * g + member) * 2 + core

    def remote(src, dst, send, recv_s, device):
        return pltpu.make_async_remote_copy(
            src_ref=src,
            dst_ref=dst,
            send_sem=send,
            recv_sem=recv_s,
            device_id=(device,),
            device_id_type=MESH,
        )

    def block(at):
        return field_ref.at[:, pl.ds(pl.multiple_of(at * cells, cells), cells)]

    def plane_of(piece):
        return flipped(h, groups - 1 - piece, groups)

    def raw_copy(piece, step):
        to = across(step)
        return remote(
            block(plane_of(piece) * g + to),
            recv.at[piece, step],
            raw_send.at[piece, step],
            raw_recv.at[piece, step],
            device_of(h, to),
        )

    def own_copy(piece):
        return pltpu.make_async_copy(
            block(plane_of(piece) * g + m), recv.at[piece, 0], own_sem.at[piece]
        )

    def idx_copy(step):
        return remote(
            idx_ref,
            idx_all.at[m],
            idx_send.at[step],
            idx_recv.at[step],
            device_of(h, across(step)),
        )

    def tile_copy(side, step):
        to = (h * g + across(step)) * 2 + (core if side == 0 else 1 - core)
        tile = tiles.at[core * g + m]
        return remote(
            tile, tile, tile_send.at[side, step], tile_recv.at[side, step], to
        )

    def edge_copy():
        return remote(
            tiles.at[jnp.where(core == 0, 0, 2 * g - 1)],
            tiles.at[2 * g],
            lone_sem.at[0],
            lone_sem.at[1],
            edge_peer,
        )

    def total_copy():
        return remote(tot_part, tot_in, lone_sem.at[2], lone_sem.at[3], partner)

    def z_copy(step):
        return remote(
            zmsg,
            zin.at[step],
            z_send.at[step],
            z_recv.at[step],
            device_of(flipped(h, step, groups), m),
        )

    def swap_copy(piece):
        return remote(
            other.at[piece],
            partner_in.at[piece],
            swap_send.at[piece],
            swap_recv.at[piece],
            partner,
        )

    def sum_copy(piece):
        return remote(
            sent.at[piece],
            got.at[piece],
            sum_send.at[0, piece],
            sum_recv.at[0, piece],
            device_of(plane_of(piece), m),
        )

    def extra_copy(piece):
        return remote(
            sent_extra.at[piece],
            got_extra.at[piece],
            sum_send.at[1, piece],
            sum_recv.at[1, piece],
            device_of(plane_of(piece), m),
        )

    def each(low_step, high_step, act):
        def body(step, carry):
            act(step)
            return carry

        lax.fori_loop(low_step, high_step, body, 0)

    load = pltpu.make_async_copy(field_hbm, field_ref, own_sem.at[groups])
    load.start()
    barrier = pltpu.get_barrier_semaphore()

    def tell(sem, device):
        pl.semaphore_signal(sem, inc=1, device_id=(device,), device_id_type=MESH)

    def tell_line(sem):
        @pl.when(h > 0)
        def _():
            tell(sem, device_of(h - 1, m))

        @pl.when(h < groups - 1)
        def _():
            tell(sem, device_of(h + 1, m))

    beside = jnp.where(h > 0, 1, 0) + jnp.where(h < groups - 1, 1, 0)
    tell_line(barrier)

    @pl.when(has_edge)
    def _():
        tell(barrier, edge_peer)

    each(1, 2 * g, lambda s: tell(barrier, (h * g + across(lax.div(s, 2))) * 2 + lax.rem(core + s, 2)))
    idx_ref[...] = jnp.zeros_like(idx_ref)
    idx_ref[0:kcount, 0:t_dev] = index_ref[...]
    lane = lax.broadcasted_iota(jnp.int32, (kcount, 128), 1)
    series = idx_ref[...]
    tile = jnp.where(
        lane < 64, series[:, :128], pltpu.roll(series, (128 - t_dev) % lanes, 1)[:, :128]
    )
    tile = jnp.where(lane == 62, jnp.sum(series, 1, keepdims=True), tile)
    tile = jnp.where(lane == 63, jnp.sum(series * series, 1, keepdims=True), tile)
    tiles[core * g + m] = tile
    idx_all[m] = series
    other[...] = jnp.zeros_like(other)
    far[...] = jnp.zeros_like(far)
    sent_extra[...] = jnp.zeros_like(sent_extra)
    small[...] = jnp.zeros_like(small)
    small[0:1, 0 : cells // 2] = mask_ref[...].astype(f32)

    @pl.when(jnp.logical_not(has_edge))
    def _():
        tiles[2 * g] = jnp.full((kcount, 128), FAR, f32)

    pl.semaphore_wait(barrier, 2 * g - 1 + beside + jnp.where(has_edge, 1, 0))

    for side in range(2):
        each(1 - side, g, lambda s, side=side: tile_copy(side, s).start())
    each(1, g, lambda s: idx_copy(s).start())
    load.wait()
    for piece in range(groups):
        own_copy(piece).start()
        each(1, g, lambda s, piece=piece: raw_copy(piece, s).start())
    for turn in range(groups - 2):
        tell_line(round_sem.at[turn])
        pl.semaphore_wait(round_sem.at[turn], beside)
    for side in range(2):
        each(1 - side, g, lambda s, side=side: tile_copy(side, s).wait())

    @pl.when(has_edge)
    def _():
        edge_copy().start()

    zero_tile = jnp.zeros((kcount, 128), f32)
    zmsg[...] = lax.fori_loop(0, 2 * g, lambda at, carry: carry + tiles[at], zero_tile)
    each(1, groups, lambda s: z_copy(s).start())
    each(1, g, lambda s: idx_copy(s).wait())

    spot = lax.broadcasted_iota(jnp.int32, (kcount, wide), 1)
    wing = jnp.zeros((kcount, 128), f32)
    tail = jnp.zeros((kcount, wide - 128), f32)

    def tile_at(order):
        inside = lax.rem(order, 2) * g + lax.div(order, 2)
        outside = jnp.logical_or(order < 0, order >= 2 * g)
        return tiles[jnp.where(outside, 2 * g, inside)]

    def window(member):
        order = member * 2 + core
        step = flipped(m, member, g)
        here = jnp.concatenate([idx_all[member], wing], 1)
        before = jnp.concatenate([tile_at(order - 1), tail], 1)
        after = jnp.concatenate([tile_at(order + 1), tail], 1)
        left = pltpu.roll(before, wide - REACH, 1)
        mid = pltpu.roll(here, REACH, 1)
        right = pltpu.roll(after, REACH + t_dev, 1)
        ext = jnp.where(spot < REACH, left, jnp.where(spot < REACH + t_dev, mid, right))
        for k in range(kcount):
            line = pltpu.roll(ext[k : k + 1], wide - REACH - MAXLAG + offset_ref[k], 1)
            line = jnp.broadcast_to(line, (BASE, wide))
            raw_win[step, k * BASE : (k + 1) * BASE, :] = pltpu.roll(
                line, 0, 1, stride=1, stride_axis=0
            )

    each(0, g - 1, lambda at: window(jnp.where(core == 0, g - 1 - at, at)))

    @pl.when(has_edge)
    def _():
        edge_copy().wait()

    window(jnp.where(core == 0, 0, g - 1))
    each(1, groups, lambda s: z_copy(s).wait())
    stats = zmsg[...]
    for s in range(1, groups):
        stats = stats + zin[s]
    mean = stats[:, 62:63] / total_days
    var = stats[:, 63:64] / total_days - mean * mean
    outer = 1.0 / jnp.sqrt(var + 1e-06)

    def center_window(step):
        for k in range(kcount):
            value = raw_win[step, k * BASE : (k + 1) * BASE, :]
            value = jnp.where(value < NEAR, value - mean[k : k + 1], 0.0).astype(jnp.bfloat16)
            for turn in range(0, ROWS, BASE):
                turned = value if turn == 0 else pltpu.roll(value, turn, 1)
                win[step, k * ROWS + turn : k * ROWS + turn + BASE, :] = turned[:, :lanes]

    low = lax.broadcasted_iota(jnp.int32, (ROWS, 128), 1) < 64
    low_row = lax.broadcasted_iota(jnp.int32, (1, 128), 1) < 64

    def pair_cols(cols, k):
        return jnp.where(low, cols[0:ROWS, k : k + 1], cols[0:ROWS, k + half_k : k + half_k + 1])

    def halves(first_half, second_half, is_low):
        turned_first = pltpu.roll(first_half, 64, 1)
        turned_second = pltpu.roll(second_half, 64, 1)
        zeroth = jnp.where(is_low, first_half, turned_second)
        oneth = jnp.where(is_low, turned_first, second_half)
        return jnp.where(core == 0, zeroth, oneth), jnp.where(core == 0, oneth, zeroth)

    group_days = 2 * g * t_dev * 1.0
    sums_at = 2 * count

    def add(pieces, step, first_time):
        width = 128 * len(pieces)
        value = jnp.concatenate([recv[piece, step] for piece in pieces], 1)
        wide_value = value.astype(f32)
        sums = jnp.sum(wide_value, 0, keepdims=True)
        squares = jnp.sum(wide_value * wide_value, 0, keepdims=True)
        found = jnp.dot(win[step, :, :t_dev], value, preferred_element_type=f32)
        if first_time:
            acc[0:sums_at, :width] = found
            acc[sums_at : sums_at + 1, :width] = sums
            acc[sums_at + 1 : sums_at + 2, :width] = squares
        else:
            acc[0:sums_at, :width] += found
            acc[sums_at : sums_at + 1, :width] += sums
            acc[sums_at + 1 : sums_at + 2, :width] += squares

    def split(piece, column):
        column = slice(column * 128, column * 128 + 128)
        for k in range(half_k):
            at = k * ROWS
            kept, given = halves(
                acc[at : at + ROWS, column], acc[count + at : count + at + ROWS, column], low
            )
            mine[piece, at : at + ROWS, :] = kept
            other[piece, at : at + ROWS, :] = given
        for row in range(2):
            value = acc[sums_at + row : sums_at + row + 1, column]
            kept, given = halves(value, value, low_row)
            mine[piece, count + row : count + row + 1, :] = kept
            other[piece, count + row : count + row + 1, :] = given
        swap_copy(piece).start()

    def products(piece):
        own_copy(piece).wait()
        add([piece], 0, True)

        def body(step, carry):
            raw_copy(piece, step).wait()
            add([piece], step, False)
            return carry

        lax.fori_loop(1, g, body, 0)
        split(piece, 0)

    def joined(piece, k):
        at = k * ROWS
        return mine[piece, at : at + ROWS, :] + partner_in[piece, at : at + ROWS, :]

    def joined_row(piece, row):
        at = count + row
        return mine[piece, at : at + 1, :] + partner_in[piece, at : at + 1, :]

    def send_sums(piece):
        swap_copy(piece).wait()
        sx = joined_row(piece, 0)
        sent_extra[piece, 0:1, :] = sx
        sent_extra[piece, 1:2, :] = joined_row(piece, 1)
        local_mean = sx / group_days
        for k in range(half_k):
            value = joined(piece, k) - local_mean * pair_cols(own_cols, k)
            top = jnp.max(jnp.abs(value), 0, keepdims=True)
            sent_extra[piece, 2 + k : 3 + k, :] = top
            scaled = value * (TOP / jnp.maximum(top, 1e-30))
            sent[piece, k * ROWS : (k + 1) * ROWS, :] = (
                jnp.round(scaled).astype(jnp.int32).astype(jnp.int16)
            )
        sent_extra[piece, EXTRA:, :] = own_tot
        sum_copy(piece).start()
        extra_copy(piece).start()

    last = groups - 1
    early_pieces = [0, 1] if last > 1 else [0]
    for piece in early_pieces:
        own_copy(piece).wait()
        each(1, g, lambda s, piece=piece: raw_copy(piece, s).wait())

    def early_body(step, first_time):
        center_window(step)
        add(early_pieces, step, first_time)

    early_body(0, True)
    if g <= 4:
        for step in range(1, g):
            early_body(step, False)
    else:
        each(1, g, lambda s: early_body(s, False))
    for piece in early_pieces:
        split(piece, piece)

    place = lax.broadcasted_iota(jnp.int32, (kcount, lanes), 1)
    day = lax.broadcasted_iota(jnp.int32, (lanes, 128), 0)
    shift = lax.broadcasted_iota(jnp.int32, (lanes, 128), 1) - MAXLAG
    late = jnp.where((day >= t_dev - shift) & (day < t_dev), 1.0, 0.0)
    early = jnp.where(day < -shift, 1.0, 0.0)

    def centered(value, valid):
        return jnp.where(valid, (value - mean).astype(jnp.bfloat16).astype(f32), 0.0)

    def center_body(at, carry):
        return carry + centered(idx_all[at], place < t_dev)

    core_sum = lax.fori_loop(0, g, center_body, jnp.zeros((kcount, lanes), f32))
    inner_block = centered(idx_all[jnp.where(core == 0, 0, g - 1)], place < t_dev)
    edge = jnp.concatenate([tiles[2 * g], tail[:, : lanes - 128]], 1)
    edge = jnp.where(core == 0, pltpu.roll(edge, t_dev - 128, 1), edge)
    opens = jnp.where(core == 0, t_dev - 64, 0)
    closes = jnp.where(core == 0, t_dev, 62)
    outer_block = centered(edge, (place >= opens) & (place < closes) & (edge < NEAR))

    def part(value, sel):
        return jnp.dot(
            value.astype(jnp.bfloat16), sel.astype(jnp.bfloat16), preferred_element_type=f32
        )

    by_shift = (
        jnp.sum(core_sum, 1, keepdims=True)
        + part(outer_block, jnp.where(core == 0, late, early))
        - part(inner_block, jnp.where(core == 0, early, late))
    )
    tot_part[...] = jnp.zeros_like(tot_part)
    for k in range(kcount):
        tot_part[k : k + 1, :] = pltpu.roll(
            by_shift[k : k + 1], lax.rem(128 - offset_ref[k], 128), 1
        )
    total_copy().start()

    total_copy().wait()
    own_tot = tot_part[...] + tot_in[...]
    own_cols = jnp.transpose(own_tot)
    for piece in early_pieces:
        send_sums(piece)
    for piece in range(len(early_pieces), last):
        products(piece)
        send_sums(piece)
    products(last)
    sx = jnp.zeros((1, 128), f32)
    sq = jnp.zeros((1, 128), f32)
    all_cols = own_cols
    for piece in range(groups - 1):
        extra_copy(piece).wait()
        sum_copy(piece).wait()
        far_x = got_extra[piece, 0:1, :]
        sx = sx + far_x
        sq = sq + got_extra[piece, 1:2, :]
        far_mean = far_x / group_days
        far_cols = jnp.transpose(got_extra[piece, EXTRA:, :])
        all_cols = all_cols + far_cols
        for k in range(half_k):
            at = k * ROWS
            coded = got[piece, at : at + ROWS, :].astype(jnp.int32).astype(f32)
            far[at : at + ROWS, :] += coded * (
                got_extra[piece, 2 + k : 3 + k, :] * (1.0 / TOP)
            ) + far_mean * pair_cols(far_cols, k)
    swap_copy(last).wait()
    sx = sx + joined_row(last, 0)
    sq = sq + joined_row(last, 1)
    mean_x = sx / total_days
    var_x = sq / total_days - mean_x * mean_x
    mask = small[0:1, :]
    mask = mask + pltpu.roll(mask, 64, 1)
    inner = mask / (total_days * jnp.sqrt(var_x + 1e-06))

    def normal(k):
        value = joined(last, k) + far[k * ROWS : (k + 1) * ROWS, :]
        value = value - mean_x * pair_cols(all_cols, k)
        scale = jnp.where(low_row, outer[k : k + 1], outer[k + half_k : k + half_k + 1])
        return value * (inner * scale)

    small_int = lag_ref[...] + MAXLAG
    small[0:1, 0 : lag_ref.shape[1]] = small_int.astype(f32)
    chosen = jnp.broadcast_to(small[0:1, :].astype(jnp.int32), (64, 128))
    kept = lag_ref.shape[1]
    for k in range(0, half_k, 2):
        upper = normal(k)
        under = normal(k + 1) if k + 1 < half_k else upper
        flat = jnp.transpose(jnp.concatenate([upper, under], 0))
        for side in range(2):
            rows = flat[side * 64 : (side + 1) * 64, :]
            out_ref[k + side * half_k] = jnp.take_along_axis(rows, chosen, axis=1)[:, :kept]
            if k + 1 < half_k:
                out_ref[k + 1 + side * half_k] = jnp.take_along_axis(
                    rows, chosen + 64, axis=1
                )[:, :kept]


def shards(field, index, lag_list, index_offset, sea_mask):
    t_dev, cells_all = field.shape
    devices = lax.axis_size("tm")
    kcount = index.shape[1]
    lanes = round_up(t_dev, 128)
    groups = GROUPS
    g = devices // 2 // groups
    rows = kcount * ROWS
    half = rows // 2
    sizes = (devices, t_dev, kcount, groups, g)
    dma = pltpu.SemaphoreType.DMA
    f32 = jnp.float32
    vmem = pl.BlockSpec(memory_space=pltpu.VMEM)
    maps = pl.pallas_call(
        functools.partial(kernel, sizes),
        out_shape=jax.ShapeDtypeStruct((kcount, 64, lag_list.shape[0]), f32),
        in_specs=[
            pl.BlockSpec(memory_space=pl.ANY),
            vmem,
            vmem,
            pl.BlockSpec(memory_space=pltpu.SMEM),
            vmem,
        ],
        out_specs=vmem,
        scratch_shapes=[
            pltpu.VMEM((t_dev, cells_all), jnp.bfloat16),
            pltpu.VMEM((kcount, lanes), f32),
            pltpu.VMEM((g, kcount, lanes), f32),
            pltpu.VMEM((2 * g + 1, kcount, 128), f32),
            pltpu.VMEM((kcount, 128), f32),
            pltpu.VMEM((groups, kcount, 128), f32),
            pltpu.VMEM((groups, g, t_dev, 128), jnp.bfloat16),
            pltpu.VMEM((g, kcount * BASE, lanes + 128), f32),
            pltpu.VMEM((g, rows, lanes), jnp.bfloat16),
            pltpu.VMEM((rows + EXTRA, 256), f32),
            pltpu.VMEM((groups, half + EXTRA, 128), f32),
            pltpu.VMEM((groups, half + EXTRA, 128), f32),
            pltpu.VMEM((groups, half + EXTRA, 128), f32),
            pltpu.VMEM((groups, half, 128), jnp.int16),
            pltpu.VMEM((groups, EXTRA + 16, 128), f32),
            pltpu.VMEM((groups, half, 128), jnp.int16),
            pltpu.VMEM((groups, EXTRA + 16, 128), f32),
            pltpu.VMEM((half, 128), f32),
            pltpu.VMEM((8, 128), f32),
            pltpu.VMEM((16, 128), f32),
            pltpu.VMEM((16, 128), f32),
            dma((groups, g)),
            dma((groups, g)),
            dma((g,)),
            dma((g,)),
            dma((2, g)),
            dma((2, g)),
            dma((4,)),
            dma((groups,)),
            dma((groups,)),
            dma((groups,)),
            dma((groups,)),
            dma((2, groups)),
            dma((2, groups)),
            dma((groups + 1,)),
            pltpu.SemaphoreType.REGULAR((groups,)),
        ],
        compiler_params=pltpu.CompilerParams(
            collective_id=0, has_side_effects=True, vmem_limit_bytes=60 * 1024 * 1024
        ),
    )(field, index.T, lag_list[None, :], index_offset, sea_mask[None, :])
    return jnp.transpose(maps, (1, 0, 2))


def solution(mesh):
    return jax.shard_map(
        shards,
        mesh=mesh,
        in_specs=(P("tm", None), P("tm", None), P(), P(), P("tm")),
        out_specs=P("tm", None, None),
        check_vma=False,
    )
```

```python
import functools

import jax
import jax.numpy as jnp
from jax import lax
from jax.experimental import pallas as pl
from jax.experimental.pallas import tpu as pltpu
from jax.sharding import PartitionSpec as P

MAXLAG = 30
MAXOFF = 14
REACH = 64
ROWS = 64
BASE = 16
EXTRA = 8
TOP = 32767.0
FAR = 1e30
NEAR = 1e29
GROUPS = 4
MESH = pl.DeviceIdType.MESH


def round_up(value, unit):
    return -(-value // unit) * unit


def kernel(
    sizes,
    field_hbm,
    index_ref,
    lag_ref,
    offset_ref,
    mask_ref,
    out_ref,
    field_ref,
    idx_ref,
    idx_all,
    tiles,
    zmsg,
    zin,
    recv,
    raw_win,
    win,
    acc,
    mine,
    other,
    partner_in,
    sent,
    sent_extra,
    got,
    got_extra,
    far,
    out_buf,
    small,
    tot_part,
    tot_in,
    raw_send,
    raw_recv,
    idx_send,
    idx_recv,
    tile_send,
    tile_recv,
    lone_sem,
    z_send,
    z_recv,
    swap_send,
    swap_recv,
    sum_send,
    sum_recv,
    own_sem,
    round_sem,
    out_sem,
):
    devices, t_dev, kcount, groups, g = sizes
    lanes = idx_ref.shape[1]
    wide = lanes + 128
    half_k = kcount // 2
    count = half_k * ROWS
    cells = 128
    me = lax.axis_index("tm")
    core = lax.rem(me, 2)
    chip = lax.div(me, 2)
    h = lax.div(chip, g)
    m = lax.rem(chip, g)
    partner = chip * 2 + (1 - core)
    edge_peer = ((h + 2 * core - 1) * g + m) * 2 + (1 - core)
    has_edge = jnp.where(core == 0, h > 0, h < groups - 1)
    f32 = jnp.float32
    total_days = devices * t_dev * 1.0

    def flipped(value, step, size):
        found, bit = 0, 1
        while bit < size:
            flip = lax.rem(lax.div(value, bit) + lax.div(step, bit), 2)
            found, bit = found + flip * bit, bit * 2
        return found

    def across(step):
        return flipped(m, step, g)

    def device_of(group, member):
        return (group * g + member) * 2 + core

    def remote(src, dst, send, recv_s, device):
        return pltpu.make_async_remote_copy(
            src_ref=src,
            dst_ref=dst,
            send_sem=send,
            recv_sem=recv_s,
            device_id=(device,),
            device_id_type=MESH,
        )

    def block(at):
        return field_ref.at[:, pl.ds(pl.multiple_of(at * cells, cells), cells)]

    inner = jnp.logical_or(h == 1, h == 2)
    upper = lax.div(h, 2)
    beside_h = h + 1 - 2 * lax.rem(h, 2)

    def plane_of(piece):
        if piece == 0:
            return (groups - 1) * (1 - upper)
        if piece == 1:
            return 2 - upper
        return beside_h if piece == 2 else h

    def raw_copy(piece, step):
        to = across(step)
        return remote(
            block(plane_of(piece) * g + to),
            recv.at[piece, step],
            raw_send.at[piece, step],
            raw_recv.at[piece, step],
            device_of(h, to),
        )

    def own_copy(piece):
        return pltpu.make_async_copy(
            block(plane_of(piece) * g + m), recv.at[piece, 0], own_sem.at[piece]
        )

    def idx_copy(step):
        return remote(
            idx_ref,
            idx_all.at[m],
            idx_send.at[step],
            idx_recv.at[step],
            device_of(h, across(step)),
        )

    def tile_copy(side, step):
        to = (h * g + across(step)) * 2 + (core if side == 0 else 1 - core)
        tile = tiles.at[core * g + m]
        return remote(
            tile, tile, tile_send.at[side, step], tile_recv.at[side, step], to
        )

    def edge_copy():
        return remote(
            tiles.at[jnp.where(core == 0, 0, 2 * g - 1)],
            tiles.at[2 * g],
            lone_sem.at[0],
            lone_sem.at[1],
            edge_peer,
        )

    def total_copy():
        return remote(tot_part, tot_in, lone_sem.at[2], lone_sem.at[3], partner)

    def z_copy(step):
        return remote(
            zmsg,
            zin.at[step],
            z_send.at[step],
            z_recv.at[step],
            device_of(flipped(h, step, groups), m),
        )

    def swap_copy(piece):
        return remote(
            other.at[piece],
            partner_in.at[piece],
            swap_send.at[piece],
            swap_recv.at[piece],
            partner,
        )

    def slot_of(piece):
        return piece if piece == 2 else jnp.where(inner, 3, piece)

    def receiver(piece):
        if piece == 2:
            return device_of(beside_h, m)
        return device_of(jnp.where(inner, plane_of(piece), beside_h), m)

    def sum_copies(piece, slot):
        return [
            remote(
                sent.at[piece],
                got.at[slot],
                sum_send.at[0, piece],
                sum_recv.at[0, slot],
                receiver(piece),
            ),
            remote(
                sent_extra.at[piece],
                got_extra.at[slot],
                sum_send.at[1, piece],
                sum_recv.at[1, slot],
                receiver(piece),
            ),
        ]

    def arrived(slot):
        for copy in sum_copies(2, slot):
            copy.wait_recv()

    def each(low_step, high_step, act):
        def body(step, carry):
            act(step)
            return carry

        lax.fori_loop(low_step, high_step, body, 0)

    load = pltpu.make_async_copy(field_hbm, field_ref, own_sem.at[groups])
    load.start()
    barrier = pltpu.get_barrier_semaphore()

    def tell(sem, device):
        pl.semaphore_signal(sem, inc=1, device_id=(device,), device_id_type=MESH)

    def tell_line(sem):
        @pl.when(h > 0)
        def _():
            tell(sem, device_of(h - 1, m))

        @pl.when(h < groups - 1)
        def _():
            tell(sem, device_of(h + 1, m))

    beside = jnp.where(h > 0, 1, 0) + jnp.where(h < groups - 1, 1, 0)
    tell_line(barrier)

    @pl.when(has_edge)
    def _():
        tell(barrier, edge_peer)

    each(1, 2 * g, lambda s: tell(barrier, (h * g + across(lax.div(s, 2))) * 2 + lax.rem(core + s, 2)))
    idx_ref[...] = jnp.zeros_like(idx_ref)
    idx_ref[0:kcount, 0:t_dev] = index_ref[...]
    lane = lax.broadcasted_iota(jnp.int32, (kcount, 128), 1)
    series = idx_ref[...]
    tile = jnp.where(
        lane < 64, series[:, :128], pltpu.roll(series, (128 - t_dev) % lanes, 1)[:, :128]
    )
    tile = jnp.where(lane == 62, jnp.sum(series, 1, keepdims=True), tile)
    tile = jnp.where(lane == 63, jnp.sum(series * series, 1, keepdims=True), tile)
    tiles[core * g + m] = tile
    idx_all[m] = series
    other[...] = jnp.zeros_like(other)
    far[...] = jnp.zeros_like(far)
    sent_extra[...] = jnp.zeros_like(sent_extra)
    small[...] = jnp.zeros_like(small)
    small[0:1, 0 : cells // 2] = mask_ref[...].astype(f32)

    @pl.when(jnp.logical_not(has_edge))
    def _():
        tiles[2 * g] = jnp.full((kcount, 128), FAR, f32)

    pl.semaphore_wait(barrier, 2 * g - 1 + beside + jnp.where(has_edge, 1, 0))

    for side in range(2):
        each(1 - side, g, lambda s, side=side: tile_copy(side, s).start())
    each(1, g, lambda s: idx_copy(s).start())
    load.wait()
    for piece in range(groups):
        own_copy(piece).start()
        each(1, g, lambda s, piece=piece: raw_copy(piece, s).start())
    for turn in range(groups - 2):
        tell_line(round_sem.at[turn])
        pl.semaphore_wait(round_sem.at[turn], beside)
    for side in range(2):
        each(1 - side, g, lambda s, side=side: tile_copy(side, s).wait())

    @pl.when(has_edge)
    def _():
        edge_copy().start()

    zero_tile = jnp.zeros((kcount, 128), f32)
    zmsg[...] = lax.fori_loop(0, 2 * g, lambda at, carry: carry + tiles[at], zero_tile)
    each(1, groups, lambda s: z_copy(s).start())
    each(1, g, lambda s: idx_copy(s).wait())

    spot = lax.broadcasted_iota(jnp.int32, (kcount, wide), 1)
    wing = jnp.zeros((kcount, 128), f32)
    tail = jnp.zeros((kcount, wide - 128), f32)

    def tile_at(order):
        inside = lax.rem(order, 2) * g + lax.div(order, 2)
        outside = jnp.logical_or(order < 0, order >= 2 * g)
        return tiles[jnp.where(outside, 2 * g, inside)]

    def window(member):
        order = member * 2 + core
        step = flipped(m, member, g)
        here = jnp.concatenate([idx_all[member], wing], 1)
        before = jnp.concatenate([tile_at(order - 1), tail], 1)
        after = jnp.concatenate([tile_at(order + 1), tail], 1)
        left = pltpu.roll(before, wide - REACH, 1)
        mid = pltpu.roll(here, REACH, 1)
        right = pltpu.roll(after, REACH + t_dev, 1)
        ext = jnp.where(spot < REACH, left, jnp.where(spot < REACH + t_dev, mid, right))
        for k in range(kcount):
            line = pltpu.roll(ext[k : k + 1], wide - REACH - MAXLAG + offset_ref[k], 1)
            line = jnp.broadcast_to(line, (BASE, wide))
            raw_win[step, k * BASE : (k + 1) * BASE, :] = pltpu.roll(
                line, 0, 1, stride=1, stride_axis=0
            )

    each(0, g - 1, lambda at: window(jnp.where(core == 0, g - 1 - at, at)))

    @pl.when(has_edge)
    def _():
        edge_copy().wait()

    window(jnp.where(core == 0, 0, g - 1))
    each(1, groups, lambda s: z_copy(s).wait())
    stats = zmsg[...]
    for s in range(1, groups):
        stats = stats + zin[s]
    mean = stats[:, 62:63] / total_days
    var = stats[:, 63:64] / total_days - mean * mean
    outer = 1.0 / jnp.sqrt(var + 1e-06)

    def center_window(step):
        for k in range(kcount):
            value = raw_win[step, k * BASE : (k + 1) * BASE, :]
            value = jnp.where(value < NEAR, value - mean[k : k + 1], 0.0).astype(jnp.bfloat16)
            for turn in range(0, ROWS, BASE):
                turned = value if turn == 0 else pltpu.roll(value, turn, 1)
                win[step, k * ROWS + turn : k * ROWS + turn + BASE, :] = turned[:, :lanes]

    low = lax.broadcasted_iota(jnp.int32, (ROWS, 128), 1) < 64
    low_row = lax.broadcasted_iota(jnp.int32, (1, 128), 1) < 64

    def pair_cols(cols, k):
        return jnp.where(low, cols[0:ROWS, k : k + 1], cols[0:ROWS, k + half_k : k + half_k + 1])

    def halves(first_half, second_half, is_low):
        turned_first = pltpu.roll(first_half, 64, 1)
        turned_second = pltpu.roll(second_half, 64, 1)
        zeroth = jnp.where(is_low, first_half, turned_second)
        oneth = jnp.where(is_low, turned_first, second_half)
        return jnp.where(core == 0, zeroth, oneth), jnp.where(core == 0, oneth, zeroth)

    group_days = 2 * g * t_dev * 1.0
    sums_at = 2 * count

    def add(pieces, step, first_time):
        width = 128 * len(pieces)
        value = jnp.concatenate([recv[piece, step] for piece in pieces], 1)
        wide_value = value.astype(f32)
        sums = jnp.sum(wide_value, 0, keepdims=True)
        squares = jnp.sum(wide_value * wide_value, 0, keepdims=True)
        found = jnp.dot(win[step, :, :t_dev], value, preferred_element_type=f32)
        if first_time:
            acc[0:sums_at, :width] = found
            acc[sums_at : sums_at + 1, :width] = sums
            acc[sums_at + 1 : sums_at + 2, :width] = squares
        else:
            acc[0:sums_at, :width] += found
            acc[sums_at : sums_at + 1, :width] += sums
            acc[sums_at + 1 : sums_at + 2, :width] += squares

    def split(piece, column):
        column = slice(column * 128, column * 128 + 128)
        for k in range(half_k):
            at = k * ROWS
            kept, given = halves(
                acc[at : at + ROWS, column], acc[count + at : count + at + ROWS, column], low
            )
            mine[piece, at : at + ROWS, :] = kept
            other[piece, at : at + ROWS, :] = given
        for row in range(2):
            value = acc[sums_at + row : sums_at + row + 1, column]
            kept, given = halves(value, value, low_row)
            mine[piece, count + row : count + row + 1, :] = kept
            other[piece, count + row : count + row + 1, :] = given
        swap_copy(piece).start()

    def products(piece):
        own_copy(piece).wait()
        add([piece], 0, True)

        def body(step, carry):
            raw_copy(piece, step).wait()
            add([piece], step, False)
            return carry

        lax.fori_loop(1, g, body, 0)
        split(piece, 0)

    def joined(piece, k):
        at = k * ROWS
        return mine[piece, at : at + ROWS, :] + partner_in[piece, at : at + ROWS, :]

    def joined_row(piece, row):
        at = count + row
        return mine[piece, at : at + 1, :] + partner_in[piece, at : at + 1, :]

    def decoded(slot, k):
        coded = got[slot, k * ROWS : (k + 1) * ROWS, :].astype(jnp.int32).astype(f32)
        return coded * (got_extra[slot, 2 + k : 3 + k, :] * (1.0 / TOP))

    def send_sums(piece, with_outer):
        sx, sq = joined_row(piece, 0), joined_row(piece, 1)
        tot, cols, days = own_tot, own_cols, group_days
        if with_outer:
            arrived(piece)
            outer_x = got_extra[piece, 0:1, :]
            outer_mean = outer_x / group_days
            sx, sq = sx + outer_x, sq + got_extra[piece, 1:2, :]
            outer_tot = got_extra[piece, EXTRA:, :]
            outer_cols = jnp.transpose(outer_tot)
            tot, cols, days = tot + outer_tot, cols + outer_cols, 2 * group_days
        sent_extra[piece, 0:1, :] = sx
        sent_extra[piece, 1:2, :] = sq
        local_mean = sx / days
        for k in range(half_k):
            value = joined(piece, k) - local_mean * pair_cols(cols, k)
            if with_outer:
                value = value + decoded(piece, k) + outer_mean * pair_cols(outer_cols, k)
            top = jnp.max(jnp.abs(value), 0, keepdims=True)
            sent_extra[piece, 2 + k : 3 + k, :] = top
            scaled = value * (TOP / jnp.maximum(top, 1e-30))
            sent[piece, k * ROWS : (k + 1) * ROWS, :] = (
                jnp.round(scaled).astype(jnp.int32).astype(jnp.int16)
            )
        sent_extra[piece, EXTRA:, :] = tot
        for copy in sum_copies(piece, slot_of(piece)):
            copy.start()

    def send_outer(piece):
        @pl.when(jnp.logical_not(inner))
        def _():
            send_sums(piece, False)

    def send_inner(piece):
        @pl.when(inner)
        def _():
            send_sums(piece, True)

    last = groups - 1
    own_copy(0).wait()
    each(1, g, lambda s: raw_copy(0, s).wait())

    def early_body(step, first_time):
        center_window(step)
        add([0], step, first_time)

    early_body(0, True)
    if g <= 4:
        for step in range(1, g):
            early_body(step, False)
    else:
        each(1, g, lambda s: early_body(s, False))
    split(0, 0)

    place = lax.broadcasted_iota(jnp.int32, (kcount, lanes), 1)
    day = lax.broadcasted_iota(jnp.int32, (lanes, 128), 0)
    shift = lax.broadcasted_iota(jnp.int32, (lanes, 128), 1) - MAXLAG
    late = jnp.where((day >= t_dev - shift) & (day < t_dev), 1.0, 0.0)
    early = jnp.where(day < -shift, 1.0, 0.0)

    def centered(value, valid):
        return jnp.where(valid, (value - mean).astype(jnp.bfloat16).astype(f32), 0.0)

    def center_body(at, carry):
        return carry + centered(idx_all[at], place < t_dev)

    core_sum = lax.fori_loop(0, g, center_body, jnp.zeros((kcount, lanes), f32))
    inner_block = centered(idx_all[jnp.where(core == 0, 0, g - 1)], place < t_dev)
    edge = jnp.concatenate([tiles[2 * g], tail[:, : lanes - 128]], 1)
    edge = jnp.where(core == 0, pltpu.roll(edge, t_dev - 128, 1), edge)
    opens = jnp.where(core == 0, t_dev - 64, 0)
    closes = jnp.where(core == 0, t_dev, 62)
    outer_block = centered(edge, (place >= opens) & (place < closes) & (edge < NEAR))

    def part(value, sel):
        return jnp.dot(
            value.astype(jnp.bfloat16), sel.astype(jnp.bfloat16), preferred_element_type=f32
        )

    by_shift = (
        jnp.sum(core_sum, 1, keepdims=True)
        + part(outer_block, jnp.where(core == 0, late, early))
        - part(inner_block, jnp.where(core == 0, early, late))
    )
    tot_part[...] = jnp.zeros_like(tot_part)
    for k in range(kcount):
        tot_part[k : k + 1, :] = pltpu.roll(
            by_shift[k : k + 1], lax.rem(128 - offset_ref[k], 128), 1
        )
    total_copy().start()

    total_copy().wait()
    own_tot = tot_part[...] + tot_in[...]
    own_cols = jnp.transpose(own_tot)
    swap_copy(0).wait()
    send_outer(0)
    products(1)
    swap_copy(1).wait()
    send_outer(1)
    send_inner(0)
    products(2)
    swap_copy(2).wait()
    send_sums(2, False)
    send_inner(1)
    products(last)
    sx = jnp.zeros((1, 128), f32)
    sq = jnp.zeros((1, 128), f32)
    all_cols = own_cols
    for slot, days in ((3, 2 * group_days), (2, group_days)):
        arrived(slot)
        far_x = got_extra[slot, 0:1, :]
        sx = sx + far_x
        sq = sq + got_extra[slot, 1:2, :]
        far_mean = far_x / days
        far_cols = jnp.transpose(got_extra[slot, EXTRA:, :])
        all_cols = all_cols + far_cols
        for k in range(half_k):
            at = k * ROWS
            far[at : at + ROWS, :] += decoded(slot, k) + far_mean * pair_cols(far_cols, k)
    for piece in range(last):
        for copy in sum_copies(piece, slot_of(piece)):
            copy.wait_send()
    swap_copy(last).wait()
    sx = sx + joined_row(last, 0)
    sq = sq + joined_row(last, 1)
    mean_x = sx / total_days
    var_x = sq / total_days - mean_x * mean_x
    mask = small[0:1, :]
    mask = mask + pltpu.roll(mask, 64, 1)
    inner = mask / (total_days * jnp.sqrt(var_x + 1e-06))

    def normal(k):
        value = joined(last, k) + far[k * ROWS : (k + 1) * ROWS, :]
        value = value - mean_x * pair_cols(all_cols, k)
        scale = jnp.where(low_row, outer[k : k + 1], outer[k + half_k : k + half_k + 1])
        return value * (inner * scale)

    small_int = lag_ref[...] + MAXLAG
    small[0:1, 0 : lag_ref.shape[1]] = small_int.astype(f32)
    chosen = jnp.broadcast_to(small[0:1, :].astype(jnp.int32), (64, 128))
    kept = lag_ref.shape[1]

    def out_copy(k):
        return pltpu.make_async_copy(out_buf.at[k], out_ref.at[k], out_sem.at[k])

    for k in range(0, half_k, 2):
        upper_rows = normal(k)
        under_rows = normal(k + 1) if k + 1 < half_k else upper_rows
        flat = jnp.transpose(jnp.concatenate([upper_rows, under_rows], 0))
        for side in range(2):
            rows = flat[side * 64 : (side + 1) * 64, :]
            for turn in range(min(2, half_k - k)):
                at = k + turn + side * half_k
                out_buf[at] = jnp.take_along_axis(rows, chosen + 64 * turn, axis=1)[:, :kept]
                out_copy(at).start()
    for k in range(kcount):
        out_copy(k).wait()


def shards(field, index, lag_list, index_offset, sea_mask):
    t_dev, cells_all = field.shape
    devices = lax.axis_size("tm")
    kcount = index.shape[1]
    lanes = round_up(t_dev, 128)
    groups = GROUPS
    g = devices // 2 // groups
    rows = kcount * ROWS
    half = rows // 2
    sizes = (devices, t_dev, kcount, groups, g)
    dma = pltpu.SemaphoreType.DMA
    f32 = jnp.float32
    vmem = pl.BlockSpec(memory_space=pltpu.VMEM)
    maps = pl.pallas_call(
        functools.partial(kernel, sizes),
        out_shape=jax.ShapeDtypeStruct((kcount, 64, lag_list.shape[0]), f32),
        in_specs=[
            pl.BlockSpec(memory_space=pl.ANY),
            vmem,
            vmem,
            pl.BlockSpec(memory_space=pltpu.SMEM),
            vmem,
        ],
        out_specs=pl.BlockSpec(memory_space=pl.ANY),
        scratch_shapes=[
            pltpu.VMEM((t_dev, cells_all), jnp.bfloat16),
            pltpu.VMEM((kcount, lanes), f32),
            pltpu.VMEM((g, kcount, lanes), f32),
            pltpu.VMEM((2 * g + 1, kcount, 128), f32),
            pltpu.VMEM((kcount, 128), f32),
            pltpu.VMEM((groups, kcount, 128), f32),
            pltpu.VMEM((groups, g, t_dev, 128), jnp.bfloat16),
            pltpu.VMEM((g, kcount * BASE, lanes + 128), f32),
            pltpu.VMEM((g, rows, lanes), jnp.bfloat16),
            pltpu.VMEM((rows + EXTRA, 256), f32),
            pltpu.VMEM((groups, half + EXTRA, 128), f32),
            pltpu.VMEM((groups, half + EXTRA, 128), f32),
            pltpu.VMEM((groups, half + EXTRA, 128), f32),
            pltpu.VMEM((groups, half, 128), jnp.int16),
            pltpu.VMEM((groups, EXTRA + 16, 128), f32),
            pltpu.VMEM((groups, half, 128), jnp.int16),
            pltpu.VMEM((groups, EXTRA + 16, 128), f32),
            pltpu.VMEM((half, 128), f32),
            pltpu.VMEM((kcount, 64, lag_list.shape[0]), f32),
            pltpu.VMEM((8, 128), f32),
            pltpu.VMEM((16, 128), f32),
            pltpu.VMEM((16, 128), f32),
            dma((groups, g)),
            dma((groups, g)),
            dma((g,)),
            dma((g,)),
            dma((2, g)),
            dma((2, g)),
            dma((4,)),
            dma((groups,)),
            dma((groups,)),
            dma((groups,)),
            dma((groups,)),
            dma((2, groups)),
            dma((2, groups)),
            dma((groups + 1,)),
            pltpu.SemaphoreType.REGULAR((groups,)),
            dma((kcount,)),
        ],
        compiler_params=pltpu.CompilerParams(
            collective_id=0, has_side_effects=True, vmem_limit_bytes=60 * 1024 * 1024
        ),
    )(field, index.T, lag_list[None, :], index_offset, sea_mask[None, :])
    return jnp.transpose(maps, (1, 0, 2))


def solution(mesh):
    return jax.shard_map(
        shards,
        mesh=mesh,
        in_specs=(P("tm", None), P("tm", None), P(), P(), P("tm")),
        out_specs=P("tm", None, None),
        check_vma=False,
    )
```

```python
import functools

import jax
import jax.numpy as jnp
from jax import lax
from jax.experimental import pallas as pl
from jax.experimental.pallas import tpu as pltpu
from jax.sharding import PartitionSpec as P

MAXLAG = 30
MAXOFF = 14
REACH = 64
ROWS = 64
BASE = 16
EXTRA = 8
TOP = 32767.0
FAR = 1e30
NEAR = 1e29
GROUPS = 4
MESH = pl.DeviceIdType.MESH


def round_up(value, unit):
    return -(-value // unit) * unit


def kernel(
    sizes,
    field_hbm,
    index_ref,
    lag_ref,
    offset_ref,
    mask_ref,
    out_ref,
    field_ref,
    idx_ref,
    idx_all,
    tiles,
    zmsg,
    zin,
    recv,
    raw_win,
    win,
    acc,
    mine,
    other,
    partner_in,
    sent,
    sent_extra,
    got,
    got_extra,
    far,
    out_buf,
    small,
    tot_part,
    tot_in,
    raw_send,
    raw_recv,
    idx_send,
    idx_recv,
    tile_send,
    tile_recv,
    lone_sem,
    z_send,
    z_recv,
    swap_send,
    swap_recv,
    sum_send,
    sum_recv,
    own_sem,
    round_sem,
    out_sem,
):
    devices, t_dev, kcount, groups, g = sizes
    lanes = idx_ref.shape[1]
    wide = lanes + 128
    half_k = kcount // 2
    count = half_k * ROWS
    cells = 128
    me = lax.axis_index("tm")
    core = lax.rem(me, 2)
    chip = lax.div(me, 2)
    h = lax.div(chip, g)
    m = lax.rem(chip, g)
    partner = chip * 2 + (1 - core)
    edge_peer = ((h + 2 * core - 1) * g + m) * 2 + (1 - core)
    has_edge = jnp.where(core == 0, h > 0, h < groups - 1)
    f32 = jnp.float32
    total_days = devices * t_dev * 1.0

    def flipped(value, step, size):
        found, bit = 0, 1
        while bit < size:
            flip = lax.rem(lax.div(value, bit) + lax.div(step, bit), 2)
            found, bit = found + flip * bit, bit * 2
        return found

    def across(step):
        return flipped(m, step, g)

    def device_of(group, member):
        return (group * g + member) * 2 + core

    def remote(src, dst, send, recv_s, device):
        return pltpu.make_async_remote_copy(
            src_ref=src,
            dst_ref=dst,
            send_sem=send,
            recv_sem=recv_s,
            device_id=(device,),
            device_id_type=MESH,
        )

    def block(at):
        return field_ref.at[:, pl.ds(pl.multiple_of(at * cells, cells), cells)]

    inner = jnp.logical_or(h == 1, h == 2)
    upper = lax.div(h, 2)
    beside_h = h + 1 - 2 * lax.rem(h, 2)

    def plane_of(piece):
        if piece == 0:
            return (groups - 1) * (1 - upper)
        if piece == 1:
            return jnp.where(inner, beside_h, 2 - upper)
        return jnp.where(inner, 2 - upper, beside_h) if piece == 2 else h

    def raw_copy(piece, step):
        to = across(step)
        return remote(
            block(plane_of(piece) * g + to),
            recv.at[piece, step],
            raw_send.at[piece, step],
            raw_recv.at[piece, step],
            device_of(h, to),
        )

    def own_copy(piece):
        return pltpu.make_async_copy(
            block(plane_of(piece) * g + m), recv.at[piece, 0], own_sem.at[piece]
        )

    def idx_copy(step):
        return remote(
            idx_ref,
            idx_all.at[m],
            idx_send.at[step],
            idx_recv.at[step],
            device_of(h, across(step)),
        )

    def tile_copy(side, step):
        to = (h * g + across(step)) * 2 + (core if side == 0 else 1 - core)
        tile = tiles.at[core * g + m]
        return remote(
            tile, tile, tile_send.at[side, step], tile_recv.at[side, step], to
        )

    def edge_copy():
        return remote(
            tiles.at[jnp.where(core == 0, 0, 2 * g - 1)],
            tiles.at[2 * g],
            lone_sem.at[0],
            lone_sem.at[1],
            edge_peer,
        )

    def total_copy():
        return remote(tot_part, tot_in, lone_sem.at[2], lone_sem.at[3], partner)

    def z_copy(step):
        return remote(
            zmsg,
            zin.at[step],
            z_send.at[step],
            z_recv.at[step],
            device_of(flipped(h, step, groups), m),
        )

    def swap_copy(piece):
        return remote(
            other.at[piece],
            partner_in.at[piece],
            swap_send.at[piece],
            swap_recv.at[piece],
            partner,
        )

    def slot_of(piece):
        return jnp.where(inner, (3, 2, 3)[piece], piece)

    def receiver(piece):
        if piece == 1:
            return device_of(beside_h, m)
        return device_of(jnp.where(inner, plane_of(piece), beside_h), m)

    def sum_copies(piece, slot):
        return [
            remote(
                sent.at[piece],
                got.at[slot],
                sum_send.at[0, piece],
                sum_recv.at[0, slot],
                receiver(piece),
            ),
            remote(
                sent_extra.at[piece],
                got_extra.at[slot],
                sum_send.at[1, piece],
                sum_recv.at[1, slot],
                receiver(piece),
            ),
        ]

    def arrived(slot):
        for copy in sum_copies(1, slot):
            copy.wait_recv()

    def each(low_step, high_step, act):
        def body(step, carry):
            act(step)
            return carry

        lax.fori_loop(low_step, high_step, body, 0)

    load = pltpu.make_async_copy(field_hbm, field_ref, own_sem.at[groups])
    load.start()
    barrier = pltpu.get_barrier_semaphore()

    def tell(sem, device):
        pl.semaphore_signal(sem, inc=1, device_id=(device,), device_id_type=MESH)

    def tell_line(sem):
        @pl.when(h > 0)
        def _():
            tell(sem, device_of(h - 1, m))

        @pl.when(h < groups - 1)
        def _():
            tell(sem, device_of(h + 1, m))

    beside = jnp.where(h > 0, 1, 0) + jnp.where(h < groups - 1, 1, 0)
    tell_line(barrier)

    @pl.when(has_edge)
    def _():
        tell(barrier, edge_peer)

    each(1, 2 * g, lambda s: tell(barrier, (h * g + across(lax.div(s, 2))) * 2 + lax.rem(core + s, 2)))
    idx_ref[...] = jnp.zeros_like(idx_ref)
    idx_ref[0:kcount, 0:t_dev] = index_ref[...]
    lane = lax.broadcasted_iota(jnp.int32, (kcount, 128), 1)
    series = idx_ref[...]
    tile = jnp.where(
        lane < 64, series[:, :128], pltpu.roll(series, (128 - t_dev) % lanes, 1)[:, :128]
    )
    tile = jnp.where(lane == 62, jnp.sum(series, 1, keepdims=True), tile)
    tile = jnp.where(lane == 63, jnp.sum(series * series, 1, keepdims=True), tile)
    tiles[core * g + m] = tile
    idx_all[m] = series
    other[...] = jnp.zeros_like(other)
    far[...] = jnp.zeros_like(far)
    sent_extra[...] = jnp.zeros_like(sent_extra)
    small[...] = jnp.zeros_like(small)
    small[0:1, 0 : cells // 2] = mask_ref[...].astype(f32)

    @pl.when(jnp.logical_not(has_edge))
    def _():
        tiles[2 * g] = jnp.full((kcount, 128), FAR, f32)

    pl.semaphore_wait(barrier, 2 * g - 1 + beside + jnp.where(has_edge, 1, 0))

    for side in range(2):
        each(1 - side, g, lambda s, side=side: tile_copy(side, s).start())
    each(1, g, lambda s: idx_copy(s).start())
    load.wait()
    for piece in range(groups):
        own_copy(piece).start()
        each(1, g, lambda s, piece=piece: raw_copy(piece, s).start())
    for turn in range(groups - 2):
        tell_line(round_sem.at[turn])
        pl.semaphore_wait(round_sem.at[turn], beside)
    for side in range(2):
        each(1 - side, g, lambda s, side=side: tile_copy(side, s).wait())

    @pl.when(has_edge)
    def _():
        edge_copy().start()

    zero_tile = jnp.zeros((kcount, 128), f32)
    zmsg[...] = lax.fori_loop(0, 2 * g, lambda at, carry: carry + tiles[at], zero_tile)
    each(1, groups, lambda s: z_copy(s).start())
    each(1, g, lambda s: idx_copy(s).wait())

    spot = lax.broadcasted_iota(jnp.int32, (kcount, wide), 1)
    wing = jnp.zeros((kcount, 128), f32)
    tail = jnp.zeros((kcount, wide - 128), f32)

    def tile_at(order):
        inside = lax.rem(order, 2) * g + lax.div(order, 2)
        outside = jnp.logical_or(order < 0, order >= 2 * g)
        return tiles[jnp.where(outside, 2 * g, inside)]

    def window(member):
        order = member * 2 + core
        step = flipped(m, member, g)
        here = jnp.concatenate([idx_all[member], wing], 1)
        before = jnp.concatenate([tile_at(order - 1), tail], 1)
        after = jnp.concatenate([tile_at(order + 1), tail], 1)
        left = pltpu.roll(before, wide - REACH, 1)
        mid = pltpu.roll(here, REACH, 1)
        right = pltpu.roll(after, REACH + t_dev, 1)
        ext = jnp.where(spot < REACH, left, jnp.where(spot < REACH + t_dev, mid, right))
        for k in range(kcount):
            line = pltpu.roll(ext[k : k + 1], wide - REACH - MAXLAG + offset_ref[k], 1)
            line = jnp.broadcast_to(line, (BASE, wide))
            raw_win[step, k * BASE : (k + 1) * BASE, :] = pltpu.roll(
                line, 0, 1, stride=1, stride_axis=0
            )

    each(0, g - 1, lambda at: window(jnp.where(core == 0, g - 1 - at, at)))

    @pl.when(has_edge)
    def _():
        edge_copy().wait()

    window(jnp.where(core == 0, 0, g - 1))
    each(1, groups, lambda s: z_copy(s).wait())
    stats = zmsg[...]
    for s in range(1, groups):
        stats = stats + zin[s]
    mean = stats[:, 62:63] / total_days
    var = stats[:, 63:64] / total_days - mean * mean
    outer = 1.0 / jnp.sqrt(var + 1e-06)

    place = lax.broadcasted_iota(jnp.int32, (kcount, lanes), 1)
    day = lax.broadcasted_iota(jnp.int32, (lanes, 128), 0)
    shift = lax.broadcasted_iota(jnp.int32, (lanes, 128), 1) - MAXLAG
    late = jnp.where((day >= t_dev - shift) & (day < t_dev), 1.0, 0.0)
    early = jnp.where(day < -shift, 1.0, 0.0)

    def centered(value, valid):
        return jnp.where(valid, (value - mean).astype(jnp.bfloat16).astype(f32), 0.0)

    def center_body(at, carry):
        return carry + centered(idx_all[at], place < t_dev)

    core_sum = lax.fori_loop(0, g, center_body, jnp.zeros((kcount, lanes), f32))
    inner_block = centered(idx_all[jnp.where(core == 0, 0, g - 1)], place < t_dev)
    edge = jnp.concatenate([tiles[2 * g], tail[:, : lanes - 128]], 1)
    edge = jnp.where(core == 0, pltpu.roll(edge, t_dev - 128, 1), edge)
    opens = jnp.where(core == 0, t_dev - 64, 0)
    closes = jnp.where(core == 0, t_dev, 62)
    outer_block = centered(edge, (place >= opens) & (place < closes) & (edge < NEAR))

    def part(value, sel):
        return jnp.dot(
            value.astype(jnp.bfloat16), sel.astype(jnp.bfloat16), preferred_element_type=f32
        )

    by_shift = (
        jnp.sum(core_sum, 1, keepdims=True)
        + part(outer_block, jnp.where(core == 0, late, early))
        - part(inner_block, jnp.where(core == 0, early, late))
    )
    tot_part[...] = jnp.zeros_like(tot_part)
    for k in range(kcount):
        tot_part[k : k + 1, :] = pltpu.roll(
            by_shift[k : k + 1], lax.rem(128 - offset_ref[k], 128), 1
        )
    total_copy().start()

    def center_window(step):
        for k in range(kcount):
            value = raw_win[step, k * BASE : (k + 1) * BASE, :]
            value = jnp.where(value < NEAR, value - mean[k : k + 1], 0.0).astype(jnp.bfloat16)
            for turn in range(0, ROWS, BASE):
                turned = value if turn == 0 else pltpu.roll(value, turn, 1)
                win[step, k * ROWS + turn : k * ROWS + turn + BASE, :] = turned[:, :lanes]

    low = lax.broadcasted_iota(jnp.int32, (ROWS, 128), 1) < 64
    low_row = lax.broadcasted_iota(jnp.int32, (1, 128), 1) < 64

    def pair_cols(cols, k):
        return jnp.where(low, cols[0:ROWS, k : k + 1], cols[0:ROWS, k + half_k : k + half_k + 1])

    def halves(first_half, second_half, is_low):
        turned_first = pltpu.roll(first_half, 64, 1)
        turned_second = pltpu.roll(second_half, 64, 1)
        zeroth = jnp.where(is_low, first_half, turned_second)
        oneth = jnp.where(is_low, turned_first, second_half)
        return jnp.where(core == 0, zeroth, oneth), jnp.where(core == 0, oneth, zeroth)

    group_days = 2 * g * t_dev * 1.0
    sums_at = 2 * count

    def add(pieces, step, first_time):
        width = 128 * len(pieces)
        value = jnp.concatenate([recv[piece, step] for piece in pieces], 1)
        wide_value = value.astype(f32)
        sums = jnp.sum(wide_value, 0, keepdims=True)
        squares = jnp.sum(wide_value * wide_value, 0, keepdims=True)
        found = jnp.dot(win[step, :, :t_dev], value, preferred_element_type=f32)
        if first_time:
            acc[0:sums_at, :width] = found
            acc[sums_at : sums_at + 1, :width] = sums
            acc[sums_at + 1 : sums_at + 2, :width] = squares
        else:
            acc[0:sums_at, :width] += found
            acc[sums_at : sums_at + 1, :width] += sums
            acc[sums_at + 1 : sums_at + 2, :width] += squares

    def split(piece, column):
        column = slice(column * 128, column * 128 + 128)
        for k in range(half_k):
            at = k * ROWS
            kept, given = halves(
                acc[at : at + ROWS, column], acc[count + at : count + at + ROWS, column], low
            )
            mine[piece, at : at + ROWS, :] = kept
            other[piece, at : at + ROWS, :] = given
        for row in range(2):
            value = acc[sums_at + row : sums_at + row + 1, column]
            kept, given = halves(value, value, low_row)
            mine[piece, count + row : count + row + 1, :] = kept
            other[piece, count + row : count + row + 1, :] = given
        swap_copy(piece).start()

    def products(piece):
        own_copy(piece).wait()
        add([piece], 0, True)

        def body(step, carry):
            raw_copy(piece, step).wait()
            add([piece], step, False)
            return carry

        lax.fori_loop(1, g, body, 0)
        split(piece, 0)

    def joined(piece, k):
        at = k * ROWS
        return mine[piece, at : at + ROWS, :] + partner_in[piece, at : at + ROWS, :]

    def joined_row(piece, row):
        at = count + row
        return mine[piece, at : at + 1, :] + partner_in[piece, at : at + 1, :]

    def decoded(slot, k):
        coded = got[slot, k * ROWS : (k + 1) * ROWS, :].astype(jnp.int32).astype(f32)
        return coded * (got_extra[slot, 2 + k : 3 + k, :] * (1.0 / TOP))

    def send_sums(piece, outer_slot):
        sx, sq = joined_row(piece, 0), joined_row(piece, 1)
        tot, cols, days = own_tot, own_cols, group_days
        if outer_slot is not None:
            arrived(outer_slot)
            outer_x = got_extra[outer_slot, 0:1, :]
            outer_mean = outer_x / group_days
            sx, sq = sx + outer_x, sq + got_extra[outer_slot, 1:2, :]
            outer_tot = got_extra[outer_slot, EXTRA:, :]
            outer_cols = jnp.transpose(outer_tot)
            tot, cols, days = tot + outer_tot, cols + outer_cols, 2 * group_days
        sent_extra[piece, 0:1, :] = sx
        sent_extra[piece, 1:2, :] = sq
        local_mean = sx / days
        for k in range(half_k):
            value = joined(piece, k) - local_mean * pair_cols(cols, k)
            if outer_slot is not None:
                value = value + decoded(outer_slot, k) + outer_mean * pair_cols(outer_cols, k)
            top = jnp.max(jnp.abs(value), 0, keepdims=True)
            sent_extra[piece, 2 + k : 3 + k, :] = top
            scaled = value * (TOP / jnp.maximum(top, 1e-30))
            sent[piece, k * ROWS : (k + 1) * ROWS, :] = (
                jnp.round(scaled).astype(jnp.int32).astype(jnp.int16)
            )
        sent_extra[piece, EXTRA:, :] = tot
        for copy in sum_copies(piece, slot_of(piece)):
            copy.start()

    def send_outer(piece):
        @pl.when(jnp.logical_not(inner))
        def _():
            send_sums(piece, None)

    def send_inner(piece, outer_slot):
        @pl.when(inner)
        def _():
            send_sums(piece, outer_slot)

    last = groups - 1
    own_copy(0).wait()
    each(1, g, lambda s: raw_copy(0, s).wait())

    def early_body(step, first_time):
        center_window(step)
        add([0], step, first_time)

    early_body(0, True)
    if g <= 4:
        for step in range(1, g):
            early_body(step, False)
    else:
        each(1, g, lambda s: early_body(s, False))
    split(0, 0)

    total_copy().wait()
    own_tot = tot_part[...] + tot_in[...]
    own_cols = jnp.transpose(own_tot)
    swap_copy(0).wait()
    send_outer(0)
    products(1)
    swap_copy(1).wait()
    send_sums(1, None)
    products(2)
    send_inner(0, 0)
    swap_copy(2).wait()
    send_outer(2)
    send_inner(2, 1)
    products(last)
    sx = jnp.zeros((1, 128), f32)
    sq = jnp.zeros((1, 128), f32)
    all_cols = own_cols
    for slot, days in ((3, 2 * group_days), (2, group_days)):
        arrived(slot)
        far_x = got_extra[slot, 0:1, :]
        sx = sx + far_x
        sq = sq + got_extra[slot, 1:2, :]
        far_mean = far_x / days
        far_cols = jnp.transpose(got_extra[slot, EXTRA:, :])
        all_cols = all_cols + far_cols
        for k in range(half_k):
            at = k * ROWS
            far[at : at + ROWS, :] += decoded(slot, k) + far_mean * pair_cols(far_cols, k)
    for piece in range(last):
        for copy in sum_copies(piece, slot_of(piece)):
            copy.wait_send()
    swap_copy(last).wait()
    sx = sx + joined_row(last, 0)
    sq = sq + joined_row(last, 1)
    mean_x = sx / total_days
    var_x = sq / total_days - mean_x * mean_x
    mask = small[0:1, :]
    mask = mask + pltpu.roll(mask, 64, 1)
    inner = mask / (total_days * jnp.sqrt(var_x + 1e-06))

    def normal(k):
        value = joined(last, k) + far[k * ROWS : (k + 1) * ROWS, :]
        value = value - mean_x * pair_cols(all_cols, k)
        scale = jnp.where(low_row, outer[k : k + 1], outer[k + half_k : k + half_k + 1])
        return value * (inner * scale)

    small_int = lag_ref[...] + MAXLAG
    small[0:1, 0 : lag_ref.shape[1]] = small_int.astype(f32)
    chosen = jnp.broadcast_to(small[0:1, :].astype(jnp.int32), (64, 128))
    kept = lag_ref.shape[1]

    def out_copy(k):
        return pltpu.make_async_copy(out_buf.at[k], out_ref.at[k], out_sem.at[k])

    for k in range(0, half_k, 2):
        upper_rows = normal(k)
        under_rows = normal(k + 1) if k + 1 < half_k else upper_rows
        flat = jnp.transpose(jnp.concatenate([upper_rows, under_rows], 0))
        for side in range(2):
            rows = flat[side * 64 : (side + 1) * 64, :]
            for turn in range(min(2, half_k - k)):
                at = k + turn + side * half_k
                out_buf[at] = jnp.take_along_axis(rows, chosen + 64 * turn, axis=1)[:, :kept]
                out_copy(at).start()
    for k in range(kcount):
        out_copy(k).wait()


def shards(field, index, lag_list, index_offset, sea_mask):
    t_dev, cells_all = field.shape
    devices = lax.axis_size("tm")
    kcount = index.shape[1]
    lanes = round_up(t_dev, 128)
    groups = GROUPS
    g = devices // 2 // groups
    rows = kcount * ROWS
    half = rows // 2
    sizes = (devices, t_dev, kcount, groups, g)
    dma = pltpu.SemaphoreType.DMA
    f32 = jnp.float32
    vmem = pl.BlockSpec(memory_space=pltpu.VMEM)
    maps = pl.pallas_call(
        functools.partial(kernel, sizes),
        out_shape=jax.ShapeDtypeStruct((kcount, 64, lag_list.shape[0]), f32),
        in_specs=[
            pl.BlockSpec(memory_space=pl.ANY),
            vmem,
            vmem,
            pl.BlockSpec(memory_space=pltpu.SMEM),
            vmem,
        ],
        out_specs=pl.BlockSpec(memory_space=pl.ANY),
        scratch_shapes=[
            pltpu.VMEM((t_dev, cells_all), jnp.bfloat16),
            pltpu.VMEM((kcount, lanes), f32),
            pltpu.VMEM((g, kcount, lanes), f32),
            pltpu.VMEM((2 * g + 1, kcount, 128), f32),
            pltpu.VMEM((kcount, 128), f32),
            pltpu.VMEM((groups, kcount, 128), f32),
            pltpu.VMEM((groups, g, t_dev, 128), jnp.bfloat16),
            pltpu.VMEM((g, kcount * BASE, lanes + 128), f32),
            pltpu.VMEM((g, rows, lanes), jnp.bfloat16),
            pltpu.VMEM((rows + EXTRA, 256), f32),
            pltpu.VMEM((groups, half + EXTRA, 128), f32),
            pltpu.VMEM((groups, half + EXTRA, 128), f32),
            pltpu.VMEM((groups, half + EXTRA, 128), f32),
            pltpu.VMEM((groups, half, 128), jnp.int16),
            pltpu.VMEM((groups, EXTRA + 16, 128), f32),
            pltpu.VMEM((groups, half, 128), jnp.int16),
            pltpu.VMEM((groups, EXTRA + 16, 128), f32),
            pltpu.VMEM((half, 128), f32),
            pltpu.VMEM((kcount, 64, lag_list.shape[0]), f32),
            pltpu.VMEM((8, 128), f32),
            pltpu.VMEM((16, 128), f32),
            pltpu.VMEM((16, 128), f32),
            dma((groups, g)),
            dma((groups, g)),
            dma((g,)),
            dma((g,)),
            dma((2, g)),
            dma((2, g)),
            dma((4,)),
            dma((groups,)),
            dma((groups,)),
            dma((groups,)),
            dma((groups,)),
            dma((2, groups)),
            dma((2, groups)),
            dma((groups + 1,)),
            pltpu.SemaphoreType.REGULAR((groups,)),
            dma((kcount,)),
        ],
        compiler_params=pltpu.CompilerParams(
            collective_id=0, has_side_effects=True, vmem_limit_bytes=60 * 1024 * 1024
        ),
    )(field, index.T, lag_list[None, :], index_offset, sea_mask[None, :])
    return jnp.transpose(maps, (1, 0, 2))


def solution(mesh):
    return jax.shard_map(
        shards,
        mesh=mesh,
        in_specs=(P("tm", None), P("tm", None), P(), P(), P("tm")),
        out_specs=P("tm", None, None),
        check_vma=False,
    )
```

```python
import functools

import jax
import jax.numpy as jnp
from jax import lax
from jax.experimental import pallas as pl
from jax.experimental.pallas import tpu as pltpu
from jax.sharding import PartitionSpec as P

MAXLAG = 30
MAXOFF = 14
REACH = 64
ROWS = 64
BASE = 16
EXTRA = 8
TOP = 32767.0
FAR = 1e30
NEAR = 1e29
GROUPS = 4
MESH = pl.DeviceIdType.MESH


def round_up(value, unit):
    return -(-value // unit) * unit


def kernel(
    sizes,
    field_hbm,
    index_ref,
    lag_ref,
    offset_ref,
    mask_ref,
    out_ref,
    field_ref,
    idx_ref,
    idx_all,
    tiles,
    zmsg,
    zin,
    recv,
    raw_win,
    win,
    acc,
    mine,
    other,
    partner_in,
    sent,
    sent_extra,
    got,
    got_extra,
    far,
    stage,
    out_buf,
    small,
    tot_part,
    tot_in,
    raw_send,
    raw_recv,
    idx_send,
    idx_recv,
    tile_send,
    tile_recv,
    lone_sem,
    z_send,
    z_recv,
    swap_send,
    swap_recv,
    sum_send,
    sum_recv,
    own_sem,
    round_sem,
    out_sem,
):
    devices, t_dev, kcount, groups, g = sizes
    lanes = idx_ref.shape[1]
    wide = lanes + 128
    half_k = kcount // 2
    count = half_k * ROWS
    cells = 128
    me = lax.axis_index("tm")
    core = lax.rem(me, 2)
    chip = lax.div(me, 2)
    h = lax.div(chip, g)
    m = lax.rem(chip, g)
    partner = chip * 2 + (1 - core)
    edge_peer = ((h + 2 * core - 1) * g + m) * 2 + (1 - core)
    has_edge = jnp.where(core == 0, h > 0, h < groups - 1)
    f32 = jnp.float32
    total_days = devices * t_dev * 1.0

    def flipped(value, step, size):
        found, bit = 0, 1
        while bit < size:
            flip = lax.rem(lax.div(value, bit) + lax.div(step, bit), 2)
            found, bit = found + flip * bit, bit * 2
        return found

    def across(step):
        return flipped(m, step, g)

    def device_of(group, member):
        return (group * g + member) * 2 + core

    def remote(src, dst, send, recv_s, device):
        return pltpu.make_async_remote_copy(
            src_ref=src,
            dst_ref=dst,
            send_sem=send,
            recv_sem=recv_s,
            device_id=(device,),
            device_id_type=MESH,
        )

    def block(at):
        return field_ref.at[:, pl.ds(pl.multiple_of(at * cells, cells), cells)]

    inner = jnp.logical_or(h == 1, h == 2)
    upper = lax.div(h, 2)
    beside_h = h + 1 - 2 * lax.rem(h, 2)

    def plane_of(piece):
        if piece == 0:
            return (groups - 1) * (1 - upper)
        if piece == 1:
            return jnp.where(inner, beside_h, 2 - upper)
        return jnp.where(inner, 2 - upper, beside_h) if piece == 2 else h

    def raw_copy(piece, step):
        to = across(step)
        return remote(
            block(plane_of(piece) * g + to),
            recv.at[piece, step],
            raw_send.at[piece, step],
            raw_recv.at[piece, step],
            device_of(h, to),
        )

    def own_copy(piece):
        return pltpu.make_async_copy(
            block(plane_of(piece) * g + m), recv.at[piece, 0], own_sem.at[piece]
        )

    def idx_copy(step):
        return remote(
            idx_ref,
            idx_all.at[m],
            idx_send.at[step],
            idx_recv.at[step],
            device_of(h, across(step)),
        )

    def tile_copy(side, step):
        to = (h * g + across(step)) * 2 + (core if side == 0 else 1 - core)
        tile = tiles.at[core * g + m]
        return remote(
            tile, tile, tile_send.at[side, step], tile_recv.at[side, step], to
        )

    def edge_copy():
        return remote(
            tiles.at[jnp.where(core == 0, 0, 2 * g - 1)],
            tiles.at[2 * g],
            lone_sem.at[0],
            lone_sem.at[1],
            edge_peer,
        )

    def total_copy():
        return remote(tot_part, tot_in, lone_sem.at[2], lone_sem.at[3], partner)

    def z_copy(step):
        return remote(
            zmsg,
            zin.at[step],
            z_send.at[step],
            z_recv.at[step],
            device_of(flipped(h, step, groups), m),
        )

    def swap_copy(piece):
        return remote(
            other.at[piece],
            partner_in.at[piece],
            swap_send.at[piece],
            swap_recv.at[piece],
            partner,
        )

    def slot_of(piece):
        return jnp.where(inner, (3, 2, 3)[piece], piece)

    def receiver(piece):
        if piece == 1:
            return device_of(beside_h, m)
        return device_of(jnp.where(inner, plane_of(piece), beside_h), m)

    def sum_copies(piece, slot):
        copies = [
            remote(
                sent_extra.at[piece],
                got_extra.at[slot],
                sum_send.at[half_k, piece],
                sum_recv.at[half_k, slot],
                receiver(piece),
            )
        ]
        for k in range(half_k):
            rows = pl.ds(k * ROWS, ROWS)
            copies.append(
                remote(
                    sent.at[piece, rows],
                    got.at[slot, rows],
                    sum_send.at[k, piece],
                    sum_recv.at[k, slot],
                    receiver(piece),
                )
            )
        return copies

    def each(low_step, high_step, act):
        def body(step, carry):
            act(step)
            return carry

        lax.fori_loop(low_step, high_step, body, 0)

    load = pltpu.make_async_copy(field_hbm, field_ref, own_sem.at[groups])
    load.start()
    barrier = pltpu.get_barrier_semaphore()

    def tell(sem, device):
        pl.semaphore_signal(sem, inc=1, device_id=(device,), device_id_type=MESH)

    def tell_line(sem):
        @pl.when(h > 0)
        def _():
            tell(sem, device_of(h - 1, m))

        @pl.when(h < groups - 1)
        def _():
            tell(sem, device_of(h + 1, m))

    beside = jnp.where(h > 0, 1, 0) + jnp.where(h < groups - 1, 1, 0)
    tell_line(barrier)

    @pl.when(has_edge)
    def _():
        tell(barrier, edge_peer)

    each(1, 2 * g, lambda s: tell(barrier, (h * g + across(lax.div(s, 2))) * 2 + lax.rem(core + s, 2)))
    idx_ref[...] = jnp.zeros_like(idx_ref)
    idx_ref[0:kcount, 0:t_dev] = index_ref[...]
    lane = lax.broadcasted_iota(jnp.int32, (kcount, 128), 1)
    series = idx_ref[...]
    tile = jnp.where(
        lane < 64, series[:, :128], pltpu.roll(series, (128 - t_dev) % lanes, 1)[:, :128]
    )
    tile = jnp.where(lane == 62, jnp.sum(series, 1, keepdims=True), tile)
    tile = jnp.where(lane == 63, jnp.sum(series * series, 1, keepdims=True), tile)
    tiles[core * g + m] = tile
    idx_all[m] = series
    other[...] = jnp.zeros_like(other)
    sent_extra[...] = jnp.zeros_like(sent_extra)
    small[...] = jnp.zeros_like(small)
    small[0:1, 0 : cells // 2] = mask_ref[...].astype(f32)

    @pl.when(jnp.logical_not(has_edge))
    def _():
        tiles[2 * g] = jnp.full((kcount, 128), FAR, f32)

    pl.semaphore_wait(barrier, 2 * g - 1 + beside + jnp.where(has_edge, 1, 0))

    for side in range(2):
        each(1 - side, g, lambda s, side=side: tile_copy(side, s).start())
    each(1, g, lambda s: idx_copy(s).start())
    load.wait()
    for piece in range(groups):
        own_copy(piece).start()
        each(1, g, lambda s, piece=piece: raw_copy(piece, s).start())
    for turn in range(groups - 2):
        tell_line(round_sem.at[turn])
        pl.semaphore_wait(round_sem.at[turn], beside)
    for side in range(2):
        each(1 - side, g, lambda s, side=side: tile_copy(side, s).wait())

    @pl.when(has_edge)
    def _():
        edge_copy().start()

    zero_tile = jnp.zeros((kcount, 128), f32)
    zmsg[...] = lax.fori_loop(0, 2 * g, lambda at, carry: carry + tiles[at], zero_tile)
    each(1, groups, lambda s: z_copy(s).start())
    each(1, g, lambda s: idx_copy(s).wait())

    spot = lax.broadcasted_iota(jnp.int32, (kcount, wide), 1)
    wing = jnp.zeros((kcount, 128), f32)
    tail = jnp.zeros((kcount, wide - 128), f32)

    def tile_at(order):
        inside = lax.rem(order, 2) * g + lax.div(order, 2)
        outside = jnp.logical_or(order < 0, order >= 2 * g)
        return tiles[jnp.where(outside, 2 * g, inside)]

    def window(member):
        order = member * 2 + core
        step = flipped(m, member, g)
        here = jnp.concatenate([idx_all[member], wing], 1)
        before = jnp.concatenate([tile_at(order - 1), tail], 1)
        after = jnp.concatenate([tile_at(order + 1), tail], 1)
        left = pltpu.roll(before, wide - REACH, 1)
        mid = pltpu.roll(here, REACH, 1)
        right = pltpu.roll(after, REACH + t_dev, 1)
        ext = jnp.where(spot < REACH, left, jnp.where(spot < REACH + t_dev, mid, right))
        for k in range(kcount):
            line = pltpu.roll(ext[k : k + 1], wide - REACH - MAXLAG + offset_ref[k], 1)
            line = jnp.broadcast_to(line, (BASE, wide))
            raw_win[step, k * BASE : (k + 1) * BASE, :] = pltpu.roll(
                line, 0, 1, stride=1, stride_axis=0
            )

    each(0, g - 1, lambda at: window(jnp.where(core == 0, g - 1 - at, at)))

    @pl.when(has_edge)
    def _():
        edge_copy().wait()

    window(jnp.where(core == 0, 0, g - 1))
    each(1, groups, lambda s: z_copy(s).wait())
    stats = zmsg[...]
    for s in range(1, groups):
        stats = stats + zin[s]
    mean = stats[:, 62:63] / total_days
    var = stats[:, 63:64] / total_days - mean * mean
    outer = 1.0 / jnp.sqrt(var + 1e-06)

    place = lax.broadcasted_iota(jnp.int32, (kcount, lanes), 1)
    day = lax.broadcasted_iota(jnp.int32, (lanes, 128), 0)
    shift = lax.broadcasted_iota(jnp.int32, (lanes, 128), 1) - MAXLAG
    late = jnp.where((day >= t_dev - shift) & (day < t_dev), 1.0, 0.0)
    early = jnp.where(day < -shift, 1.0, 0.0)

    def centered(value, valid):
        return jnp.where(valid, (value - mean).astype(jnp.bfloat16).astype(f32), 0.0)

    def center_body(at, carry):
        return carry + centered(idx_all[at], place < t_dev)

    core_sum = lax.fori_loop(0, g, center_body, jnp.zeros((kcount, lanes), f32))
    inner_block = centered(idx_all[jnp.where(core == 0, 0, g - 1)], place < t_dev)
    edge = jnp.concatenate([tiles[2 * g], tail[:, : lanes - 128]], 1)
    edge = jnp.where(core == 0, pltpu.roll(edge, t_dev - 128, 1), edge)
    opens = jnp.where(core == 0, t_dev - 64, 0)
    closes = jnp.where(core == 0, t_dev, 62)
    outer_block = centered(edge, (place >= opens) & (place < closes) & (edge < NEAR))

    def part(value, sel):
        return jnp.dot(
            value.astype(jnp.bfloat16), sel.astype(jnp.bfloat16), preferred_element_type=f32
        )

    by_shift = (
        jnp.sum(core_sum, 1, keepdims=True)
        + part(outer_block, jnp.where(core == 0, late, early))
        - part(inner_block, jnp.where(core == 0, early, late))
    )
    tot_part[...] = jnp.zeros_like(tot_part)
    for k in range(kcount):
        tot_part[k : k + 1, :] = pltpu.roll(
            by_shift[k : k + 1], lax.rem(128 - offset_ref[k], 128), 1
        )
    total_copy().start()

    def center_window(step):
        for k in range(kcount):
            value = raw_win[step, k * BASE : (k + 1) * BASE, :]
            value = jnp.where(value < NEAR, value - mean[k : k + 1], 0.0).astype(jnp.bfloat16)
            for turn in range(0, ROWS, BASE):
                turned = value if turn == 0 else pltpu.roll(value, turn, 1)
                win[step, k * ROWS + turn : k * ROWS + turn + BASE, :] = turned[:, :lanes]

    low = lax.broadcasted_iota(jnp.int32, (ROWS, 128), 1) < 64
    low_row = lax.broadcasted_iota(jnp.int32, (1, 128), 1) < 64

    def pair_cols(cols, k):
        return jnp.where(low, cols[0:ROWS, k : k + 1], cols[0:ROWS, k + half_k : k + half_k + 1])

    def halves(first_half, second_half, is_low):
        turned_first = pltpu.roll(first_half, 64, 1)
        turned_second = pltpu.roll(second_half, 64, 1)
        zeroth = jnp.where(is_low, first_half, turned_second)
        oneth = jnp.where(is_low, turned_first, second_half)
        return jnp.where(core == 0, zeroth, oneth), jnp.where(core == 0, oneth, zeroth)

    group_days = 2 * g * t_dev * 1.0
    sums_at = 2 * count

    def add(pieces, step, first_time):
        width = 128 * len(pieces)
        value = jnp.concatenate([recv[piece, step] for piece in pieces], 1)
        wide_value = value.astype(f32)
        sums = jnp.sum(wide_value, 0, keepdims=True)
        squares = jnp.sum(wide_value * wide_value, 0, keepdims=True)
        found = jnp.dot(win[step, :, :t_dev], value, preferred_element_type=f32)
        if first_time:
            acc[0:sums_at, :width] = found
            acc[sums_at : sums_at + 1, :width] = sums
            acc[sums_at + 1 : sums_at + 2, :width] = squares
        else:
            acc[0:sums_at, :width] += found
            acc[sums_at : sums_at + 1, :width] += sums
            acc[sums_at + 1 : sums_at + 2, :width] += squares

    def split(piece, column):
        column = slice(column * 128, column * 128 + 128)
        for k in range(half_k):
            at = k * ROWS
            kept, given = halves(
                acc[at : at + ROWS, column], acc[count + at : count + at + ROWS, column], low
            )
            mine[piece, at : at + ROWS, :] = kept
            other[piece, at : at + ROWS, :] = given
        for row in range(2):
            value = acc[sums_at + row : sums_at + row + 1, column]
            kept, given = halves(value, value, low_row)
            mine[piece, count + row : count + row + 1, :] = kept
            other[piece, count + row : count + row + 1, :] = given
        swap_copy(piece).start()

    def products(piece):
        own_copy(piece).wait()
        add([piece], 0, True)

        def body(step, carry):
            raw_copy(piece, step).wait()
            add([piece], step, False)
            return carry

        lax.fori_loop(1, g, body, 0)
        split(piece, 0)

    def joined(piece, k):
        at = k * ROWS
        return mine[piece, at : at + ROWS, :] + partner_in[piece, at : at + ROWS, :]

    def joined_row(piece, row):
        at = count + row
        return mine[piece, at : at + 1, :] + partner_in[piece, at : at + 1, :]

    def decoded(slot, k):
        coded = got[slot, k * ROWS : (k + 1) * ROWS, :].astype(jnp.int32).astype(f32)
        return coded * (got_extra[slot, 2 + k : 3 + k, :] * (1.0 / TOP))

    def send_sums(piece, outer_slot):
        sx, sq = joined_row(piece, 0), joined_row(piece, 1)
        tot, cols, days = own_tot, own_cols, group_days
        copies = sum_copies(piece, slot_of(piece))
        if outer_slot is not None:
            arriving = sum_copies(1, outer_slot)
            arriving[0].wait_recv()
            outer_x = got_extra[outer_slot, 0:1, :]
            outer_mean = outer_x / group_days
            sx, sq = sx + outer_x, sq + got_extra[outer_slot, 1:2, :]
            outer_tot = got_extra[outer_slot, EXTRA:, :]
            outer_cols = jnp.transpose(outer_tot)
            tot, cols, days = tot + outer_tot, cols + outer_cols, 2 * group_days
        sent_extra[piece, 0:1, :] = sx
        sent_extra[piece, 1:2, :] = sq
        local_mean = sx / days
        for k in range(half_k):
            value = joined(piece, k) - local_mean * pair_cols(cols, k)
            if outer_slot is not None:
                value = value + outer_mean * pair_cols(outer_cols, k)
            stage[k * ROWS : (k + 1) * ROWS, :] = value
            top = jnp.max(jnp.abs(value), 0, keepdims=True)
            if outer_slot is not None:
                top = top + got_extra[outer_slot, 2 + k : 3 + k, :]
            sent_extra[piece, 2 + k : 3 + k, :] = top
        sent_extra[piece, EXTRA:, :] = tot
        copies[0].start()
        for k in range(half_k):
            value = stage[k * ROWS : (k + 1) * ROWS, :]
            if outer_slot is not None:
                arriving[1 + k].wait_recv()
                value = value + decoded(outer_slot, k)
            scaled = value * (TOP / jnp.maximum(sent_extra[piece, 2 + k : 3 + k, :], 1e-30))
            sent[piece, k * ROWS : (k + 1) * ROWS, :] = (
                jnp.round(scaled).astype(jnp.int32).astype(jnp.int16)
            )
            copies[1 + k].start()

    def send_outer(piece):
        @pl.when(jnp.logical_not(inner))
        def _():
            send_sums(piece, None)

    def send_inner(piece, outer_slot):
        @pl.when(inner)
        def _():
            send_sums(piece, outer_slot)

    last = groups - 1
    own_copy(0).wait()
    each(1, g, lambda s: raw_copy(0, s).wait())

    def early_body(step, first_time):
        center_window(step)
        add([0], step, first_time)

    early_body(0, True)
    if g <= 4:
        for step in range(1, g):
            early_body(step, False)
    else:
        each(1, g, lambda s: early_body(s, False))
    split(0, 0)

    total_copy().wait()
    own_tot = tot_part[...] + tot_in[...]
    own_cols = jnp.transpose(own_tot)
    swap_copy(0).wait()
    send_outer(0)
    products(1)
    swap_copy(1).wait()
    send_sums(1, None)
    send_inner(0, 0)
    products(2)
    swap_copy(2).wait()
    send_outer(2)
    send_inner(2, 1)
    products(last)
    sx = jnp.zeros((1, 128), f32)
    sq = jnp.zeros((1, 128), f32)
    all_cols = own_cols
    for slot, days in ((2, group_days), (3, 2 * group_days)):
        arriving = sum_copies(1, slot)
        arriving[0].wait_recv()
        far_x = got_extra[slot, 0:1, :]
        sx = sx + far_x
        sq = sq + got_extra[slot, 1:2, :]
        far_mean = far_x / days
        far_cols = jnp.transpose(got_extra[slot, EXTRA:, :])
        all_cols = all_cols + far_cols
        for k in range(half_k):
            at = k * ROWS
            arriving[1 + k].wait_recv()
            value = decoded(slot, k) + far_mean * pair_cols(far_cols, k)
            far[at : at + ROWS, :] = value if slot == 2 else far[at : at + ROWS, :] + value
    for piece in range(last):
        for copy in sum_copies(piece, slot_of(piece)):
            copy.wait_send()
    swap_copy(last).wait()
    sx = sx + joined_row(last, 0)
    sq = sq + joined_row(last, 1)
    mean_x = sx / total_days
    var_x = sq / total_days - mean_x * mean_x
    mask = small[0:1, :]
    mask = mask + pltpu.roll(mask, 64, 1)
    inner = mask / (total_days * jnp.sqrt(var_x + 1e-06))

    def normal(k):
        value = joined(last, k) + far[k * ROWS : (k + 1) * ROWS, :]
        value = value - mean_x * pair_cols(all_cols, k)
        scale = jnp.where(low_row, outer[k : k + 1], outer[k + half_k : k + half_k + 1])
        return value * (inner * scale)

    small_int = lag_ref[...] + MAXLAG
    small[0:1, 0 : lag_ref.shape[1]] = small_int.astype(f32)
    chosen = jnp.broadcast_to(small[0:1, :].astype(jnp.int32), (64, 128))
    kept = lag_ref.shape[1]

    def out_copy(k):
        return pltpu.make_async_copy(out_buf.at[k], out_ref.at[k], out_sem.at[k])

    for k in range(0, half_k, 2):
        upper_rows = normal(k)
        under_rows = normal(k + 1) if k + 1 < half_k else upper_rows
        flat = jnp.transpose(jnp.concatenate([upper_rows, under_rows], 0))
        for side in range(2):
            rows = flat[side * 64 : (side + 1) * 64, :]
            for turn in range(min(2, half_k - k)):
                at = k + turn + side * half_k
                out_buf[at] = jnp.take_along_axis(rows, chosen + 64 * turn, axis=1)[:, :kept]
                out_copy(at).start()
    for k in range(kcount):
        out_copy(k).wait()


def shards(field, index, lag_list, index_offset, sea_mask):
    t_dev, cells_all = field.shape
    devices = lax.axis_size("tm")
    kcount = index.shape[1]
    lanes = round_up(t_dev, 128)
    groups = GROUPS
    g = devices // 2 // groups
    rows = kcount * ROWS
    half = rows // 2
    sizes = (devices, t_dev, kcount, groups, g)
    dma = pltpu.SemaphoreType.DMA
    f32 = jnp.float32
    vmem = pl.BlockSpec(memory_space=pltpu.VMEM)
    maps = pl.pallas_call(
        functools.partial(kernel, sizes),
        out_shape=jax.ShapeDtypeStruct((kcount, 64, lag_list.shape[0]), f32),
        in_specs=[
            pl.BlockSpec(memory_space=pl.ANY),
            vmem,
            vmem,
            pl.BlockSpec(memory_space=pltpu.SMEM),
            vmem,
        ],
        out_specs=pl.BlockSpec(memory_space=pl.ANY),
        scratch_shapes=[
            pltpu.VMEM((t_dev, cells_all), jnp.bfloat16),
            pltpu.VMEM((kcount, lanes), f32),
            pltpu.VMEM((g, kcount, lanes), f32),
            pltpu.VMEM((2 * g + 1, kcount, 128), f32),
            pltpu.VMEM((kcount, 128), f32),
            pltpu.VMEM((groups, kcount, 128), f32),
            pltpu.VMEM((groups, g, t_dev, 128), jnp.bfloat16),
            pltpu.VMEM((g, kcount * BASE, lanes + 128), f32),
            pltpu.VMEM((g, rows, lanes), jnp.bfloat16),
            pltpu.VMEM((rows + EXTRA, 256), f32),
            pltpu.VMEM((groups, half + EXTRA, 128), f32),
            pltpu.VMEM((groups, half + EXTRA, 128), f32),
            pltpu.VMEM((groups, half + EXTRA, 128), f32),
            pltpu.VMEM((groups, half, 128), jnp.int16),
            pltpu.VMEM((groups, EXTRA + 16, 128), f32),
            pltpu.VMEM((groups, half, 128), jnp.int16),
            pltpu.VMEM((groups, EXTRA + 16, 128), f32),
            pltpu.VMEM((half, 128), f32),
            pltpu.VMEM((half, 128), f32),
            pltpu.VMEM((kcount, 64, lag_list.shape[0]), f32),
            pltpu.VMEM((8, 128), f32),
            pltpu.VMEM((16, 128), f32),
            pltpu.VMEM((16, 128), f32),
            dma((groups, g)),
            dma((groups, g)),
            dma((g,)),
            dma((g,)),
            dma((2, g)),
            dma((2, g)),
            dma((4,)),
            dma((groups,)),
            dma((groups,)),
            dma((groups,)),
            dma((groups,)),
            dma((kcount // 2 + 1, groups)),
            dma((kcount // 2 + 1, groups)),
            dma((groups + 1,)),
            pltpu.SemaphoreType.REGULAR((groups,)),
            dma((kcount,)),
        ],
        compiler_params=pltpu.CompilerParams(
            collective_id=0, has_side_effects=True, vmem_limit_bytes=60 * 1024 * 1024
        ),
    )(field, index.T, lag_list[None, :], index_offset, sea_mask[None, :])
    return jnp.transpose(maps, (1, 0, 2))


def solution(mesh):
    return jax.shard_map(
        shards,
        mesh=mesh,
        in_specs=(P("tm", None), P("tm", None), P(), P(), P("tm")),
        out_specs=P("tm", None, None),
        check_vma=False,
    )
```

```python
import functools

import jax
import jax.numpy as jnp
from jax import lax
from jax.experimental import pallas as pl
from jax.experimental.pallas import tpu as pltpu
from jax.sharding import PartitionSpec as P

MAXLAG = 30
MAXOFF = 14
REACH = 64
ROWS = 64
BASE = 16
EXTRA = 8
TOP = 32767.0
FAR = 1e30
NEAR = 1e29
GROUPS = 4
MESH = pl.DeviceIdType.MESH


def round_up(value, unit):
    return -(-value // unit) * unit


def kernel(
    sizes,
    field_hbm,
    index_hbm,
    lag_hbm,
    offset_hbm,
    mask_hbm,
    out_ref,
    index_ref,
    lag_ref,
    offset_ref,
    mask_ref,
    field_ref,
    idx_ref,
    idx_all,
    tiles,
    zmsg,
    zin,
    recv,
    raw_win,
    win,
    acc,
    mine,
    other,
    partner_in,
    sent,
    sent_extra,
    got,
    got_extra,
    far,
    stage,
    out_buf,
    small,
    tot_part,
    tot_in,
    raw_send,
    raw_recv,
    idx_send,
    idx_recv,
    tile_send,
    tile_recv,
    lone_sem,
    z_send,
    z_recv,
    swap_send,
    swap_recv,
    sum_send,
    sum_recv,
    own_sem,
    round_sem,
    out_sem,
    in_sem,
):
    devices, t_dev, kcount, groups, g = sizes
    lanes = idx_ref.shape[1]
    wide = lanes + 128
    half_k = kcount // 2
    count = half_k * ROWS
    cells = 128
    me = lax.axis_index("tm")
    core = lax.rem(me, 2)
    chip = lax.div(me, 2)
    h = lax.div(chip, g)
    m = lax.rem(chip, g)
    partner = chip * 2 + (1 - core)
    edge_peer = ((h + 2 * core - 1) * g + m) * 2 + (1 - core)
    has_edge = jnp.where(core == 0, h > 0, h < groups - 1)
    f32 = jnp.float32
    total_days = devices * t_dev * 1.0

    def flipped(value, step, size):
        found, bit = 0, 1
        while bit < size:
            flip = lax.rem(lax.div(value, bit) + lax.div(step, bit), 2)
            found, bit = found + flip * bit, bit * 2
        return found

    def across(step):
        return flipped(m, step, g)

    def device_of(group, member):
        return (group * g + member) * 2 + core

    def remote(src, dst, send, recv_s, device):
        return pltpu.make_async_remote_copy(
            src_ref=src,
            dst_ref=dst,
            send_sem=send,
            recv_sem=recv_s,
            device_id=(device,),
            device_id_type=MESH,
        )

    def block(at):
        return field_ref.at[:, pl.ds(pl.multiple_of(at * cells, cells), cells)]

    inner = jnp.logical_or(h == 1, h == 2)
    upper = lax.div(h, 2)
    beside_h = h + 1 - 2 * lax.rem(h, 2)

    def plane_of(piece):
        if piece == 0:
            return (groups - 1) * (1 - upper)
        if piece == 1:
            return jnp.where(inner, beside_h, 2 - upper)
        return jnp.where(inner, 2 - upper, beside_h) if piece == 2 else h

    def raw_copy(piece, step):
        to = across(step)
        return remote(
            block(plane_of(piece) * g + to),
            recv.at[piece, step],
            raw_send.at[piece],
            raw_recv.at[piece, step - 1],
            device_of(h, to),
        )

    def own_copy(piece):
        return pltpu.make_async_copy(
            block(plane_of(piece) * g + m), recv.at[piece, 0], own_sem.at[piece]
        )

    def idx_copy(step):
        return remote(
            idx_ref,
            idx_all.at[m],
            idx_send.at[0],
            idx_recv.at[step - 1],
            device_of(h, across(step)),
        )

    def tile_copy(side, step):
        to = (h * g + across(step)) * 2 + (core if side == 0 else 1 - core)
        tile = tiles.at[core * g + m]
        return remote(
            tile, tile, tile_send.at[0], tile_recv.at[side * g + step - 1], to
        )

    def edge_copy():
        return remote(
            tiles.at[jnp.where(core == 0, 0, 2 * g - 1)],
            tiles.at[2 * g],
            lone_sem.at[0],
            lone_sem.at[1],
            edge_peer,
        )

    def total_copy():
        return remote(tot_part, tot_in, lone_sem.at[2], lone_sem.at[3], partner)

    def z_copy(step):
        return remote(
            zmsg,
            zin.at[step],
            z_send.at[0],
            z_recv.at[step - 1],
            device_of(flipped(h, step, groups), m),
        )

    def swap_copy(piece, k):
        rows = pl.ds(k * ROWS, ROWS if k < half_k else EXTRA)
        return remote(
            other.at[piece, rows],
            partner_in.at[piece, rows],
            swap_send.at[piece],
            swap_recv.at[piece, k],
            partner,
        )

    def slot_of(piece):
        return jnp.where(inner, (3, 2, 3)[piece], piece)

    def receiver(piece):
        if piece == 1:
            return device_of(beside_h, m)
        return device_of(jnp.where(inner, plane_of(piece), beside_h), m)

    def sum_copies(piece, slot):
        copies = [
            remote(
                sent_extra.at[piece],
                got_extra.at[slot],
                sum_send.at[1, piece],
                sum_recv.at[half_k, slot],
                receiver(piece),
            )
        ]
        for k in range(half_k):
            rows = pl.ds(k * ROWS, ROWS)
            copies.append(
                remote(
                    sent.at[piece, rows],
                    got.at[slot, rows],
                    sum_send.at[0, piece],
                    sum_recv.at[k, slot],
                    receiver(piece),
                )
            )
        return copies

    def each(low_step, high_step, act):
        def body(step, carry):
            act(step)
            return carry

        lax.fori_loop(low_step, high_step, body, 0)

    load = pltpu.make_async_copy(field_hbm, field_ref, own_sem.at[groups])
    inputs = [
        pltpu.make_async_copy(src, dst, in_sem.at[at])
        for at, (src, dst) in enumerate(
            (
                (index_hbm, index_ref),
                (lag_hbm, lag_ref),
                (offset_hbm, offset_ref),
                (mask_hbm, mask_ref),
            )
        )
    ]
    barrier = pltpu.get_barrier_semaphore()

    def tell(sem, device):
        pl.semaphore_signal(sem, inc=1, device_id=(device,), device_id_type=MESH)

    def tell_line(sem):
        @pl.when(h > 0)
        def _():
            tell(sem, device_of(h - 1, m))

        @pl.when(h < groups - 1)
        def _():
            tell(sem, device_of(h + 1, m))

    beside = jnp.where(h > 0, 1, 0) + jnp.where(h < groups - 1, 1, 0)
    tell_line(barrier)

    @pl.when(has_edge)
    def _():
        tell(barrier, edge_peer)

    each(1, 2 * g, lambda s: tell(barrier, (h * g + across(lax.div(s, 2))) * 2 + lax.rem(core + s, 2)))
    inputs[0].start()
    load.start()
    for copy in inputs[1:]:
        copy.start()
    idx_ref[...] = jnp.zeros_like(idx_ref)
    other[...] = jnp.zeros_like(other)
    sent_extra[...] = jnp.zeros_like(sent_extra)
    small[...] = jnp.zeros_like(small)
    inputs[0].wait()
    idx_ref[0:kcount, 0:t_dev] = index_ref[...]
    lane = lax.broadcasted_iota(jnp.int32, (kcount, 128), 1)
    series = idx_ref[...]
    tile = jnp.where(
        lane < 64, series[:, :128], pltpu.roll(series, (128 - t_dev) % lanes, 1)[:, :128]
    )
    tile = jnp.where(lane == 62, jnp.sum(series, 1, keepdims=True), tile)
    tile = jnp.where(lane == 63, jnp.sum(series * series, 1, keepdims=True), tile)
    tiles[core * g + m] = tile
    idx_all[m] = series

    @pl.when(jnp.logical_not(has_edge))
    def _():
        tiles[2 * g] = jnp.full((kcount, 128), FAR, f32)

    pl.semaphore_wait(barrier, 2 * g - 1 + beside + jnp.where(has_edge, 1, 0))

    for side in range(2):
        each(1 - side, g, lambda s, side=side: tile_copy(side, s).start())
    each(1, g, lambda s: idx_copy(s).start())
    load.wait()
    for copy in inputs[1:]:
        copy.wait()
    small[0:1, 0 : cells // 2] = mask_ref[...].astype(f32)
    for piece in range(groups):
        own_copy(piece).start()
        each(1, g, lambda s, piece=piece: raw_copy(piece, s).start())
    for turn in range(groups - 2):
        tell_line(round_sem.at[turn])
        pl.semaphore_wait(round_sem.at[turn], beside)
    for side in range(2):
        each(1 - side, g, lambda s, side=side: tile_copy(side, s).wait_recv())

    @pl.when(has_edge)
    def _():
        edge_copy().start()

    zero_tile = jnp.zeros((kcount, 128), f32)
    zmsg[...] = lax.fori_loop(0, 2 * g, lambda at, carry: carry + tiles[at], zero_tile)
    each(1, groups, lambda s: z_copy(s).start())
    each(1, g, lambda s: idx_copy(s).wait_recv())

    spot = lax.broadcasted_iota(jnp.int32, (kcount, wide), 1)
    wing = jnp.zeros((kcount, 128), f32)
    tail = jnp.zeros((kcount, wide - 128), f32)

    def tile_at(order):
        inside = lax.rem(order, 2) * g + lax.div(order, 2)
        outside = jnp.logical_or(order < 0, order >= 2 * g)
        return tiles[jnp.where(outside, 2 * g, inside)]

    def window(member):
        order = member * 2 + core
        step = flipped(m, member, g)
        here = jnp.concatenate([idx_all[member], wing], 1)
        before = jnp.concatenate([tile_at(order - 1), tail], 1)
        after = jnp.concatenate([tile_at(order + 1), tail], 1)
        left = pltpu.roll(before, wide - REACH, 1)
        mid = pltpu.roll(here, REACH, 1)
        right = pltpu.roll(after, REACH + t_dev, 1)
        ext = jnp.where(spot < REACH, left, jnp.where(spot < REACH + t_dev, mid, right))
        for k in range(kcount):
            line = pltpu.roll(ext[k : k + 1], wide - REACH - MAXLAG + offset_ref[k], 1)
            line = jnp.broadcast_to(line, (BASE, wide))
            raw_win[step, k * BASE : (k + 1) * BASE, :] = pltpu.roll(
                line, 0, 1, stride=1, stride_axis=0
            )

    each(0, g - 1, lambda at: window(jnp.where(core == 0, g - 1 - at, at)))

    @pl.when(has_edge)
    def _():
        edge_copy().wait()

    window(jnp.where(core == 0, 0, g - 1))
    each(1, groups, lambda s: z_copy(s).wait_recv())
    stats = zmsg[...]
    for s in range(1, groups):
        stats = stats + zin[s]
    mean = stats[:, 62:63] / total_days
    var = stats[:, 63:64] / total_days - mean * mean
    outer = 1.0 / jnp.sqrt(var + 1e-06)

    place = lax.broadcasted_iota(jnp.int32, (kcount, lanes), 1)
    day = lax.broadcasted_iota(jnp.int32, (lanes, 128), 0)
    shift = lax.broadcasted_iota(jnp.int32, (lanes, 128), 1) - MAXLAG
    late = jnp.where((day >= t_dev - shift) & (day < t_dev), 1.0, 0.0)
    early = jnp.where(day < -shift, 1.0, 0.0)

    def centered(value, valid):
        return jnp.where(valid, (value - mean).astype(jnp.bfloat16).astype(f32), 0.0)

    def center_body(at, carry):
        return carry + centered(idx_all[at], place < t_dev)

    core_sum = lax.fori_loop(0, g, center_body, jnp.zeros((kcount, lanes), f32))
    inner_block = centered(idx_all[jnp.where(core == 0, 0, g - 1)], place < t_dev)
    edge = jnp.concatenate([tiles[2 * g], tail[:, : lanes - 128]], 1)
    edge = jnp.where(core == 0, pltpu.roll(edge, t_dev - 128, 1), edge)
    opens = jnp.where(core == 0, t_dev - 64, 0)
    closes = jnp.where(core == 0, t_dev, 62)
    outer_block = centered(edge, (place >= opens) & (place < closes) & (edge < NEAR))

    def part(value, sel):
        return jnp.dot(
            value.astype(jnp.bfloat16), sel.astype(jnp.bfloat16), preferred_element_type=f32
        )

    by_shift = (
        jnp.sum(core_sum, 1, keepdims=True)
        + part(outer_block, jnp.where(core == 0, late, early))
        - part(inner_block, jnp.where(core == 0, early, late))
    )
    tot_part[...] = jnp.zeros_like(tot_part)
    for k in range(kcount):
        tot_part[k : k + 1, :] = pltpu.roll(
            by_shift[k : k + 1], lax.rem(128 - offset_ref[k], 128), 1
        )
    total_copy().start()

    def center_window(step):
        for k in range(kcount):
            value = raw_win[step, k * BASE : (k + 1) * BASE, :]
            value = jnp.where(value < NEAR, value - mean[k : k + 1], 0.0).astype(jnp.bfloat16)
            for turn in range(0, ROWS, BASE):
                turned = value if turn == 0 else pltpu.roll(value, turn, 1)
                win[step, k * ROWS + turn : k * ROWS + turn + BASE, :] = turned[:, :lanes]

    low = lax.broadcasted_iota(jnp.int32, (ROWS, 128), 1) < 64
    low_row = lax.broadcasted_iota(jnp.int32, (1, 128), 1) < 64

    def pair_cols(cols, k):
        return jnp.where(low, cols[0:ROWS, k : k + 1], cols[0:ROWS, k + half_k : k + half_k + 1])

    def halves(first_half, second_half, is_low):
        turned_first = pltpu.roll(first_half, 64, 1)
        turned_second = pltpu.roll(second_half, 64, 1)
        zeroth = jnp.where(is_low, first_half, turned_second)
        oneth = jnp.where(is_low, turned_first, second_half)
        return jnp.where(core == 0, zeroth, oneth), jnp.where(core == 0, oneth, zeroth)

    group_days = 2 * g * t_dev * 1.0
    sums_at = 2 * count

    def add(pieces, step, first_time):
        width = 128 * len(pieces)
        value = jnp.concatenate([recv[piece, step] for piece in pieces], 1)
        wide_value = value.astype(f32)
        sums = jnp.sum(wide_value, 0, keepdims=True)
        squares = jnp.sum(wide_value * wide_value, 0, keepdims=True)
        found = jnp.dot(win[step, :, :t_dev], value, preferred_element_type=f32)
        if first_time:
            acc[0:sums_at, :width] = found
            acc[sums_at : sums_at + 1, :width] = sums
            acc[sums_at + 1 : sums_at + 2, :width] = squares
        else:
            acc[0:sums_at, :width] += found
            acc[sums_at : sums_at + 1, :width] += sums
            acc[sums_at + 1 : sums_at + 2, :width] += squares

    def split(piece, column):
        column = slice(column * 128, column * 128 + 128)
        for row in range(2):
            value = acc[sums_at + row : sums_at + row + 1, column]
            kept, given = halves(value, value, low_row)
            mine[piece, count + row : count + row + 1, :] = kept
            other[piece, count + row : count + row + 1, :] = given
        swap_copy(piece, half_k).start()
        for k in range(half_k):
            at = k * ROWS
            kept, given = halves(
                acc[at : at + ROWS, column], acc[count + at : count + at + ROWS, column], low
            )
            mine[piece, at : at + ROWS, :] = kept
            other[piece, at : at + ROWS, :] = given
            swap_copy(piece, k).start()

    def products(piece):
        own_copy(piece).wait()
        add([piece], 0, True)

        def body(step, carry):
            raw_copy(piece, step).wait_recv()
            add([piece], step, False)
            return carry

        lax.fori_loop(1, g, body, 0)
        split(piece, 0)

    def joined(piece, k):
        at = k * ROWS
        swap_copy(piece, k).wait_recv()
        return mine[piece, at : at + ROWS, :] + partner_in[piece, at : at + ROWS, :]

    def joined_row(piece, row):
        at = count + row
        return mine[piece, at : at + 1, :] + partner_in[piece, at : at + 1, :]

    def decoded(slot, k):
        coded = got[slot, k * ROWS : (k + 1) * ROWS, :].astype(jnp.int32).astype(f32)
        return coded * (got_extra[slot, 2 + k : 3 + k, :] * (1.0 / TOP))

    def send_sums(piece, outer_slot):
        swap_copy(piece, half_k).wait_recv()
        sx, sq = joined_row(piece, 0), joined_row(piece, 1)
        tot, cols, days = own_tot, own_cols, group_days
        copies = sum_copies(piece, slot_of(piece))
        if outer_slot is not None:
            arriving = sum_copies(1, outer_slot)
            arriving[0].wait_recv()
            outer_x = got_extra[outer_slot, 0:1, :]
            outer_mean = outer_x / group_days
            sx, sq = sx + outer_x, sq + got_extra[outer_slot, 1:2, :]
            outer_tot = got_extra[outer_slot, EXTRA:, :]
            outer_cols = jnp.transpose(outer_tot)
            tot, cols, days = tot + outer_tot, cols + outer_cols, 2 * group_days
        sent_extra[piece, 0:1, :] = sx
        sent_extra[piece, 1:2, :] = sq
        local_mean = sx / days
        for k in range(half_k):
            value = joined(piece, k) - local_mean * pair_cols(cols, k)
            if outer_slot is not None:
                value = value + outer_mean * pair_cols(outer_cols, k)
            stage[k * ROWS : (k + 1) * ROWS, :] = value
            top = jnp.max(jnp.abs(value), 0, keepdims=True)
            if outer_slot is not None:
                top = top + got_extra[outer_slot, 2 + k : 3 + k, :]
            sent_extra[piece, 2 + k : 3 + k, :] = top
        sent_extra[piece, EXTRA:, :] = tot
        copies[0].start()
        for k in range(half_k):
            value = stage[k * ROWS : (k + 1) * ROWS, :]
            if outer_slot is not None:
                arriving[1 + k].wait_recv()
                value = value + decoded(outer_slot, k)
            scaled = value * (TOP / jnp.maximum(sent_extra[piece, 2 + k : 3 + k, :], 1e-30))
            sent[piece, k * ROWS : (k + 1) * ROWS, :] = (
                jnp.round(scaled).astype(jnp.int32).astype(jnp.int16)
            )
            copies[1 + k].start()

    def send_outer(piece):
        @pl.when(jnp.logical_not(inner))
        def _():
            send_sums(piece, None)

    def send_inner(piece, outer_slot):
        @pl.when(inner)
        def _():
            send_sums(piece, outer_slot)

    last = groups - 1
    own_copy(0).wait()
    each(1, g, lambda s: raw_copy(0, s).wait_recv())

    def early_body(step, first_time):
        center_window(step)
        add([0], step, first_time)

    early_body(0, True)
    if g <= 4:
        for step in range(1, g):
            early_body(step, False)
    else:
        each(1, g, lambda s: early_body(s, False))
    split(0, 0)

    total_copy().wait()
    own_tot = tot_part[...] + tot_in[...]
    own_cols = jnp.transpose(own_tot)
    send_outer(0)
    products(1)
    send_sums(1, None)
    send_inner(0, 0)
    products(2)
    send_outer(2)
    send_inner(2, 1)
    products(last)
    sx = jnp.zeros((1, 128), f32)
    sq = jnp.zeros((1, 128), f32)
    all_cols = own_cols
    for slot, days in ((2, group_days), (3, 2 * group_days)):
        arriving = sum_copies(1, slot)
        arriving[0].wait_recv()
        far_x = got_extra[slot, 0:1, :]
        sx = sx + far_x
        sq = sq + got_extra[slot, 1:2, :]
        far_mean = far_x / days
        far_cols = jnp.transpose(got_extra[slot, EXTRA:, :])
        all_cols = all_cols + far_cols
        for k in range(half_k):
            at = k * ROWS
            arriving[1 + k].wait_recv()
            value = decoded(slot, k) + far_mean * pair_cols(far_cols, k)
            far[at : at + ROWS, :] = value if slot == 2 else far[at : at + ROWS, :] + value
    swap_copy(last, half_k).wait_recv()
    sx = sx + joined_row(last, 0)
    sq = sq + joined_row(last, 1)
    mean_x = sx / total_days
    var_x = sq / total_days - mean_x * mean_x
    mask = small[0:1, :]
    mask = mask + pltpu.roll(mask, 64, 1)
    inner = mask / (total_days * jnp.sqrt(var_x + 1e-06))

    def normal(k):
        value = joined(last, k) + far[k * ROWS : (k + 1) * ROWS, :]
        value = value - mean_x * pair_cols(all_cols, k)
        scale = jnp.where(low_row, outer[k : k + 1], outer[k + half_k : k + half_k + 1])
        return value * (inner * scale)

    small_int = lag_ref[...] + MAXLAG
    small[0:1, 0 : lag_ref.shape[1]] = small_int.astype(f32)
    chosen = jnp.broadcast_to(small[0:1, :].astype(jnp.int32), (64, 128))
    kept = lag_ref.shape[1]

    def out_copy(k):
        return pltpu.make_async_copy(out_buf.at[k], out_ref.at[k], out_sem.at[0])

    for k in range(0, half_k, 2):
        upper_rows = normal(k)
        under_rows = normal(k + 1) if k + 1 < half_k else upper_rows
        flat = jnp.transpose(jnp.concatenate([upper_rows, under_rows], 0))
        for side in range(2):
            rows = flat[side * 64 : (side + 1) * 64, :]
            for turn in range(min(2, half_k - k)):
                at = k + turn + side * half_k
                out_buf[at] = jnp.take_along_axis(rows, chosen + 64 * turn, axis=1)[:, :kept]
                out_copy(at).start()
    def drained(ref, sem):
        remote(ref, ref, sem, sem, partner).wait_send()

    drained(idx_all.at[pl.ds(0, g - 1)], idx_send.at[0])
    drained(tiles.at[pl.ds(0, 2 * g - 1)], tile_send.at[0])
    drained(zin.at[pl.ds(0, groups - 1)], z_send.at[0])
    for piece in range(groups):
        drained(recv.at[piece, pl.ds(0, g - 1)], raw_send.at[piece])
        drained(other.at[piece], swap_send.at[piece])
        if piece < last:
            drained(sent.at[piece], sum_send.at[0, piece])
            drained(sent_extra.at[piece], sum_send.at[1, piece])
    pltpu.make_async_copy(out_buf, out_ref, out_sem.at[0]).wait()


def shards(field, index, lag_list, index_offset, sea_mask):
    t_dev, cells_all = field.shape
    devices = lax.axis_size("tm")
    kcount = index.shape[1]
    lanes = round_up(t_dev, 128)
    groups = GROUPS
    g = devices // 2 // groups
    rows = kcount * ROWS
    half = rows // 2
    sizes = (devices, t_dev, kcount, groups, g)
    dma = pltpu.SemaphoreType.DMA
    f32 = jnp.float32
    maps = pl.pallas_call(
        functools.partial(kernel, sizes),
        out_shape=jax.ShapeDtypeStruct((kcount, 64, lag_list.shape[0]), f32),
        in_specs=[pl.BlockSpec(memory_space=pl.ANY)] * 5,
        out_specs=pl.BlockSpec(memory_space=pl.ANY),
        scratch_shapes=[
            pltpu.VMEM((kcount, t_dev), f32),
            pltpu.VMEM((1, lag_list.shape[0]), jnp.int32),
            pltpu.SMEM((kcount,), jnp.int32),
            pltpu.VMEM((1, sea_mask.shape[0]), jnp.int32),
            pltpu.VMEM((t_dev, cells_all), jnp.bfloat16),
            pltpu.VMEM((kcount, lanes), f32),
            pltpu.VMEM((g, kcount, lanes), f32),
            pltpu.VMEM((2 * g + 1, kcount, 128), f32),
            pltpu.VMEM((kcount, 128), f32),
            pltpu.VMEM((groups, kcount, 128), f32),
            pltpu.VMEM((groups, g, t_dev, 128), jnp.bfloat16),
            pltpu.VMEM((g, kcount * BASE, lanes + 128), f32),
            pltpu.VMEM((g, rows, lanes), jnp.bfloat16),
            pltpu.VMEM((rows + EXTRA, 256), f32),
            pltpu.VMEM((groups, half + EXTRA, 128), f32),
            pltpu.VMEM((groups, half + EXTRA, 128), f32),
            pltpu.VMEM((groups, half + EXTRA, 128), f32),
            pltpu.VMEM((groups, half, 128), jnp.int16),
            pltpu.VMEM((groups, EXTRA + 16, 128), f32),
            pltpu.VMEM((groups, half, 128), jnp.int16),
            pltpu.VMEM((groups, EXTRA + 16, 128), f32),
            pltpu.VMEM((half, 128), f32),
            pltpu.VMEM((half, 128), f32),
            pltpu.VMEM((kcount, 64, lag_list.shape[0]), f32),
            pltpu.VMEM((8, 128), f32),
            pltpu.VMEM((16, 128), f32),
            pltpu.VMEM((16, 128), f32),
            dma((groups,)),
            dma((groups, g - 1)),
            dma((1,)),
            dma((g - 1,)),
            dma((1,)),
            dma((2 * g - 1,)),
            dma((4,)),
            dma((1,)),
            dma((groups - 1,)),
            dma((groups,)),
            dma((groups, kcount // 2 + 1)),
            dma((2, groups - 1)),
            dma((kcount // 2 + 1, groups)),
            dma((groups + 1,)),
            pltpu.SemaphoreType.REGULAR((groups - 2,)),
            dma((1,)),
            dma((4,)),
        ],
        compiler_params=pltpu.CompilerParams(
            collective_id=0, has_side_effects=True, vmem_limit_bytes=60 * 1024 * 1024
        ),
    )(field, index.T, lag_list[None, :], index_offset, sea_mask[None, :])
    return jnp.transpose(maps, (1, 0, 2))


def solution(mesh):
    return jax.shard_map(
        shards,
        mesh=mesh,
        in_specs=(P("tm", None), P("tm", None), P(), P(), P("tm")),
        out_specs=P("tm", None, None),
        check_vma=False,
    )
```

```python
import functools

import jax
import jax.numpy as jnp
from jax import lax
from jax.experimental import pallas as pl
from jax.experimental.pallas import tpu as pltpu
from jax.sharding import PartitionSpec as P

MAXLAG = 30
MAXOFF = 14
REACH = 64
ROWS = 64
BASE = 16
EXTRA = 8
TOP = 32767.0
FAR = 1e30
NEAR = 1e29
GROUPS = 4
MESH = pl.DeviceIdType.MESH


def round_up(value, unit):
    return -(-value // unit) * unit


def kernel(
    sizes,
    field_hbm,
    index_hbm,
    lag_hbm,
    offset_hbm,
    mask_hbm,
    out_ref,
    index_ref,
    lag_ref,
    offset_ref,
    mask_ref,
    field_ref,
    idx_ref,
    idx_all,
    tiles,
    zmsg,
    zin,
    recv,
    raw_win,
    win,
    acc,
    mine,
    other,
    partner_in,
    sent,
    sent_extra,
    got,
    got_extra,
    far,
    stage,
    chooser,
    out_buf,
    small,
    tot_part,
    tot_in,
    raw_send,
    raw_recv,
    idx_send,
    idx_recv,
    tile_send,
    tile_recv,
    lone_sem,
    z_send,
    z_recv,
    swap_send,
    swap_recv,
    sum_send,
    sum_recv,
    own_sem,
    round_sem,
    out_sem,
    in_sem,
):
    devices, t_dev, kcount, groups, g = sizes
    lanes = idx_ref.shape[1]
    wide = lanes + 128
    half_k = kcount // 2
    count = half_k * ROWS
    cells = 128
    me = lax.axis_index("tm")
    core = lax.rem(me, 2)
    chip = lax.div(me, 2)
    h = lax.div(chip, g)
    m = lax.rem(chip, g)
    partner = chip * 2 + (1 - core)
    edge_peer = ((h + 2 * core - 1) * g + m) * 2 + (1 - core)
    has_edge = jnp.where(core == 0, h > 0, h < groups - 1)
    f32 = jnp.float32
    total_days = devices * t_dev * 1.0

    def flipped(value, step, size):
        found, bit = 0, 1
        while bit < size:
            flip = lax.rem(lax.div(value, bit) + lax.div(step, bit), 2)
            found, bit = found + flip * bit, bit * 2
        return found

    def across(step):
        return flipped(m, step, g)

    def device_of(group, member):
        return (group * g + member) * 2 + core

    def remote(src, dst, send, recv_s, device):
        return pltpu.make_async_remote_copy(
            src_ref=src,
            dst_ref=dst,
            send_sem=send,
            recv_sem=recv_s,
            device_id=(device,),
            device_id_type=MESH,
        )

    def block(at):
        return field_ref.at[:, pl.ds(pl.multiple_of(at * cells, cells), cells)]

    inner = jnp.logical_or(h == 1, h == 2)
    upper = lax.div(h, 2)
    beside_h = h + 1 - 2 * lax.rem(h, 2)

    def plane_of(piece):
        if piece == 0:
            return (groups - 1) * (1 - upper)
        if piece == 1:
            return jnp.where(inner, beside_h, 2 - upper)
        return jnp.where(inner, 2 - upper, beside_h) if piece == 2 else h

    def raw_copy(piece, step):
        to = across(step)
        return remote(
            block(plane_of(piece) * g + to),
            recv.at[piece, step],
            raw_send.at[piece],
            raw_recv.at[piece, step - 1],
            device_of(h, to),
        )

    def own_copy(piece):
        return pltpu.make_async_copy(
            block(plane_of(piece) * g + m), recv.at[piece, 0], own_sem.at[piece]
        )

    def idx_copy(step):
        return remote(
            idx_ref,
            idx_all.at[m],
            idx_send.at[0],
            idx_recv.at[step - 1],
            device_of(h, across(step)),
        )

    def tile_copy(side, step):
        to = (h * g + across(step)) * 2 + (core if side == 0 else 1 - core)
        tile = tiles.at[core * g + m]
        return remote(
            tile, tile, tile_send.at[0], tile_recv.at[side * g + step - 1], to
        )

    def edge_copy():
        return remote(
            tiles.at[jnp.where(core == 0, 0, 2 * g - 1)],
            tiles.at[2 * g],
            lone_sem.at[0],
            lone_sem.at[1],
            edge_peer,
        )

    def total_copy():
        return remote(tot_part, tot_in, lone_sem.at[2], lone_sem.at[3], partner)

    def z_copy(step):
        return remote(
            zmsg,
            zin.at[step],
            z_send.at[0],
            z_recv.at[step - 1],
            device_of(flipped(h, step, groups), m),
        )

    def swap_copy(piece, k):
        rows = pl.ds(k * ROWS, ROWS if k < half_k else EXTRA)
        return remote(
            other.at[piece, rows],
            partner_in.at[piece, rows],
            swap_send.at[piece],
            swap_recv.at[piece, k],
            partner,
        )

    def slot_of(piece):
        return jnp.where(inner, (3, 2, 3)[piece], piece)

    def receiver(piece):
        if piece == 1:
            return device_of(beside_h, m)
        return device_of(jnp.where(inner, plane_of(piece), beside_h), m)

    def sum_copies(piece, slot):
        copies = [
            remote(
                sent_extra.at[piece],
                got_extra.at[slot],
                sum_send.at[1, piece],
                sum_recv.at[half_k, slot],
                receiver(piece),
            )
        ]
        for k in range(half_k):
            rows = pl.ds(k * ROWS, ROWS)
            copies.append(
                remote(
                    sent.at[piece, rows],
                    got.at[slot, rows],
                    sum_send.at[0, piece],
                    sum_recv.at[k, slot],
                    receiver(piece),
                )
            )
        return copies

    def each(low_step, high_step, act):
        def body(step, carry):
            act(step)
            return carry

        lax.fori_loop(low_step, high_step, body, 0)

    load = pltpu.make_async_copy(field_hbm, field_ref, own_sem.at[groups])
    inputs = [
        pltpu.make_async_copy(src, dst, in_sem.at[at])
        for at, (src, dst) in enumerate(
            (
                (index_hbm, index_ref),
                (lag_hbm, lag_ref),
                (offset_hbm, offset_ref),
                (mask_hbm, mask_ref),
            )
        )
    ]
    barrier = pltpu.get_barrier_semaphore()

    def tell(sem, device):
        pl.semaphore_signal(sem, inc=1, device_id=(device,), device_id_type=MESH)

    def tell_line(sem):
        @pl.when(h > 0)
        def _():
            tell(sem, device_of(h - 1, m))

        @pl.when(h < groups - 1)
        def _():
            tell(sem, device_of(h + 1, m))

    beside = jnp.where(h > 0, 1, 0) + jnp.where(h < groups - 1, 1, 0)
    tell_line(barrier)

    @pl.when(has_edge)
    def _():
        tell(barrier, edge_peer)

    each(1, 2 * g, lambda s: tell(barrier, (h * g + across(lax.div(s, 2))) * 2 + lax.rem(core + s, 2)))
    inputs[0].start()
    load.start()
    for copy in inputs[1:]:
        copy.start()
    idx_ref[...] = jnp.zeros_like(idx_ref)
    other[...] = jnp.zeros_like(other)
    sent_extra[...] = jnp.zeros_like(sent_extra)
    small[...] = jnp.zeros_like(small)
    inputs[0].wait()
    idx_ref[0:kcount, 0:t_dev] = index_ref[...]
    lane = lax.broadcasted_iota(jnp.int32, (kcount, 128), 1)
    series = idx_ref[...]
    tile = jnp.where(
        lane < 64, series[:, :128], pltpu.roll(series, (128 - t_dev) % lanes, 1)[:, :128]
    )
    tile = jnp.where(lane == 62, jnp.sum(series, 1, keepdims=True), tile)
    tile = jnp.where(lane == 63, jnp.sum(series * series, 1, keepdims=True), tile)
    tiles[core * g + m] = tile
    idx_all[m] = series

    @pl.when(jnp.logical_not(has_edge))
    def _():
        tiles[2 * g] = jnp.full((kcount, 128), FAR, f32)

    pl.semaphore_wait(barrier, 2 * g - 1 + beside + jnp.where(has_edge, 1, 0))

    for side in range(2):
        each(1 - side, g, lambda s, side=side: tile_copy(side, s).start())
    each(1, g, lambda s: idx_copy(s).start())
    load.wait()
    for copy in inputs[1:]:
        copy.wait()
    small[0:1, 0 : cells // 2] = mask_ref[...].astype(f32)
    for piece in range(groups):
        own_copy(piece).start()
        each(1, g, lambda s, piece=piece: raw_copy(piece, s).start())
    for turn in range(groups - 2):
        tell_line(round_sem.at[turn])
        pl.semaphore_wait(round_sem.at[turn], beside)
    for side in range(2):
        each(1 - side, g, lambda s, side=side: tile_copy(side, s).wait_recv())

    @pl.when(has_edge)
    def _():
        edge_copy().start()

    zero_tile = jnp.zeros((kcount, 128), f32)
    zmsg[...] = lax.fori_loop(0, 2 * g, lambda at, carry: carry + tiles[at], zero_tile)
    each(1, groups, lambda s: z_copy(s).start())
    each(1, g, lambda s: idx_copy(s).wait_recv())

    spot = lax.broadcasted_iota(jnp.int32, (kcount, wide), 1)
    wing = jnp.zeros((kcount, 128), f32)
    tail = jnp.zeros((kcount, wide - 128), f32)

    def tile_at(order):
        inside = lax.rem(order, 2) * g + lax.div(order, 2)
        outside = jnp.logical_or(order < 0, order >= 2 * g)
        return tiles[jnp.where(outside, 2 * g, inside)]

    def window(member):
        order = member * 2 + core
        step = flipped(m, member, g)
        here = jnp.concatenate([idx_all[member], wing], 1)
        before = jnp.concatenate([tile_at(order - 1), tail], 1)
        after = jnp.concatenate([tile_at(order + 1), tail], 1)
        left = pltpu.roll(before, wide - REACH, 1)
        mid = pltpu.roll(here, REACH, 1)
        right = pltpu.roll(after, REACH + t_dev, 1)
        ext = jnp.where(spot < REACH, left, jnp.where(spot < REACH + t_dev, mid, right))
        for k in range(kcount):
            line = pltpu.roll(ext[k : k + 1], wide - REACH - MAXLAG + offset_ref[k], 1)
            line = jnp.broadcast_to(line, (BASE, wide))
            raw_win[step, k * BASE : (k + 1) * BASE, :] = pltpu.roll(
                line, 0, 1, stride=1, stride_axis=0
            )

    each(0, g - 1, lambda at: window(jnp.where(core == 0, g - 1 - at, at)))

    @pl.when(has_edge)
    def _():
        edge_copy().wait()

    window(jnp.where(core == 0, 0, g - 1))
    day = lax.broadcasted_iota(jnp.int32, (lanes, 128), 0)
    shift = lax.broadcasted_iota(jnp.int32, (lanes, 128), 1) - MAXLAG
    late = jnp.where((day >= t_dev - shift) & (day < t_dev), 1.0, 0.0)
    early = jnp.where(day < -shift, 1.0, 0.0)
    chooser[0] = jnp.where(core == 0, late, early).astype(jnp.bfloat16)
    chooser[1] = jnp.where(core == 0, early, late).astype(jnp.bfloat16)
    each(1, groups, lambda s: z_copy(s).wait_recv())
    stats = zmsg[...]
    for s in range(1, groups):
        stats = stats + zin[s]
    mean = stats[:, 62:63] / total_days
    var = stats[:, 63:64] / total_days - mean * mean
    outer = 1.0 / jnp.sqrt(var + 1e-06)

    place = lax.broadcasted_iota(jnp.int32, (kcount, lanes), 1)

    def centered(value, valid):
        return jnp.where(valid, (value - mean).astype(jnp.bfloat16).astype(f32), 0.0)

    def center_body(at, carry):
        return carry + centered(idx_all[at], place < t_dev)

    core_sum = lax.fori_loop(0, g, center_body, jnp.zeros((kcount, lanes), f32))
    inner_block = centered(idx_all[jnp.where(core == 0, 0, g - 1)], place < t_dev)
    edge = jnp.concatenate([tiles[2 * g], tail[:, : lanes - 128]], 1)
    edge = jnp.where(core == 0, pltpu.roll(edge, t_dev - 128, 1), edge)
    opens = jnp.where(core == 0, t_dev - 64, 0)
    closes = jnp.where(core == 0, t_dev, 62)
    outer_block = centered(edge, (place >= opens) & (place < closes) & (edge < NEAR))

    def part(value, side):
        return jnp.dot(
            value.astype(jnp.bfloat16), chooser[side], preferred_element_type=f32
        )

    by_shift = (
        jnp.sum(core_sum, 1, keepdims=True)
        + part(outer_block, 0)
        - part(inner_block, 1)
    )
    tot_part[...] = jnp.zeros_like(tot_part)
    for k in range(kcount):
        tot_part[k : k + 1, :] = pltpu.roll(
            by_shift[k : k + 1], lax.rem(128 - offset_ref[k], 128), 1
        )
    total_copy().start()

    def center_window(step):
        for k in range(kcount):
            value = raw_win[step, k * BASE : (k + 1) * BASE, :]
            value = jnp.where(value < NEAR, value - mean[k : k + 1], 0.0).astype(jnp.bfloat16)
            for turn in range(0, ROWS, BASE):
                turned = value if turn == 0 else pltpu.roll(value, turn, 1)
                win[step, k * ROWS + turn : k * ROWS + turn + BASE, :] = turned[:, :lanes]

    low = lax.broadcasted_iota(jnp.int32, (ROWS, 128), 1) < 64
    low_row = lax.broadcasted_iota(jnp.int32, (1, 128), 1) < 64

    def pair_cols(cols, k):
        return jnp.where(low, cols[0:ROWS, k : k + 1], cols[0:ROWS, k + half_k : k + half_k + 1])

    def halves(first_half, second_half, is_low):
        turned_first = pltpu.roll(first_half, 64, 1)
        turned_second = pltpu.roll(second_half, 64, 1)
        zeroth = jnp.where(is_low, first_half, turned_second)
        oneth = jnp.where(is_low, turned_first, second_half)
        return jnp.where(core == 0, zeroth, oneth), jnp.where(core == 0, oneth, zeroth)

    group_days = 2 * g * t_dev * 1.0
    sums_at = 2 * count

    def add(pieces, step, first_time):
        width = 128 * len(pieces)
        value = jnp.concatenate([recv[piece, step] for piece in pieces], 1)
        wide_value = value.astype(f32)
        sums = jnp.sum(wide_value, 0, keepdims=True)
        squares = jnp.sum(wide_value * wide_value, 0, keepdims=True)
        found = jnp.dot(win[step, :, :t_dev], value, preferred_element_type=f32)
        if first_time:
            acc[0:sums_at, :width] = found
            acc[sums_at : sums_at + 1, :width] = sums
            acc[sums_at + 1 : sums_at + 2, :width] = squares
        else:
            acc[0:sums_at, :width] += found
            acc[sums_at : sums_at + 1, :width] += sums
            acc[sums_at + 1 : sums_at + 2, :width] += squares

    def split(piece, column):
        column = slice(column * 128, column * 128 + 128)
        for row in range(2):
            value = acc[sums_at + row : sums_at + row + 1, column]
            kept, given = halves(value, value, low_row)
            mine[piece, count + row : count + row + 1, :] = kept
            other[piece, count + row : count + row + 1, :] = given
        swap_copy(piece, half_k).start()
        for k in range(half_k):
            at = k * ROWS
            kept, given = halves(
                acc[at : at + ROWS, column], acc[count + at : count + at + ROWS, column], low
            )
            mine[piece, at : at + ROWS, :] = kept
            other[piece, at : at + ROWS, :] = given
            swap_copy(piece, k).start()

    def products(piece):
        own_copy(piece).wait()
        add([piece], 0, True)

        def body(step, carry):
            raw_copy(piece, step).wait_recv()
            add([piece], step, False)
            return carry

        lax.fori_loop(1, g, body, 0)
        split(piece, 0)

    def joined(piece, k):
        at = k * ROWS
        swap_copy(piece, k).wait_recv()
        return mine[piece, at : at + ROWS, :] + partner_in[piece, at : at + ROWS, :]

    def joined_row(piece, row):
        at = count + row
        return mine[piece, at : at + 1, :] + partner_in[piece, at : at + 1, :]

    def decoded(slot, k):
        coded = got[slot, k * ROWS : (k + 1) * ROWS, :].astype(jnp.int32).astype(f32)
        return coded * (got_extra[slot, 2 + k : 3 + k, :] * (1.0 / TOP))

    def send_sums(piece, outer_slot):
        swap_copy(piece, half_k).wait_recv()
        sx, sq = joined_row(piece, 0), joined_row(piece, 1)
        tot, cols, days = own_tot, own_cols, group_days
        copies = sum_copies(piece, slot_of(piece))
        if outer_slot is not None:
            arriving = sum_copies(1, outer_slot)
            arriving[0].wait_recv()
            outer_x = got_extra[outer_slot, 0:1, :]
            outer_mean = outer_x / group_days
            sx, sq = sx + outer_x, sq + got_extra[outer_slot, 1:2, :]
            outer_tot = got_extra[outer_slot, EXTRA:, :]
            outer_cols = jnp.transpose(outer_tot)
            tot, cols, days = tot + outer_tot, cols + outer_cols, 2 * group_days
        sent_extra[piece, 0:1, :] = sx
        sent_extra[piece, 1:2, :] = sq
        local_mean = sx / days
        for k in range(half_k):
            value = joined(piece, k) - local_mean * pair_cols(cols, k)
            if outer_slot is not None:
                value = value + outer_mean * pair_cols(outer_cols, k)
            stage[k * ROWS : (k + 1) * ROWS, :] = value
            top = jnp.max(jnp.abs(value), 0, keepdims=True)
            if outer_slot is not None:
                top = top + got_extra[outer_slot, 2 + k : 3 + k, :]
            sent_extra[piece, 2 + k : 3 + k, :] = top
        sent_extra[piece, EXTRA:, :] = tot
        copies[0].start()
        for k in range(half_k):
            value = stage[k * ROWS : (k + 1) * ROWS, :]
            if outer_slot is not None:
                arriving[1 + k].wait_recv()
                value = value + decoded(outer_slot, k)
            scaled = value * (TOP / jnp.maximum(sent_extra[piece, 2 + k : 3 + k, :], 1e-30))
            sent[piece, k * ROWS : (k + 1) * ROWS, :] = (
                jnp.round(scaled).astype(jnp.int32).astype(jnp.int16)
            )
            copies[1 + k].start()

    def send_outer(piece):
        @pl.when(jnp.logical_not(inner))
        def _():
            send_sums(piece, None)

    def send_inner(piece, outer_slot):
        @pl.when(inner)
        def _():
            send_sums(piece, outer_slot)

    last = groups - 1
    own_copy(0).wait()
    each(1, g, lambda s: raw_copy(0, s).wait_recv())

    def early_body(step, first_time):
        center_window(step)
        add([0], step, first_time)

    early_body(0, True)
    if g <= 4:
        for step in range(1, g):
            early_body(step, False)
    else:
        each(1, g, lambda s: early_body(s, False))
    split(0, 0)

    total_copy().wait()
    own_tot = tot_part[...] + tot_in[...]
    own_cols = jnp.transpose(own_tot)
    send_outer(0)
    products(1)
    send_sums(1, None)
    send_inner(0, 0)
    products(2)
    send_outer(2)
    send_inner(2, 1)
    products(last)
    near_blocks, far_blocks = sum_copies(1, 2), sum_copies(1, 3)

    def opened(slot, copies, days):
        copies[0].wait_recv()
        far_x = got_extra[slot, 0:1, :]
        cols = jnp.transpose(got_extra[slot, EXTRA:, :])
        return far_x, got_extra[slot, 1:2, :], far_x / days, cols

    near_x, near_sq, near_mean, near_cols = opened(2, near_blocks, group_days)
    for k in range(half_k):
        near_blocks[1 + k].wait_recv()
        far[k * ROWS : (k + 1) * ROWS, :] = decoded(2, k) + near_mean * pair_cols(near_cols, k)
    swap_copy(last, half_k).wait_recv()
    far_x, far_sq, far_mean, far_cols = opened(3, far_blocks, 2 * group_days)
    mean_x = (joined_row(last, 0) + near_x + far_x) / total_days
    var_x = (joined_row(last, 1) + near_sq + far_sq) / total_days - mean_x * mean_x
    all_cols = own_cols + near_cols + far_cols
    mask = small[0:1, :]
    mask = mask + pltpu.roll(mask, 64, 1)
    inner = mask / (total_days * jnp.sqrt(var_x + 1e-06))
    for k in range(half_k):
        at = k * ROWS
        far[at : at + ROWS, :] += (
            joined(last, k)
            + far_mean * pair_cols(far_cols, k)
            - mean_x * pair_cols(all_cols, k)
        )

    def normal(k):
        far_blocks[1 + k].wait_recv()
        value = far[k * ROWS : (k + 1) * ROWS, :] + decoded(3, k)
        scale = jnp.where(low_row, outer[k : k + 1], outer[k + half_k : k + half_k + 1])
        return value * (inner * scale)

    small_int = lag_ref[...] + MAXLAG
    small[0:1, 0 : lag_ref.shape[1]] = small_int.astype(f32)
    chosen = jnp.broadcast_to(small[0:1, :].astype(jnp.int32), (64, 128))
    kept = lag_ref.shape[1]

    def out_copy(k):
        return pltpu.make_async_copy(out_buf.at[k], out_ref.at[k], out_sem.at[0])

    for k in range(0, half_k, 2):
        upper_rows = normal(k)
        under_rows = normal(k + 1) if k + 1 < half_k else upper_rows
        flat = jnp.transpose(jnp.concatenate([upper_rows, under_rows], 0))
        for side in range(2):
            rows = flat[side * 64 : (side + 1) * 64, :]
            for turn in range(min(2, half_k - k)):
                at = k + turn + side * half_k
                out_buf[at] = jnp.take_along_axis(rows, chosen + 64 * turn, axis=1)[:, :kept]
                out_copy(at).start()
    def drained(ref, sem):
        remote(ref, ref, sem, sem, partner).wait_send()

    drained(idx_all.at[pl.ds(0, g - 1)], idx_send.at[0])
    drained(tiles.at[pl.ds(0, 2 * g - 1)], tile_send.at[0])
    drained(zin.at[pl.ds(0, groups - 1)], z_send.at[0])
    for piece in range(groups):
        drained(recv.at[piece, pl.ds(0, g - 1)], raw_send.at[piece])
        drained(other.at[piece], swap_send.at[piece])
        if piece < last:
            drained(sent.at[piece], sum_send.at[0, piece])
            drained(sent_extra.at[piece], sum_send.at[1, piece])
    pltpu.make_async_copy(out_buf, out_ref, out_sem.at[0]).wait()


def shards(field, index, lag_list, index_offset, sea_mask):
    t_dev, cells_all = field.shape
    devices = lax.axis_size("tm")
    kcount = index.shape[1]
    lanes = round_up(t_dev, 128)
    groups = GROUPS
    g = devices // 2 // groups
    rows = kcount * ROWS
    half = rows // 2
    sizes = (devices, t_dev, kcount, groups, g)
    dma = pltpu.SemaphoreType.DMA
    f32 = jnp.float32
    maps = pl.pallas_call(
        functools.partial(kernel, sizes),
        out_shape=jax.ShapeDtypeStruct((kcount, 64, lag_list.shape[0]), f32),
        in_specs=[pl.BlockSpec(memory_space=pl.ANY)] * 5,
        out_specs=pl.BlockSpec(memory_space=pl.ANY),
        scratch_shapes=[
            pltpu.VMEM((kcount, t_dev), f32),
            pltpu.VMEM((1, lag_list.shape[0]), jnp.int32),
            pltpu.SMEM((kcount,), jnp.int32),
            pltpu.VMEM((1, sea_mask.shape[0]), jnp.int32),
            pltpu.VMEM((t_dev, cells_all), jnp.bfloat16),
            pltpu.VMEM((kcount, lanes), f32),
            pltpu.VMEM((g, kcount, lanes), f32),
            pltpu.VMEM((2 * g + 1, kcount, 128), f32),
            pltpu.VMEM((kcount, 128), f32),
            pltpu.VMEM((groups, kcount, 128), f32),
            pltpu.VMEM((groups, g, t_dev, 128), jnp.bfloat16),
            pltpu.VMEM((g, kcount * BASE, lanes + 128), f32),
            pltpu.VMEM((g, rows, lanes), jnp.bfloat16),
            pltpu.VMEM((rows + EXTRA, 256), f32),
            pltpu.VMEM((groups, half + EXTRA, 128), f32),
            pltpu.VMEM((groups, half + EXTRA, 128), f32),
            pltpu.VMEM((groups, half + EXTRA, 128), f32),
            pltpu.VMEM((groups, half, 128), jnp.int16),
            pltpu.VMEM((groups, EXTRA + 16, 128), f32),
            pltpu.VMEM((groups, half, 128), jnp.int16),
            pltpu.VMEM((groups, EXTRA + 16, 128), f32),
            pltpu.VMEM((half, 128), f32),
            pltpu.VMEM((half, 128), f32),
            pltpu.VMEM((2, lanes, 128), jnp.bfloat16),
            pltpu.VMEM((kcount, 64, lag_list.shape[0]), f32),
            pltpu.VMEM((8, 128), f32),
            pltpu.VMEM((16, 128), f32),
            pltpu.VMEM((16, 128), f32),
            dma((groups,)),
            dma((groups, g - 1)),
            dma((1,)),
            dma((g - 1,)),
            dma((1,)),
            dma((2 * g - 1,)),
            dma((4,)),
            dma((1,)),
            dma((groups - 1,)),
            dma((groups,)),
            dma((groups, kcount // 2 + 1)),
            dma((2, groups - 1)),
            dma((kcount // 2 + 1, groups)),
            dma((groups + 1,)),
            pltpu.SemaphoreType.REGULAR((groups - 2,)),
            dma((1,)),
            dma((4,)),
        ],
        compiler_params=pltpu.CompilerParams(
            collective_id=0, has_side_effects=True, vmem_limit_bytes=60 * 1024 * 1024
        ),
    )(field, index.T, lag_list[None, :], index_offset, sea_mask[None, :])
    return jnp.transpose(maps, (1, 0, 2))


def solution(mesh):
    return jax.shard_map(
        shards,
        mesh=mesh,
        in_specs=(P("tm", None), P("tm", None), P(), P(), P("tm")),
        out_specs=P("tm", None, None),
        check_vma=False,
    )
```

```python
import functools

import jax
import jax.numpy as jnp
from jax import lax
from jax.experimental import pallas as pl
from jax.experimental.pallas import tpu as pltpu
from jax.sharding import PartitionSpec as P

MAXLAG = 30
MAXOFF = 14
REACH = 64
ROWS = 64
BASE = 16
EXTRA = 8
TOP = 32767.0
FAR = 1e30
NEAR = 1e29
GROUPS = 4
MESH = pl.DeviceIdType.MESH


def round_up(value, unit):
    return -(-value // unit) * unit


def kernel(
    sizes,
    field_hbm,
    index_hbm,
    lag_hbm,
    offset_hbm,
    mask_hbm,
    out_ref,
    index_ref,
    lag_ref,
    offset_ref,
    mask_ref,
    field_ref,
    idx_ref,
    pack_ref,
    packs,
    idx_all,
    tiles,
    zmsg,
    zin,
    recv,
    raw_win,
    win,
    acc,
    mine,
    other,
    partner_in,
    sent,
    sent_extra,
    got,
    got_extra,
    far,
    stage,
    chooser,
    out_buf,
    small,
    tot_part,
    tot_in,
    raw_send,
    raw_recv,
    idx_send,
    idx_recv,
    tile_send,
    tile_recv,
    lone_sem,
    z_send,
    z_recv,
    swap_send,
    swap_recv,
    sum_send,
    sum_recv,
    own_sem,
    round_sem,
    out_sem,
    in_sem,
):
    devices, t_dev, kcount, groups, g = sizes
    lanes = idx_ref.shape[1]
    wide = lanes + 128
    half_k = kcount // 2
    spare = [
        ((row - 8) * (lanes // 128) + column, row, column * 128)
        for row in range(8, kcount)
        for column in range(lanes // 128)
    ]
    count = half_k * ROWS
    cells = 128
    me = lax.axis_index("tm")
    core = lax.rem(me, 2)
    chip = lax.div(me, 2)
    h = lax.div(chip, g)
    m = lax.rem(chip, g)
    partner = chip * 2 + (1 - core)
    edge_peer = ((h + 2 * core - 1) * g + m) * 2 + (1 - core)
    has_edge = jnp.where(core == 0, h > 0, h < groups - 1)
    f32 = jnp.float32
    total_days = devices * t_dev * 1.0

    def flipped(value, step, size):
        found, bit = 0, 1
        while bit < size:
            flip = lax.rem(lax.div(value, bit) + lax.div(step, bit), 2)
            found, bit = found + flip * bit, bit * 2
        return found

    def across(step):
        return flipped(m, step, g)

    def device_of(group, member):
        return (group * g + member) * 2 + core

    def remote(src, dst, send, recv_s, device):
        return pltpu.make_async_remote_copy(
            src_ref=src,
            dst_ref=dst,
            send_sem=send,
            recv_sem=recv_s,
            device_id=(device,),
            device_id_type=MESH,
        )

    def block(at):
        return field_ref.at[:, pl.ds(pl.multiple_of(at * cells, cells), cells)]

    inner = jnp.logical_or(h == 1, h == 2)
    upper = lax.div(h, 2)
    beside_h = h + 1 - 2 * lax.rem(h, 2)

    def plane_of(piece):
        if piece == 0:
            return (groups - 1) * (1 - upper)
        if piece == 1:
            return jnp.where(inner, beside_h, 2 - upper)
        return jnp.where(inner, 2 - upper, beside_h) if piece == 2 else h

    def raw_copy(piece, step):
        to = across(step)
        return remote(
            block(plane_of(piece) * g + to),
            recv.at[piece, step],
            raw_send.at[piece],
            raw_recv.at[piece, step - 1],
            device_of(h, to),
        )

    def own_copy(piece):
        return pltpu.make_async_copy(
            block(plane_of(piece) * g + m), recv.at[piece, 0], own_sem.at[piece]
        )

    def idx_copy(step):
        return remote(
            pack_ref,
            packs.at[m],
            idx_send.at[0],
            idx_recv.at[step - 1],
            device_of(h, across(step)),
        )

    def tile_copy(side, step):
        to = (h * g + across(step)) * 2 + (core if side == 0 else 1 - core)
        tile = tiles.at[core * g + m]
        return remote(
            tile, tile, tile_send.at[0], tile_recv.at[side * g + step - 1], to
        )

    def edge_copy():
        return remote(
            tiles.at[jnp.where(core == 0, 0, 2 * g - 1)],
            tiles.at[2 * g],
            lone_sem.at[0],
            lone_sem.at[1],
            edge_peer,
        )

    def total_copy():
        return remote(tot_part, tot_in, lone_sem.at[2], lone_sem.at[3], partner)

    def z_copy(step):
        return remote(
            zmsg,
            zin.at[step],
            z_send.at[0],
            z_recv.at[step - 1],
            device_of(flipped(h, step, groups), m),
        )

    def swap_copy(piece, k):
        rows = pl.ds(k * ROWS, ROWS if k < half_k else EXTRA)
        return remote(
            other.at[piece, rows],
            partner_in.at[piece, rows],
            swap_send.at[piece],
            swap_recv.at[piece, k],
            partner,
        )

    def slot_of(piece):
        return jnp.where(inner, (3, 2, 3)[piece], piece)

    def receiver(piece):
        if piece == 1:
            return device_of(beside_h, m)
        return device_of(jnp.where(inner, plane_of(piece), beside_h), m)

    def sum_copies(piece, slot):
        copies = [
            remote(
                sent_extra.at[piece],
                got_extra.at[slot],
                sum_send.at[1, piece],
                sum_recv.at[half_k, slot],
                receiver(piece),
            )
        ]
        for k in range(half_k):
            rows = pl.ds(k * ROWS, ROWS)
            copies.append(
                remote(
                    sent.at[piece, rows],
                    got.at[slot, rows],
                    sum_send.at[0, piece],
                    sum_recv.at[k, slot],
                    receiver(piece),
                )
            )
        return copies

    def each(low_step, high_step, act):
        def body(step, carry):
            act(step)
            return carry

        lax.fori_loop(low_step, high_step, body, 0)

    load = pltpu.make_async_copy(field_hbm, field_ref, own_sem.at[groups])
    inputs = [
        pltpu.make_async_copy(src, dst, in_sem.at[at])
        for at, (src, dst) in enumerate(
            (
                (index_hbm, index_ref),
                (lag_hbm, lag_ref),
                (offset_hbm, offset_ref),
                (mask_hbm, mask_ref),
            )
        )
    ]
    barrier = pltpu.get_barrier_semaphore()

    def tell(sem, device):
        pl.semaphore_signal(sem, inc=1, device_id=(device,), device_id_type=MESH)

    def tell_line(sem):
        @pl.when(h > 0)
        def _():
            tell(sem, device_of(h - 1, m))

        @pl.when(h < groups - 1)
        def _():
            tell(sem, device_of(h + 1, m))

    beside = jnp.where(h > 0, 1, 0) + jnp.where(h < groups - 1, 1, 0)
    tell_line(barrier)

    @pl.when(has_edge)
    def _():
        tell(barrier, edge_peer)

    each(1, 2 * g, lambda s: tell(barrier, (h * g + across(lax.div(s, 2))) * 2 + lax.rem(core + s, 2)))
    inputs[0].start()
    load.start()
    for copy in inputs[1:]:
        copy.start()
    idx_ref[...] = jnp.zeros_like(idx_ref)
    other[...] = jnp.zeros_like(other)
    sent_extra[...] = jnp.zeros_like(sent_extra)
    small[...] = jnp.zeros_like(small)
    inputs[0].wait()
    idx_ref[0:kcount, 0:t_dev] = index_ref[...]
    lane = lax.broadcasted_iota(jnp.int32, (kcount, 128), 1)
    series = idx_ref[...]
    tile = jnp.where(
        lane < 64, series[:, :128], pltpu.roll(series, (128 - t_dev) % lanes, 1)[:, :128]
    )
    tile = jnp.where(lane == 62, jnp.sum(series, 1, keepdims=True), tile)
    tile = jnp.where(lane == 63, jnp.sum(series * series, 1, keepdims=True), tile)
    tiles[core * g + m] = tile
    idx_all[m] = series
    pack_ref[:, :lanes] = series[:8]
    pack_ref[:, lanes:] = jnp.zeros((8, 128), f32)
    for at, row, column in spare:
        pack_ref[at : at + 1, lanes:] = series[row : row + 1, column : column + 128]

    @pl.when(jnp.logical_not(has_edge))
    def _():
        tiles[2 * g] = jnp.full((kcount, 128), FAR, f32)

    pl.semaphore_wait(barrier, 2 * g - 1 + beside + jnp.where(has_edge, 1, 0))

    for side in range(2):
        each(1 - side, g, lambda s, side=side: tile_copy(side, s).start())
    each(1, g, lambda s: idx_copy(s).start())
    load.wait()
    for copy in inputs[1:]:
        copy.wait()
    small[0:1, 0 : cells // 2] = mask_ref[...].astype(f32)
    for piece in range(groups):
        own_copy(piece).start()
        each(1, g, lambda s, piece=piece: raw_copy(piece, g - s).start())
    for turn in range(groups - 2):
        tell_line(round_sem.at[turn])
        pl.semaphore_wait(round_sem.at[turn], beside)
    for side in range(2):
        each(1 - side, g, lambda s, side=side: tile_copy(side, s).wait_recv())

    @pl.when(has_edge)
    def _():
        edge_copy().start()

    zero_tile = jnp.zeros((kcount, 128), f32)
    zmsg[...] = lax.fori_loop(0, 2 * g, lambda at, carry: carry + tiles[at], zero_tile)
    each(1, groups, lambda s: z_copy(s).start())

    def unpack(step):
        member = across(step)
        idx_copy(step).wait_recv()
        idx_all[member, 0:8, :] = packs[member, :, :lanes]
        for at, row, column in spare:
            idx_all[member, row : row + 1, column : column + 128] = packs[
                member, at : at + 1, lanes:
            ]

    each(1, g, unpack)

    spot = lax.broadcasted_iota(jnp.int32, (kcount, wide), 1)
    wing = jnp.zeros((kcount, 128), f32)
    tail = jnp.zeros((kcount, wide - 128), f32)

    def tile_at(order):
        inside = lax.rem(order, 2) * g + lax.div(order, 2)
        outside = jnp.logical_or(order < 0, order >= 2 * g)
        return tiles[jnp.where(outside, 2 * g, inside)]

    def window(member):
        order = member * 2 + core
        step = flipped(m, member, g)
        here = jnp.concatenate([idx_all[member], wing], 1)
        before = jnp.concatenate([tile_at(order - 1), tail], 1)
        after = jnp.concatenate([tile_at(order + 1), tail], 1)
        left = pltpu.roll(before, wide - REACH, 1)
        mid = pltpu.roll(here, REACH, 1)
        right = pltpu.roll(after, REACH + t_dev, 1)
        ext = jnp.where(spot < REACH, left, jnp.where(spot < REACH + t_dev, mid, right))
        for k in range(kcount):
            line = pltpu.roll(ext[k : k + 1], wide - REACH - MAXLAG + offset_ref[k], 1)
            line = jnp.broadcast_to(line, (BASE, wide))
            raw_win[step, k * BASE : (k + 1) * BASE, :] = pltpu.roll(
                line, 0, 1, stride=1, stride_axis=0
            )

    each(0, g - 1, lambda at: window(jnp.where(core == 0, g - 1 - at, at)))

    @pl.when(has_edge)
    def _():
        edge_copy().wait()

    window(jnp.where(core == 0, 0, g - 1))
    day = lax.broadcasted_iota(jnp.int32, (lanes, 128), 0)
    shift = lax.broadcasted_iota(jnp.int32, (lanes, 128), 1) - MAXLAG
    late = jnp.where((day >= t_dev - shift) & (day < t_dev), 1.0, 0.0)
    early = jnp.where(day < -shift, 1.0, 0.0)
    chooser[0] = jnp.where(core == 0, late, early).astype(jnp.bfloat16)
    chooser[1] = jnp.where(core == 0, early, late).astype(jnp.bfloat16)
    each(1, groups, lambda s: z_copy(s).wait_recv())
    stats = zmsg[...]
    for s in range(1, groups):
        stats = stats + zin[s]
    mean = stats[:, 62:63] / total_days
    var = stats[:, 63:64] / total_days - mean * mean
    outer = 1.0 / jnp.sqrt(var + 1e-06)

    def center_window(step):
        for k in range(kcount):
            value = raw_win[step, k * BASE : (k + 1) * BASE, :]
            value = jnp.where(value < NEAR, value - mean[k : k + 1], 0.0).astype(jnp.bfloat16)
            for turn in range(0, ROWS, BASE):
                turned = value if turn == 0 else pltpu.roll(value, turn, 1)
                win[step, k * ROWS + turn : k * ROWS + turn + BASE, :] = turned[:, :lanes]

    low = lax.broadcasted_iota(jnp.int32, (ROWS, 128), 1) < 64
    low_row = lax.broadcasted_iota(jnp.int32, (1, 128), 1) < 64

    def pair_cols(cols, k):
        return jnp.where(low, cols[0:ROWS, k : k + 1], cols[0:ROWS, k + half_k : k + half_k + 1])

    def halves(first_half, second_half, is_low):
        turned_first = pltpu.roll(first_half, 64, 1)
        turned_second = pltpu.roll(second_half, 64, 1)
        zeroth = jnp.where(is_low, first_half, turned_second)
        oneth = jnp.where(is_low, turned_first, second_half)
        return jnp.where(core == 0, zeroth, oneth), jnp.where(core == 0, oneth, zeroth)

    group_days = 2 * g * t_dev * 1.0
    sums_at = 2 * count

    def add(pieces, step, first_time):
        width = 128 * len(pieces)
        value = jnp.concatenate([recv[piece, step] for piece in pieces], 1)
        wide_value = value.astype(f32)
        sums = jnp.sum(wide_value, 0, keepdims=True)
        squares = jnp.sum(wide_value * wide_value, 0, keepdims=True)
        found = jnp.dot(win[step, :, :t_dev], value, preferred_element_type=f32)
        if first_time:
            acc[0:sums_at, :width] = found
            acc[sums_at : sums_at + 1, :width] = sums
            acc[sums_at + 1 : sums_at + 2, :width] = squares
        else:
            acc[0:sums_at, :width] += found
            acc[sums_at : sums_at + 1, :width] += sums
            acc[sums_at + 1 : sums_at + 2, :width] += squares

    def split(piece, column):
        column = slice(column * 128, column * 128 + 128)
        for row in range(2):
            value = acc[sums_at + row : sums_at + row + 1, column]
            kept, given = halves(value, value, low_row)
            mine[piece, count + row : count + row + 1, :] = kept
            other[piece, count + row : count + row + 1, :] = given
        swap_copy(piece, half_k).start()
        for k in range(half_k):
            at = k * ROWS
            kept, given = halves(
                acc[at : at + ROWS, column], acc[count + at : count + at + ROWS, column], low
            )
            mine[piece, at : at + ROWS, :] = kept
            other[piece, at : at + ROWS, :] = given
            swap_copy(piece, k).start()

    def products(piece):
        own_copy(piece).wait()
        add([piece], 0, True)

        def body(turn, carry):
            step = g - turn
            raw_copy(piece, step).wait_recv()
            add([piece], step, False)
            return carry

        lax.fori_loop(1, g, body, 0)
        split(piece, 0)

    def joined(piece, k):
        at = k * ROWS
        swap_copy(piece, k).wait_recv()
        return mine[piece, at : at + ROWS, :] + partner_in[piece, at : at + ROWS, :]

    def joined_row(piece, row):
        at = count + row
        return mine[piece, at : at + 1, :] + partner_in[piece, at : at + 1, :]

    def decoded(slot, k):
        coded = got[slot, k * ROWS : (k + 1) * ROWS, :].astype(jnp.int32).astype(f32)
        return coded * (got_extra[slot, 2 + k : 3 + k, :] * (1.0 / TOP))

    def send_sums(piece, outer_slot):
        swap_copy(piece, half_k).wait_recv()
        sx, sq = joined_row(piece, 0), joined_row(piece, 1)
        tot, cols, days = own_tot, own_cols, group_days
        copies = sum_copies(piece, slot_of(piece))
        if outer_slot is not None:
            arriving = sum_copies(1, outer_slot)
            arriving[0].wait_recv()
            outer_x = got_extra[outer_slot, 0:1, :]
            outer_mean = outer_x / group_days
            sx, sq = sx + outer_x, sq + got_extra[outer_slot, 1:2, :]
            outer_tot = got_extra[outer_slot, EXTRA:, :]
            outer_cols = jnp.transpose(outer_tot)
            tot, cols, days = tot + outer_tot, cols + outer_cols, 2 * group_days
        sent_extra[piece, 0:1, :] = sx
        sent_extra[piece, 1:2, :] = sq
        local_mean = sx / days
        for k in range(half_k):
            value = joined(piece, k) - local_mean * pair_cols(cols, k)
            if outer_slot is not None:
                value = value + outer_mean * pair_cols(outer_cols, k)
            stage[k * ROWS : (k + 1) * ROWS, :] = value
            top = jnp.max(jnp.abs(value), 0, keepdims=True)
            if outer_slot is not None:
                top = top + got_extra[outer_slot, 2 + k : 3 + k, :]
            sent_extra[piece, 2 + k : 3 + k, :] = top
        sent_extra[piece, EXTRA:, :] = tot
        copies[0].start()
        for k in range(half_k):
            value = stage[k * ROWS : (k + 1) * ROWS, :]
            if outer_slot is not None:
                arriving[1 + k].wait_recv()
                value = value + decoded(outer_slot, k)
            scaled = value * (TOP / jnp.maximum(sent_extra[piece, 2 + k : 3 + k, :], 1e-30))
            sent[piece, k * ROWS : (k + 1) * ROWS, :] = (
                jnp.round(scaled).astype(jnp.int32).astype(jnp.int16)
            )
            copies[1 + k].start()

    def send_outer(piece):
        @pl.when(jnp.logical_not(inner))
        def _():
            send_sums(piece, None)

    def send_inner(piece, outer_slot):
        @pl.when(inner)
        def _():
            send_sums(piece, outer_slot)

    last = groups - 1
    own_copy(0).wait()
    each(1, g, lambda s: raw_copy(0, s).wait_recv())

    def early_body(step, first_time):
        center_window(step)
        add([0], step, first_time)

    early_body(0, True)

    place = lax.broadcasted_iota(jnp.int32, (kcount, lanes), 1)

    def centered(value, valid):
        return jnp.where(valid, (value - mean).astype(jnp.bfloat16).astype(f32), 0.0)

    def center_body(at, carry):
        return carry + centered(idx_all[at], place < t_dev)

    core_sum = jnp.zeros((kcount, lanes), f32)
    if g <= 4:
        for at in range(g):
            core_sum = center_body(at, core_sum)
    else:
        core_sum = lax.fori_loop(0, g, center_body, core_sum)
    inner_block = centered(idx_all[jnp.where(core == 0, 0, g - 1)], place < t_dev)
    edge = jnp.concatenate([tiles[2 * g], tail[:, : lanes - 128]], 1)
    edge = jnp.where(core == 0, pltpu.roll(edge, t_dev - 128, 1), edge)
    opens = jnp.where(core == 0, t_dev - 64, 0)
    closes = jnp.where(core == 0, t_dev, 62)
    outer_block = centered(edge, (place >= opens) & (place < closes) & (edge < NEAR))

    def part(value, side):
        return jnp.dot(
            value.astype(jnp.bfloat16), chooser[side], preferred_element_type=f32
        )

    by_shift = (
        jnp.sum(core_sum, 1, keepdims=True)
        + part(outer_block, 0)
        - part(inner_block, 1)
    )
    tot_part[...] = jnp.zeros_like(tot_part)
    for k in range(kcount):
        tot_part[k : k + 1, :] = pltpu.roll(
            by_shift[k : k + 1], lax.rem(128 - offset_ref[k], 128), 1
        )

    if g <= 4:
        for step in range(1, g):
            early_body(step, False)
    else:
        each(1, g, lambda s: early_body(s, False))
    total_copy().start()
    split(0, 0)

    total_copy().wait()
    own_tot = tot_part[...] + tot_in[...]
    own_cols = jnp.transpose(own_tot)
    send_outer(0)
    products(1)
    send_sums(1, None)
    send_inner(0, 0)
    products(2)
    send_outer(2)
    send_inner(2, 1)
    products(last)
    near_blocks, far_blocks = sum_copies(1, 2), sum_copies(1, 3)

    def opened(slot, copies, days):
        copies[0].wait_recv()
        far_x = got_extra[slot, 0:1, :]
        cols = jnp.transpose(got_extra[slot, EXTRA:, :])
        return far_x, got_extra[slot, 1:2, :], far_x / days, cols

    near_x, near_sq, near_mean, near_cols = opened(2, near_blocks, group_days)
    for k in range(half_k):
        near_blocks[1 + k].wait_recv()
        far[k * ROWS : (k + 1) * ROWS, :] = decoded(2, k) + near_mean * pair_cols(near_cols, k)
    swap_copy(last, half_k).wait_recv()
    far_x, far_sq, far_mean, far_cols = opened(3, far_blocks, 2 * group_days)
    mean_x = (joined_row(last, 0) + near_x + far_x) / total_days
    var_x = (joined_row(last, 1) + near_sq + far_sq) / total_days - mean_x * mean_x
    all_cols = own_cols + near_cols + far_cols
    mask = small[0:1, :]
    mask = mask + pltpu.roll(mask, 64, 1)
    scaling = mask / (total_days * jnp.sqrt(var_x + 1e-06))
    for k in range(half_k):
        at = k * ROWS
        far[at : at + ROWS, :] += (
            joined(last, k)
            + far_mean * pair_cols(far_cols, k)
            - mean_x * pair_cols(all_cols, k)
        )

    def normal(k):
        far_blocks[1 + k].wait_recv()
        value = far[k * ROWS : (k + 1) * ROWS, :] + decoded(3, k)
        scale = jnp.where(low_row, outer[k : k + 1], outer[k + half_k : k + half_k + 1])
        return value * (scaling * scale)

    small_int = lag_ref[...] + MAXLAG
    small[0:1, 0 : lag_ref.shape[1]] = small_int.astype(f32)
    chosen = jnp.broadcast_to(small[0:1, :].astype(jnp.int32), (64, 128))
    kept = lag_ref.shape[1]

    def out_copy(k):
        return pltpu.make_async_copy(out_buf.at[k], out_ref.at[k], out_sem.at[0])

    for k in range(0, half_k, 2):
        upper_rows = normal(k)
        under_rows = normal(k + 1) if k + 1 < half_k else upper_rows
        flat = jnp.transpose(jnp.concatenate([upper_rows, under_rows], 0))
        for side in range(2):
            rows = flat[side * 64 : (side + 1) * 64, :]
            for turn in range(min(2, half_k - k)):
                at = k + turn + side * half_k
                out_buf[at] = jnp.take_along_axis(rows, chosen + 64 * turn, axis=1)[:, :kept]
                out_copy(at).start()
    def drained(ref, sem):
        remote(ref, ref, sem, sem, partner).wait_send()

    drained(packs.at[pl.ds(0, g - 1)], idx_send.at[0])
    drained(tiles.at[pl.ds(0, 2 * g - 1)], tile_send.at[0])
    drained(zin.at[pl.ds(0, groups - 1)], z_send.at[0])
    for piece in range(groups):
        drained(recv.at[piece, pl.ds(0, g - 1)], raw_send.at[piece])
        drained(other.at[piece], swap_send.at[piece])
        if piece < last:
            drained(sent.at[piece], sum_send.at[0, piece])
            drained(sent_extra.at[piece], sum_send.at[1, piece])
    pltpu.make_async_copy(out_buf, out_ref, out_sem.at[0]).wait()


def shards(field, index, lag_list, index_offset, sea_mask):
    t_dev, cells_all = field.shape
    devices = lax.axis_size("tm")
    kcount = index.shape[1]
    lanes = round_up(t_dev, 128)
    groups = GROUPS
    g = devices // 2 // groups
    rows = kcount * ROWS
    half = rows // 2
    sizes = (devices, t_dev, kcount, groups, g)
    dma = pltpu.SemaphoreType.DMA
    f32 = jnp.float32
    maps = pl.pallas_call(
        functools.partial(kernel, sizes),
        out_shape=jax.ShapeDtypeStruct((kcount, 64, lag_list.shape[0]), f32),
        in_specs=[pl.BlockSpec(memory_space=pl.ANY)] * 5,
        out_specs=pl.BlockSpec(memory_space=pl.ANY),
        scratch_shapes=[
            pltpu.VMEM((kcount, t_dev), f32),
            pltpu.VMEM((1, lag_list.shape[0]), jnp.int32),
            pltpu.SMEM((kcount,), jnp.int32),
            pltpu.VMEM((1, sea_mask.shape[0]), jnp.int32),
            pltpu.VMEM((t_dev, cells_all), jnp.bfloat16),
            pltpu.VMEM((kcount, lanes), f32),
            pltpu.VMEM((8, lanes + 128), f32),
            pltpu.VMEM((g, 8, lanes + 128), f32),
            pltpu.VMEM((g, kcount, lanes), f32),
            pltpu.VMEM((2 * g + 1, kcount, 128), f32),
            pltpu.VMEM((kcount, 128), f32),
            pltpu.VMEM((groups, kcount, 128), f32),
            pltpu.VMEM((groups, g, t_dev, 128), jnp.bfloat16),
            pltpu.VMEM((g, kcount * BASE, lanes + 128), f32),
            pltpu.VMEM((g, rows, lanes), jnp.bfloat16),
            pltpu.VMEM((rows + EXTRA, 256), f32),
            pltpu.VMEM((groups, half + EXTRA, 128), f32),
            pltpu.VMEM((groups, half + EXTRA, 128), f32),
            pltpu.VMEM((groups, half + EXTRA, 128), f32),
            pltpu.VMEM((groups, half, 128), jnp.int16),
            pltpu.VMEM((groups, EXTRA + 16, 128), f32),
            pltpu.VMEM((groups, half, 128), jnp.int16),
            pltpu.VMEM((groups, EXTRA + 16, 128), f32),
            pltpu.VMEM((half, 128), f32),
            pltpu.VMEM((half, 128), f32),
            pltpu.VMEM((2, lanes, 128), jnp.bfloat16),
            pltpu.VMEM((kcount, 64, lag_list.shape[0]), f32),
            pltpu.VMEM((8, 128), f32),
            pltpu.VMEM((16, 128), f32),
            pltpu.VMEM((16, 128), f32),
            dma((groups,)),
            dma((groups, g - 1)),
            dma((1,)),
            dma((g - 1,)),
            dma((1,)),
            dma((2 * g - 1,)),
            dma((4,)),
            dma((1,)),
            dma((groups - 1,)),
            dma((groups,)),
            dma((groups, kcount // 2 + 1)),
            dma((2, groups - 1)),
            dma((kcount // 2 + 1, groups)),
            dma((groups + 1,)),
            pltpu.SemaphoreType.REGULAR((groups - 2,)),
            dma((1,)),
            dma((4,)),
        ],
        compiler_params=pltpu.CompilerParams(
            collective_id=0, has_side_effects=True, vmem_limit_bytes=60 * 1024 * 1024
        ),
    )(field, index.T, lag_list[None, :], index_offset, sea_mask[None, :])
    return jnp.transpose(maps, (1, 0, 2))


def solution(mesh):
    return jax.shard_map(
        shards,
        mesh=mesh,
        in_specs=(P("tm", None), P("tm", None), P(), P(), P("tm")),
        out_specs=P("tm", None, None),
        check_vma=False,
    )
```

```python
import functools

import jax
import jax.numpy as jnp
from jax import lax
from jax.experimental import pallas as pl
from jax.experimental.pallas import tpu as pltpu
from jax.sharding import PartitionSpec as P

MAXLAG = 30
MAXOFF = 14
REACH = 64
ROWS = 64
BASE = 16
EXTRA = 8
TOP = 32767.0
FAR = 1e30
NEAR = 1e29
GROUPS = 4
MESH = pl.DeviceIdType.MESH


def round_up(value, unit):
    return -(-value // unit) * unit


def kernel(
    sizes,
    field_hbm,
    index_hbm,
    lag_hbm,
    offset_hbm,
    mask_hbm,
    out_ref,
    index_ref,
    lag_ref,
    offset_ref,
    mask_ref,
    field_ref,
    idx_ref,
    pack_ref,
    packs,
    idx_all,
    tiles,
    zmsg,
    zin,
    recv,
    raw_win,
    win,
    acc,
    mine,
    other,
    partner_in,
    sent,
    sent_extra,
    got,
    got_extra,
    far,
    stage,
    chooser,
    out_buf,
    small,
    tot_part,
    tot_in,
    raw_send,
    raw_recv,
    idx_send,
    idx_recv,
    tile_send,
    tile_recv,
    lone_sem,
    z_send,
    z_recv,
    swap_send,
    swap_recv,
    sum_send,
    sum_recv,
    own_sem,
    round_sem,
    out_sem,
    in_sem,
):
    devices, t_dev, kcount, groups, g = sizes
    lanes = idx_ref.shape[1]
    wide = lanes + 128
    half_k = kcount // 2
    spare = [
        ((row - 8) * (lanes // 128) + column, row, column * 128)
        for row in range(8, kcount)
        for column in range(lanes // 128)
    ]
    count = half_k * ROWS
    cells = 128
    me = lax.axis_index("tm")
    core = lax.rem(me, 2)
    chip = lax.div(me, 2)
    h = lax.div(chip, g)
    m = lax.rem(chip, g)
    partner = chip * 2 + (1 - core)
    edge_peer = ((h + 2 * core - 1) * g + m) * 2 + (1 - core)
    has_edge = jnp.where(core == 0, h > 0, h < groups - 1)
    f32 = jnp.float32
    total_days = devices * t_dev * 1.0

    def flipped(value, step, size):
        found, bit = 0, 1
        while bit < size:
            flip = lax.rem(lax.div(value, bit) + lax.div(step, bit), 2)
            found, bit = found + flip * bit, bit * 2
        return found

    def across(step):
        return flipped(m, step, g)

    def device_of(group, member):
        return (group * g + member) * 2 + core

    def remote(src, dst, send, recv_s, device):
        return pltpu.make_async_remote_copy(
            src_ref=src,
            dst_ref=dst,
            send_sem=send,
            recv_sem=recv_s,
            device_id=(device,),
            device_id_type=MESH,
        )

    def block(at):
        return field_ref.at[:, pl.ds(pl.multiple_of(at * cells, cells), cells)]

    inner = jnp.logical_or(h == 1, h == 2)
    upper = lax.div(h, 2)
    beside_h = h + 1 - 2 * lax.rem(h, 2)

    def plane_of(piece):
        if piece == 0:
            return (groups - 1) * (1 - upper)
        if piece == 1:
            return jnp.where(inner, beside_h, 2 - upper)
        return jnp.where(inner, 2 - upper, beside_h) if piece == 2 else h

    def raw_copy(piece, step):
        to = across(step)
        return remote(
            block(plane_of(piece) * g + to),
            recv.at[piece, step],
            raw_send.at[piece],
            raw_recv.at[piece, step - 1],
            device_of(h, to),
        )

    def own_copy(piece):
        return pltpu.make_async_copy(
            block(plane_of(piece) * g + m), recv.at[piece, 0], own_sem.at[piece]
        )

    def idx_copy(step):
        return remote(
            pack_ref,
            packs.at[m],
            idx_send.at[0],
            idx_recv.at[step - 1],
            device_of(h, across(step)),
        )

    def tile_copy(side, step):
        to = (h * g + across(step)) * 2 + (core if side == 0 else 1 - core)
        tile = tiles.at[core * g + m]
        return remote(
            tile, tile, tile_send.at[0], tile_recv.at[side * g + step - 1], to
        )

    def edge_copy():
        return remote(
            tiles.at[jnp.where(core == 0, 0, 2 * g - 1)],
            tiles.at[2 * g],
            lone_sem.at[0],
            lone_sem.at[1],
            edge_peer,
        )

    def total_copy():
        return remote(tot_part, tot_in, lone_sem.at[2], lone_sem.at[3], partner)

    def z_copy(step):
        return remote(
            zmsg,
            zin.at[step],
            z_send.at[0],
            z_recv.at[step - 1],
            device_of(flipped(h, step, groups), m),
        )

    def swap_copy(piece, k):
        rows = pl.ds(k * ROWS, ROWS if k < half_k else EXTRA)
        return remote(
            other.at[piece, rows],
            partner_in.at[piece, rows],
            swap_send.at[piece],
            swap_recv.at[piece, k],
            partner,
        )

    def slot_of(piece):
        return jnp.where(inner, (3, 2, 3)[piece], piece)

    def receiver(piece):
        if piece == 1:
            return device_of(beside_h, m)
        return device_of(jnp.where(inner, plane_of(piece), beside_h), m)

    def sum_copies(piece, slot):
        copies = [
            remote(
                sent_extra.at[piece],
                got_extra.at[slot],
                sum_send.at[1, piece],
                sum_recv.at[half_k, slot],
                receiver(piece),
            )
        ]
        for k in range(half_k):
            rows = pl.ds(k * ROWS, ROWS)
            copies.append(
                remote(
                    sent.at[piece, rows],
                    got.at[slot, rows],
                    sum_send.at[0, piece],
                    sum_recv.at[k, slot],
                    receiver(piece),
                )
            )
        return copies

    def each(low_step, high_step, act):
        def body(step, carry):
            act(step)
            return carry

        lax.fori_loop(low_step, high_step, body, 0)

    load = pltpu.make_async_copy(field_hbm, field_ref, own_sem.at[groups])
    inputs = [
        pltpu.make_async_copy(src, dst, in_sem.at[at])
        for at, (src, dst) in enumerate(
            (
                (index_hbm, index_ref),
                (lag_hbm, lag_ref),
                (offset_hbm, offset_ref),
                (mask_hbm, mask_ref),
            )
        )
    ]
    barrier = pltpu.get_barrier_semaphore()

    def tell(sem, device):
        pl.semaphore_signal(sem, inc=1, device_id=(device,), device_id_type=MESH)

    def tell_line(sem):
        @pl.when(h > 0)
        def _():
            tell(sem, device_of(h - 1, m))

        @pl.when(h < groups - 1)
        def _():
            tell(sem, device_of(h + 1, m))

    beside = jnp.where(h > 0, 1, 0) + jnp.where(h < groups - 1, 1, 0)
    tell_line(barrier)

    @pl.when(has_edge)
    def _():
        tell(barrier, edge_peer)

    each(1, 2 * g, lambda s: tell(barrier, (h * g + across(lax.div(s, 2))) * 2 + lax.rem(core + s, 2)))
    inputs[0].start()
    load.start()
    for copy in inputs[1:]:
        copy.start()
    idx_ref[...] = jnp.zeros_like(idx_ref)
    other[...] = jnp.zeros_like(other)
    sent_extra[...] = jnp.zeros_like(sent_extra)
    small[...] = jnp.zeros_like(small)
    inputs[0].wait()
    idx_ref[0:kcount, 0:t_dev] = index_ref[...]
    lane = lax.broadcasted_iota(jnp.int32, (kcount, 128), 1)
    series = idx_ref[...]
    tile = jnp.where(
        lane < 64, series[:, :128], pltpu.roll(series, (128 - t_dev) % lanes, 1)[:, :128]
    )
    tile = jnp.where(lane == 62, jnp.sum(series, 1, keepdims=True), tile)
    tile = jnp.where(lane == 63, jnp.sum(series * series, 1, keepdims=True), tile)
    tiles[core * g + m] = tile
    idx_all[m] = series
    pack_ref[:, :lanes] = series[:8]
    pack_ref[:, lanes:] = jnp.zeros((8, 128), f32)
    for at, row, column in spare:
        pack_ref[at : at + 1, lanes:] = series[row : row + 1, column : column + 128]

    @pl.when(jnp.logical_not(has_edge))
    def _():
        tiles[2 * g] = jnp.full((kcount, 128), FAR, f32)

    pl.semaphore_wait(barrier, 2 * g - 1 + beside + jnp.where(has_edge, 1, 0))

    for side in range(2):
        each(1 - side, g, lambda s, side=side: tile_copy(side, s).start())
    each(1, g, lambda s: idx_copy(s).start())
    load.wait()
    for copy in inputs[1:]:
        copy.wait()
    small[0:1, 0 : cells // 2] = mask_ref[...].astype(f32)
    for piece in range(groups):
        own_copy(piece).start()
        each(1, g, lambda s, piece=piece: raw_copy(piece, s).start())
    for turn in range(groups - 2):
        tell_line(round_sem.at[turn])
        pl.semaphore_wait(round_sem.at[turn], beside)
    for side in range(2):
        each(1 - side, g, lambda s, side=side: tile_copy(side, s).wait_recv())

    @pl.when(has_edge)
    def _():
        edge_copy().start()

    zero_tile = jnp.zeros((kcount, 128), f32)
    zmsg[...] = lax.fori_loop(0, 2 * g, lambda at, carry: carry + tiles[at], zero_tile)
    each(1, groups, lambda s: z_copy(s).start())

    def unpack(step):
        member = across(step)
        idx_copy(step).wait_recv()
        idx_all[member, 0:8, :] = packs[member, :, :lanes]
        for at, row, column in spare:
            idx_all[member, row : row + 1, column : column + 128] = packs[
                member, at : at + 1, lanes:
            ]

    each(1, g, unpack)

    spot = lax.broadcasted_iota(jnp.int32, (kcount, wide), 1)
    wing = jnp.zeros((kcount, 128), f32)
    tail = jnp.zeros((kcount, wide - 128), f32)

    def tile_at(order):
        inside = lax.rem(order, 2) * g + lax.div(order, 2)
        outside = jnp.logical_or(order < 0, order >= 2 * g)
        return tiles[jnp.where(outside, 2 * g, inside)]

    def window(member):
        order = member * 2 + core
        step = flipped(m, member, g)
        here = jnp.concatenate([idx_all[member], wing], 1)
        before = jnp.concatenate([tile_at(order - 1), tail], 1)
        after = jnp.concatenate([tile_at(order + 1), tail], 1)
        left = pltpu.roll(before, wide - REACH, 1)
        mid = pltpu.roll(here, REACH, 1)
        right = pltpu.roll(after, REACH + t_dev, 1)
        ext = jnp.where(spot < REACH, left, jnp.where(spot < REACH + t_dev, mid, right))
        for k in range(kcount):
            line = pltpu.roll(ext[k : k + 1], wide - REACH - MAXLAG + offset_ref[k], 1)
            line = jnp.broadcast_to(line, (BASE, wide))
            raw_win[step, k * BASE : (k + 1) * BASE, :] = pltpu.roll(
                line, 0, 1, stride=1, stride_axis=0
            )

    each(0, g - 1, lambda at: window(jnp.where(core == 0, g - 1 - at, at)))

    @pl.when(has_edge)
    def _():
        edge_copy().wait()

    window(jnp.where(core == 0, 0, g - 1))
    day = lax.broadcasted_iota(jnp.int32, (lanes, 128), 0)
    shift = lax.broadcasted_iota(jnp.int32, (lanes, 128), 1) - MAXLAG
    late = jnp.where((day >= t_dev - shift) & (day < t_dev), 1.0, 0.0)
    early = jnp.where(day < -shift, 1.0, 0.0)
    chooser[0] = jnp.where(core == 0, late, early).astype(jnp.bfloat16)
    chooser[1] = jnp.where(core == 0, early, late).astype(jnp.bfloat16)
    each(1, groups, lambda s: z_copy(s).wait_recv())
    stats = zmsg[...]
    for s in range(1, groups):
        stats = stats + zin[s]
    mean = stats[:, 62:63] / total_days
    var = stats[:, 63:64] / total_days - mean * mean
    outer = 1.0 / jnp.sqrt(var + 1e-06)

    def center_window(step):
        for k in range(kcount):
            value = raw_win[step, k * BASE : (k + 1) * BASE, :]
            value = jnp.where(value < NEAR, value - mean[k : k + 1], 0.0).astype(jnp.bfloat16)
            for turn in range(0, ROWS, BASE):
                turned = value if turn == 0 else pltpu.roll(value, turn, 1)
                win[step, k * ROWS + turn : k * ROWS + turn + BASE, :] = turned[:, :lanes]

    low = lax.broadcasted_iota(jnp.int32, (ROWS, 128), 1) < 64
    low_row = lax.broadcasted_iota(jnp.int32, (1, 128), 1) < 64

    def pair_cols(cols, k):
        return jnp.where(low, cols[0:ROWS, k : k + 1], cols[0:ROWS, k + half_k : k + half_k + 1])

    def halves(first_half, second_half, is_low):
        turned_first = pltpu.roll(first_half, 64, 1)
        turned_second = pltpu.roll(second_half, 64, 1)
        zeroth = jnp.where(is_low, first_half, turned_second)
        oneth = jnp.where(is_low, turned_first, second_half)
        return jnp.where(core == 0, zeroth, oneth), jnp.where(core == 0, oneth, zeroth)

    group_days = 2 * g * t_dev * 1.0
    sums_at = 2 * count

    def add(pieces, step, first_time):
        width = 128 * len(pieces)
        value = jnp.concatenate([recv[piece, step] for piece in pieces], 1)
        wide_value = value.astype(f32)
        sums = jnp.sum(wide_value, 0, keepdims=True)
        squares = jnp.sum(wide_value * wide_value, 0, keepdims=True)
        found = jnp.dot(win[step, :, :t_dev], value, preferred_element_type=f32)
        if first_time:
            acc[0:sums_at, :width] = found
            acc[sums_at : sums_at + 1, :width] = sums
            acc[sums_at + 1 : sums_at + 2, :width] = squares
        else:
            acc[0:sums_at, :width] += found
            acc[sums_at : sums_at + 1, :width] += sums
            acc[sums_at + 1 : sums_at + 2, :width] += squares

    def split(piece, column):
        column = slice(column * 128, column * 128 + 128)
        for row in range(2):
            value = acc[sums_at + row : sums_at + row + 1, column]
            kept, given = halves(value, value, low_row)
            mine[piece, count + row : count + row + 1, :] = kept
            other[piece, count + row : count + row + 1, :] = given
        swap_copy(piece, half_k).start()
        for k in range(half_k):
            at = k * ROWS
            kept, given = halves(
                acc[at : at + ROWS, column], acc[count + at : count + at + ROWS, column], low
            )
            mine[piece, at : at + ROWS, :] = kept
            other[piece, at : at + ROWS, :] = given
            swap_copy(piece, k).start()

    def products(piece):
        own_copy(piece).wait()
        add([piece], 0, True)

        def body(turn, carry):
            step = turn
            raw_copy(piece, step).wait_recv()
            add([piece], step, False)
            return carry

        lax.fori_loop(1, g, body, 0)
        split(piece, 0)

    def joined(piece, k):
        at = k * ROWS
        swap_copy(piece, k).wait_recv()
        return mine[piece, at : at + ROWS, :] + partner_in[piece, at : at + ROWS, :]

    def joined_row(piece, row):
        at = count + row
        return mine[piece, at : at + 1, :] + partner_in[piece, at : at + 1, :]

    def decoded(slot, k):
        coded = got[slot, k * ROWS : (k + 1) * ROWS, :].astype(jnp.int32).astype(f32)
        return coded * (got_extra[slot, 2 + k : 3 + k, :] * (1.0 / TOP))

    def send_sums(piece, outer_slot):
        swap_copy(piece, half_k).wait_recv()
        sx, sq = joined_row(piece, 0), joined_row(piece, 1)
        tot, cols, days = own_tot, own_cols, group_days
        copies = sum_copies(piece, slot_of(piece))
        if outer_slot is not None:
            arriving = sum_copies(1, outer_slot)
            arriving[0].wait_recv()
            outer_x = got_extra[outer_slot, 0:1, :]
            outer_mean = outer_x / group_days
            sx, sq = sx + outer_x, sq + got_extra[outer_slot, 1:2, :]
            outer_tot = got_extra[outer_slot, EXTRA:, :]
            outer_cols = jnp.transpose(outer_tot)
            tot, cols, days = tot + outer_tot, cols + outer_cols, 2 * group_days
        sent_extra[piece, 0:1, :] = sx
        sent_extra[piece, 1:2, :] = sq
        local_mean = sx / days
        for k in range(half_k):
            value = joined(piece, k) - local_mean * pair_cols(cols, k)
            if outer_slot is not None:
                value = value + outer_mean * pair_cols(outer_cols, k)
            stage[k * ROWS : (k + 1) * ROWS, :] = value
            top = jnp.max(jnp.abs(value), 0, keepdims=True)
            if outer_slot is not None:
                top = top + got_extra[outer_slot, 2 + k : 3 + k, :]
            sent_extra[piece, 2 + k : 3 + k, :] = top
        sent_extra[piece, EXTRA:, :] = tot
        copies[0].start()
        for k in range(half_k):
            value = stage[k * ROWS : (k + 1) * ROWS, :]
            if outer_slot is not None:
                arriving[1 + k].wait_recv()
                value = value + decoded(outer_slot, k)
            scaled = value * (TOP / jnp.maximum(sent_extra[piece, 2 + k : 3 + k, :], 1e-30))
            sent[piece, k * ROWS : (k + 1) * ROWS, :] = (
                jnp.round(scaled).astype(jnp.int32).astype(jnp.int16)
            )
            copies[1 + k].start()

    def send_outer(piece):
        @pl.when(jnp.logical_not(inner))
        def _():
            send_sums(piece, None)

    def send_inner(piece, outer_slot):
        @pl.when(inner)
        def _():
            send_sums(piece, outer_slot)

    last = groups - 1
    own_copy(0).wait()
    each(1, g, lambda s: raw_copy(0, s).wait_recv())

    def early_body(step, first_time):
        center_window(step)
        add([0], step, first_time)

    early_body(0, True)

    place = lax.broadcasted_iota(jnp.int32, (kcount, lanes), 1)

    def centered(value, valid):
        return jnp.where(valid, (value - mean).astype(jnp.bfloat16).astype(f32), 0.0)

    def center_body(at, carry):
        return carry + centered(idx_all[at], place < t_dev)

    core_sum = jnp.zeros((kcount, lanes), f32)
    if g <= 4:
        for at in range(g):
            core_sum = center_body(at, core_sum)
    else:
        core_sum = lax.fori_loop(0, g, center_body, core_sum)
    inner_block = centered(idx_all[jnp.where(core == 0, 0, g - 1)], place < t_dev)
    edge = jnp.concatenate([tiles[2 * g], tail[:, : lanes - 128]], 1)
    edge = jnp.where(core == 0, pltpu.roll(edge, t_dev - 128, 1), edge)
    opens = jnp.where(core == 0, t_dev - 64, 0)
    closes = jnp.where(core == 0, t_dev, 62)
    outer_block = centered(edge, (place >= opens) & (place < closes) & (edge < NEAR))

    def part(value, side):
        return jnp.dot(
            value.astype(jnp.bfloat16), chooser[side], preferred_element_type=f32
        )

    by_shift = (
        jnp.sum(core_sum, 1, keepdims=True)
        + part(outer_block, 0)
        - part(inner_block, 1)
    )
    tot_part[...] = jnp.zeros_like(tot_part)
    for k in range(kcount):
        tot_part[k : k + 1, :] = pltpu.roll(
            by_shift[k : k + 1], lax.rem(128 - offset_ref[k], 128), 1
        )

    if g <= 4:
        for step in range(1, g):
            early_body(step, False)
    else:
        each(1, g, lambda s: early_body(s, False))
    total_copy().start()
    split(0, 0)

    total_copy().wait()
    own_tot = tot_part[...] + tot_in[...]
    own_cols = jnp.transpose(own_tot)
    send_outer(0)
    products(1)
    send_sums(1, None)
    send_inner(0, 0)
    products(2)
    send_outer(2)
    send_inner(2, 1)
    products(last)
    near_blocks, far_blocks = sum_copies(1, 2), sum_copies(1, 3)

    def opened(slot, copies, days):
        copies[0].wait_recv()
        far_x = got_extra[slot, 0:1, :]
        cols = jnp.transpose(got_extra[slot, EXTRA:, :])
        return far_x, got_extra[slot, 1:2, :], far_x / days, cols

    near_x, near_sq, near_mean, near_cols = opened(2, near_blocks, group_days)
    for k in range(half_k):
        near_blocks[1 + k].wait_recv()
        far[k * ROWS : (k + 1) * ROWS, :] = decoded(2, k) + near_mean * pair_cols(near_cols, k)
    swap_copy(last, half_k).wait_recv()
    far_x, far_sq, far_mean, far_cols = opened(3, far_blocks, 2 * group_days)
    mean_x = (joined_row(last, 0) + near_x + far_x) / total_days
    var_x = (joined_row(last, 1) + near_sq + far_sq) / total_days - mean_x * mean_x
    all_cols = own_cols + near_cols + far_cols
    mask = small[0:1, :]
    mask = mask + pltpu.roll(mask, 64, 1)
    scaling = mask / (total_days * jnp.sqrt(var_x + 1e-06))
    for k in range(half_k):
        at = k * ROWS
        far[at : at + ROWS, :] += (
            joined(last, k)
            + far_mean * pair_cols(far_cols, k)
            - mean_x * pair_cols(all_cols, k)
        )

    def normal(k):
        far_blocks[1 + k].wait_recv()
        value = far[k * ROWS : (k + 1) * ROWS, :] + decoded(3, k)
        scale = jnp.where(low_row, outer[k : k + 1], outer[k + half_k : k + half_k + 1])
        return value * (scaling * scale)

    small_int = lag_ref[...] + MAXLAG
    small[0:1, 0 : lag_ref.shape[1]] = small_int.astype(f32)
    chosen = jnp.broadcast_to(small[0:1, :].astype(jnp.int32), (64, 128))
    kept = lag_ref.shape[1]

    def out_copy(k):
        return pltpu.make_async_copy(out_buf.at[k], out_ref.at[k], out_sem.at[0])

    for k in range(0, half_k, 2):
        upper_rows = normal(k)
        under_rows = normal(k + 1) if k + 1 < half_k else upper_rows
        flat = jnp.transpose(jnp.concatenate([upper_rows, under_rows], 0))
        for side in range(2):
            rows = flat[side * 64 : (side + 1) * 64, :]
            for turn in range(min(2, half_k - k)):
                at = k + turn + side * half_k
                out_buf[at] = jnp.take_along_axis(rows, chosen + 64 * turn, axis=1)[:, :kept]
                out_copy(at).start()
    def drained(ref, sem):
        remote(ref, ref, sem, sem, partner).wait_send()

    drained(packs.at[pl.ds(0, g - 1)], idx_send.at[0])
    drained(tiles.at[pl.ds(0, 2 * g - 1)], tile_send.at[0])
    drained(zin.at[pl.ds(0, groups - 1)], z_send.at[0])
    for piece in range(groups):
        drained(recv.at[piece, pl.ds(0, g - 1)], raw_send.at[piece])
        drained(other.at[piece], swap_send.at[piece])
        if piece < last:
            drained(sent.at[piece], sum_send.at[0, piece])
            drained(sent_extra.at[piece], sum_send.at[1, piece])
    pltpu.make_async_copy(out_buf, out_ref, out_sem.at[0]).wait()


def shards(field, index, lag_list, index_offset, sea_mask):
    t_dev, cells_all = field.shape
    devices = lax.axis_size("tm")
    kcount = index.shape[1]
    lanes = round_up(t_dev, 128)
    groups = GROUPS
    g = devices // 2 // groups
    rows = kcount * ROWS
    half = rows // 2
    sizes = (devices, t_dev, kcount, groups, g)
    dma = pltpu.SemaphoreType.DMA
    f32 = jnp.float32
    maps = pl.pallas_call(
        functools.partial(kernel, sizes),
        out_shape=jax.ShapeDtypeStruct((kcount, 64, lag_list.shape[0]), f32),
        in_specs=[pl.BlockSpec(memory_space=pl.ANY)] * 5,
        out_specs=pl.BlockSpec(memory_space=pl.ANY),
        scratch_shapes=[
            pltpu.VMEM((kcount, t_dev), f32),
            pltpu.VMEM((1, lag_list.shape[0]), jnp.int32),
            pltpu.SMEM((kcount,), jnp.int32),
            pltpu.VMEM((1, sea_mask.shape[0]), jnp.int32),
            pltpu.VMEM((t_dev, cells_all), jnp.bfloat16),
            pltpu.VMEM((kcount, lanes), f32),
            pltpu.VMEM((8, lanes + 128), f32),
            pltpu.VMEM((g, 8, lanes + 128), f32),
            pltpu.VMEM((g, kcount, lanes), f32),
            pltpu.VMEM((2 * g + 1, kcount, 128), f32),
            pltpu.VMEM((kcount, 128), f32),
            pltpu.VMEM((groups, kcount, 128), f32),
            pltpu.VMEM((groups, g, t_dev, 128), jnp.bfloat16),
            pltpu.VMEM((g, kcount * BASE, lanes + 128), f32),
            pltpu.VMEM((g, rows, lanes), jnp.bfloat16),
            pltpu.VMEM((rows + EXTRA, 256), f32),
            pltpu.VMEM((groups, half + EXTRA, 128), f32),
            pltpu.VMEM((groups, half + EXTRA, 128), f32),
            pltpu.VMEM((groups, half + EXTRA, 128), f32),
            pltpu.VMEM((groups, half, 128), jnp.int16),
            pltpu.VMEM((groups, EXTRA + 16, 128), f32),
            pltpu.VMEM((groups, half, 128), jnp.int16),
            pltpu.VMEM((groups, EXTRA + 16, 128), f32),
            pltpu.VMEM((half, 128), f32),
            pltpu.VMEM((half, 128), f32),
            pltpu.VMEM((2, lanes, 128), jnp.bfloat16),
            pltpu.VMEM((kcount, 64, lag_list.shape[0]), f32),
            pltpu.VMEM((8, 128), f32),
            pltpu.VMEM((16, 128), f32),
            pltpu.VMEM((16, 128), f32),
            dma((groups,)),
            dma((groups, g - 1)),
            dma((1,)),
            dma((g - 1,)),
            dma((1,)),
            dma((2 * g - 1,)),
            dma((4,)),
            dma((1,)),
            dma((groups - 1,)),
            dma((groups,)),
            dma((groups, kcount // 2 + 1)),
            dma((2, groups - 1)),
            dma((kcount // 2 + 1, groups)),
            dma((groups + 1,)),
            pltpu.SemaphoreType.REGULAR((groups - 2,)),
            dma((1,)),
            dma((4,)),
        ],
        compiler_params=pltpu.CompilerParams(
            collective_id=0, has_side_effects=True, vmem_limit_bytes=60 * 1024 * 1024
        ),
    )(field, index.T, lag_list[None, :], index_offset, sea_mask[None, :])
    return jnp.transpose(maps, (1, 0, 2))


def solution(mesh):
    return jax.shard_map(
        shards,
        mesh=mesh,
        in_specs=(P("tm", None), P("tm", None), P(), P(), P("tm")),
        out_specs=P("tm", None, None),
        check_vma=False,
    )
```

```python
import functools

import jax
import jax.numpy as jnp
from jax import lax
from jax.experimental import pallas as pl
from jax.experimental.pallas import tpu as pltpu
from jax.sharding import PartitionSpec as P

MAXLAG = 30
MAXOFF = 14
REACH = 64
ROWS = 64
BASE = 16
EXTRA = 8
TOP = 32767.0
FAR = 1e30
NEAR = 1e29
GROUPS = 4
MESH = pl.DeviceIdType.MESH


def round_up(value, unit):
    return -(-value // unit) * unit


def kernel(
    sizes,
    field_hbm,
    index_hbm,
    lag_hbm,
    offset_hbm,
    mask_hbm,
    out_ref,
    index_ref,
    lag_ref,
    offset_ref,
    mask_ref,
    field_ref,
    idx_ref,
    pack_ref,
    packs,
    idx_all,
    tiles,
    zmsg,
    zin,
    recv,
    raw_win,
    win,
    acc,
    mine,
    other,
    partner_in,
    sent,
    sent_extra,
    got,
    got_extra,
    far,
    stage,
    chooser,
    out_buf,
    small,
    tot_part,
    tot_in,
    raw_send,
    raw_recv,
    idx_send,
    idx_recv,
    tile_send,
    tile_recv,
    lone_sem,
    z_send,
    z_recv,
    swap_send,
    swap_recv,
    sum_send,
    sum_recv,
    own_sem,
    round_sem,
    out_sem,
    in_sem,
):
    devices, t_dev, kcount, groups, g = sizes
    lanes = idx_ref.shape[1]
    wide = lanes + 128
    half_k = kcount // 2
    spare = [
        ((row - 8) * (lanes // 128) + column, row, column * 128)
        for row in range(8, kcount)
        for column in range(lanes // 128)
    ]
    count = half_k * ROWS
    cells = 128
    me = lax.axis_index("tm")
    core = lax.rem(me, 2)
    chip = lax.div(me, 2)
    h = lax.div(chip, g)
    m = lax.rem(chip, g)
    partner = chip * 2 + (1 - core)
    edge_peer = ((h + 2 * core - 1) * g + m) * 2 + (1 - core)
    has_edge = jnp.where(core == 0, h > 0, h < groups - 1)
    f32 = jnp.float32
    total_days = devices * t_dev * 1.0

    def flipped(value, step, size):
        found, bit = 0, 1
        while bit < size:
            flip = lax.rem(lax.div(value, bit) + lax.div(step, bit), 2)
            found, bit = found + flip * bit, bit * 2
        return found

    def across(step):
        return flipped(m, step, g)

    def device_of(group, member):
        return (group * g + member) * 2 + core

    def remote(src, dst, send, recv_s, device):
        return pltpu.make_async_remote_copy(
            src_ref=src,
            dst_ref=dst,
            send_sem=send,
            recv_sem=recv_s,
            device_id=(device,),
            device_id_type=MESH,
        )

    def block(at):
        return field_ref.at[:, pl.ds(pl.multiple_of(at * cells, cells), cells)]

    inner = jnp.logical_or(h == 1, h == 2)
    upper = lax.div(h, 2)
    beside_h = h + 1 - 2 * lax.rem(h, 2)

    def plane_of(piece):
        if piece == 0:
            return (groups - 1) * (1 - upper)
        if piece == 1:
            return jnp.where(inner, beside_h, 2 - upper)
        return jnp.where(inner, 2 - upper, beside_h) if piece == 2 else h

    def raw_copy(piece, step):
        to = across(step)
        return remote(
            block(plane_of(piece) * g + to),
            recv.at[piece, step],
            raw_send.at[piece],
            raw_recv.at[piece, step - 1],
            device_of(h, to),
        )

    def own_copy(piece):
        return pltpu.make_async_copy(
            block(plane_of(piece) * g + m), recv.at[piece, 0], own_sem.at[piece]
        )

    def idx_copy(step):
        return remote(
            pack_ref,
            packs.at[m],
            idx_send.at[0],
            idx_recv.at[step - 1],
            device_of(h, across(step)),
        )

    def tile_copy(side, step):
        to = (h * g + across(step)) * 2 + (core if side == 0 else 1 - core)
        tile = tiles.at[core * g + m]
        return remote(
            tile, tile, tile_send.at[0], tile_recv.at[side * g + step - 1], to
        )

    def edge_copy():
        return remote(
            tiles.at[jnp.where(core == 0, 0, 2 * g - 1)],
            tiles.at[2 * g],
            lone_sem.at[0],
            lone_sem.at[1],
            edge_peer,
        )

    def total_copy():
        return remote(tot_part, tot_in, lone_sem.at[2], lone_sem.at[3], partner)

    def z_copy(step):
        return remote(
            zmsg,
            zin.at[step],
            z_send.at[0],
            z_recv.at[step - 1],
            device_of(flipped(h, step, groups), m),
        )

    chunks = (half_k + 1) // 2

    def swap_copy(piece, chunk):
        begin = EXTRA + 2 * chunk * ROWS if chunk else 0
        end = EXTRA + min(2 * chunk + 2, half_k) * ROWS
        rows = pl.ds(begin, end - begin)
        return remote(
            other.at[piece, rows],
            partner_in.at[piece, rows],
            swap_send.at[piece],
            swap_recv.at[piece, chunk],
            partner,
        )

    def slot_of(piece):
        return jnp.where(inner, (3, 2, 3)[piece], piece)

    def receiver(piece):
        if piece == 1:
            return device_of(beside_h, m)
        return device_of(jnp.where(inner, plane_of(piece), beside_h), m)

    def sum_copies(piece, slot):
        copies = [
            remote(
                sent_extra.at[piece],
                got_extra.at[slot],
                sum_send.at[1, piece],
                sum_recv.at[chunks, slot],
                receiver(piece),
            )
        ]
        for chunk in range(chunks):
            rows = pl.ds(2 * chunk * ROWS, min(2, half_k - 2 * chunk) * ROWS)
            copies.append(
                remote(
                    sent.at[piece, rows],
                    got.at[slot, rows],
                    sum_send.at[0, piece],
                    sum_recv.at[chunk, slot],
                    receiver(piece),
                )
            )
        return copies

    def each(low_step, high_step, act):
        def body(step, carry):
            act(step)
            return carry

        lax.fori_loop(low_step, high_step, body, 0)

    load = pltpu.make_async_copy(field_hbm, field_ref, own_sem.at[groups])
    inputs = [
        pltpu.make_async_copy(src, dst, in_sem.at[at])
        for at, (src, dst) in enumerate(
            (
                (index_hbm, index_ref),
                (lag_hbm, lag_ref),
                (offset_hbm, offset_ref),
                (mask_hbm, mask_ref),
            )
        )
    ]
    barrier = pltpu.get_barrier_semaphore()

    def tell(sem, device):
        pl.semaphore_signal(sem, inc=1, device_id=(device,), device_id_type=MESH)

    def tell_line(sem):
        @pl.when(h > 0)
        def _():
            tell(sem, device_of(h - 1, m))

        @pl.when(h < groups - 1)
        def _():
            tell(sem, device_of(h + 1, m))

    beside = jnp.where(h > 0, 1, 0) + jnp.where(h < groups - 1, 1, 0)
    tell_line(barrier)

    @pl.when(has_edge)
    def _():
        tell(barrier, edge_peer)

    each(1, 2 * g, lambda s: tell(barrier, (h * g + across(lax.div(s, 2))) * 2 + lax.rem(core + s, 2)))
    inputs[0].start()
    load.start()
    for copy in inputs[1:]:
        copy.start()
    idx_ref[...] = jnp.zeros_like(idx_ref)
    other[...] = jnp.zeros_like(other)
    sent_extra[...] = jnp.zeros_like(sent_extra)
    small[...] = jnp.zeros_like(small)
    inputs[0].wait()
    idx_ref[0:kcount, 0:t_dev] = index_ref[...]
    lane = lax.broadcasted_iota(jnp.int32, (kcount, 128), 1)
    series = idx_ref[...]
    tile = jnp.where(
        lane < 64, series[:, :128], pltpu.roll(series, (128 - t_dev) % lanes, 1)[:, :128]
    )
    tile = jnp.where(lane == 62, jnp.sum(series, 1, keepdims=True), tile)
    tile = jnp.where(lane == 63, jnp.sum(series * series, 1, keepdims=True), tile)
    tiles[core * g + m] = tile
    idx_all[m] = series
    pack_ref[:, :lanes] = series[:8]
    pack_ref[:, lanes:] = jnp.zeros((8, 128), f32)
    for at, row, column in spare:
        pack_ref[at : at + 1, lanes:] = series[row : row + 1, column : column + 128]

    @pl.when(jnp.logical_not(has_edge))
    def _():
        tiles[2 * g] = jnp.full((kcount, 128), FAR, f32)

    pl.semaphore_wait(barrier, 2 * g - 1 + beside + jnp.where(has_edge, 1, 0))

    for side in range(2):
        each(1 - side, g, lambda s, side=side: tile_copy(side, s).start())
    each(1, g, lambda s: idx_copy(s).start())
    load.wait()
    for copy in inputs[1:]:
        copy.wait()
    small[0:1, 0 : cells // 2] = mask_ref[...].astype(f32)
    for piece in range(groups):
        own_copy(piece).start()
        each(1, g, lambda s, piece=piece: raw_copy(piece, s).start())
    for turn in range(groups - 2):
        tell_line(round_sem.at[turn])
        pl.semaphore_wait(round_sem.at[turn], beside)
    for side in range(2):
        each(1 - side, g, lambda s, side=side: tile_copy(side, s).wait_recv())

    @pl.when(has_edge)
    def _():
        edge_copy().start()

    zero_tile = jnp.zeros((kcount, 128), f32)
    zmsg[...] = lax.fori_loop(0, 2 * g, lambda at, carry: carry + tiles[at], zero_tile)
    each(1, groups, lambda s: z_copy(s).start())

    def unpack(step):
        member = across(step)
        idx_copy(step).wait_recv()
        idx_all[member, 0:8, :] = packs[member, :, :lanes]
        for at, row, column in spare:
            idx_all[member, row : row + 1, column : column + 128] = packs[
                member, at : at + 1, lanes:
            ]

    each(1, g, unpack)

    spot = lax.broadcasted_iota(jnp.int32, (kcount, wide), 1)
    wing = jnp.zeros((kcount, 128), f32)
    tail = jnp.zeros((kcount, wide - 128), f32)

    def tile_at(order):
        inside = lax.rem(order, 2) * g + lax.div(order, 2)
        outside = jnp.logical_or(order < 0, order >= 2 * g)
        return tiles[jnp.where(outside, 2 * g, inside)]

    def window(member):
        order = member * 2 + core
        step = flipped(m, member, g)
        here = jnp.concatenate([idx_all[member], wing], 1)
        before = jnp.concatenate([tile_at(order - 1), tail], 1)
        after = jnp.concatenate([tile_at(order + 1), tail], 1)
        left = pltpu.roll(before, wide - REACH, 1)
        mid = pltpu.roll(here, REACH, 1)
        right = pltpu.roll(after, REACH + t_dev, 1)
        ext = jnp.where(spot < REACH, left, jnp.where(spot < REACH + t_dev, mid, right))
        for k in range(kcount):
            line = pltpu.roll(ext[k : k + 1], wide - REACH - MAXLAG + offset_ref[k], 1)
            line = jnp.broadcast_to(line, (BASE, wide))
            raw_win[step, k * BASE : (k + 1) * BASE, :] = pltpu.roll(
                line, 0, 1, stride=1, stride_axis=0
            )

    each(0, g - 1, lambda at: window(jnp.where(core == 0, g - 1 - at, at)))

    @pl.when(has_edge)
    def _():
        edge_copy().wait()

    window(jnp.where(core == 0, 0, g - 1))
    day = lax.broadcasted_iota(jnp.int32, (lanes, 128), 0)
    shift = lax.broadcasted_iota(jnp.int32, (lanes, 128), 1) - MAXLAG
    late = jnp.where((day >= t_dev - shift) & (day < t_dev), 1.0, 0.0)
    early = jnp.where(day < -shift, 1.0, 0.0)
    chooser[0] = jnp.where(core == 0, late, early).astype(jnp.bfloat16)
    chooser[1] = jnp.where(core == 0, early, late).astype(jnp.bfloat16)
    each(1, groups, lambda s: z_copy(s).wait_recv())
    stats = zmsg[...]
    for s in range(1, groups):
        stats = stats + zin[s]
    mean = stats[:, 62:63] / total_days
    var = stats[:, 63:64] / total_days - mean * mean
    outer = 1.0 / jnp.sqrt(var + 1e-06)

    def center_window(step):
        for k in range(kcount):
            value = raw_win[step, k * BASE : (k + 1) * BASE, :]
            value = jnp.where(value < NEAR, value - mean[k : k + 1], 0.0).astype(jnp.bfloat16)
            for turn in range(0, ROWS, BASE):
                turned = value if turn == 0 else pltpu.roll(value, turn, 1)
                win[step, k * ROWS + turn : k * ROWS + turn + BASE, :] = turned[:, :lanes]

    low = lax.broadcasted_iota(jnp.int32, (ROWS, 128), 1) < 64
    low_row = lax.broadcasted_iota(jnp.int32, (1, 128), 1) < 64

    def pair_cols(cols, k):
        return jnp.where(low, cols[0:ROWS, k : k + 1], cols[0:ROWS, k + half_k : k + half_k + 1])

    def halves(first_half, second_half, is_low):
        turned_first = pltpu.roll(first_half, 64, 1)
        turned_second = pltpu.roll(second_half, 64, 1)
        zeroth = jnp.where(is_low, first_half, turned_second)
        oneth = jnp.where(is_low, turned_first, second_half)
        return jnp.where(core == 0, zeroth, oneth), jnp.where(core == 0, oneth, zeroth)

    group_days = 2 * g * t_dev * 1.0
    sums_at = 2 * count

    def add(pieces, step, first_time):
        width = 128 * len(pieces)
        value = jnp.concatenate([recv[piece, step] for piece in pieces], 1)
        wide_value = value.astype(f32)
        sums = jnp.sum(wide_value, 0, keepdims=True)
        squares = jnp.sum(wide_value * wide_value, 0, keepdims=True)
        found = jnp.dot(win[step, :, :t_dev], value, preferred_element_type=f32)
        if first_time:
            acc[0:sums_at, :width] = found
            acc[sums_at : sums_at + 1, :width] = sums
            acc[sums_at + 1 : sums_at + 2, :width] = squares
        else:
            acc[0:sums_at, :width] += found
            acc[sums_at : sums_at + 1, :width] += sums
            acc[sums_at + 1 : sums_at + 2, :width] += squares

    def split(piece, column):
        column = slice(column * 128, column * 128 + 128)
        for row in range(2):
            value = acc[sums_at + row : sums_at + row + 1, column]
            kept, given = halves(value, value, low_row)
            mine[piece, row : row + 1, :] = kept
            other[piece, row : row + 1, :] = given
        for k in range(half_k):
            at = k * ROWS
            kept, given = halves(
                acc[at : at + ROWS, column], acc[count + at : count + at + ROWS, column], low
            )
            mine[piece, EXTRA + at : EXTRA + at + ROWS, :] = kept
            other[piece, EXTRA + at : EXTRA + at + ROWS, :] = given
            if k % 2 == 1 or k == half_k - 1:
                swap_copy(piece, k // 2).start()

    def products(piece):
        own_copy(piece).wait()
        add([piece], 0, True)

        def body(turn, carry):
            step = turn
            raw_copy(piece, step).wait_recv()
            add([piece], step, False)
            return carry

        lax.fori_loop(1, g, body, 0)
        split(piece, 0)

    def joined(piece, k):
        at = EXTRA + k * ROWS
        if k % 2 == 0 and k > 0:
            swap_copy(piece, k // 2).wait_recv()
        return mine[piece, at : at + ROWS, :] + partner_in[piece, at : at + ROWS, :]

    def joined_row(piece, row):
        at = row
        return mine[piece, at : at + 1, :] + partner_in[piece, at : at + 1, :]

    def decoded(slot, k):
        coded = got[slot, k * ROWS : (k + 1) * ROWS, :].astype(jnp.int32).astype(f32)
        return coded * (got_extra[slot, 2 + k : 3 + k, :] * (1.0 / TOP))

    def send_sums(piece, outer_slot):
        swap_copy(piece, 0).wait_recv()
        sx, sq = joined_row(piece, 0), joined_row(piece, 1)
        tot, cols, days = own_tot, own_cols, group_days
        copies = sum_copies(piece, slot_of(piece))
        if outer_slot is not None:
            arriving = sum_copies(1, outer_slot)
            arriving[0].wait_recv()
            outer_x = got_extra[outer_slot, 0:1, :]
            outer_mean = outer_x / group_days
            sx, sq = sx + outer_x, sq + got_extra[outer_slot, 1:2, :]
            outer_tot = got_extra[outer_slot, EXTRA:, :]
            outer_cols = jnp.transpose(outer_tot)
            tot, cols, days = tot + outer_tot, cols + outer_cols, 2 * group_days
        sent_extra[piece, 0:1, :] = sx
        sent_extra[piece, 1:2, :] = sq
        local_mean = sx / days
        for k in range(half_k):
            value = joined(piece, k) - local_mean * pair_cols(cols, k)
            if outer_slot is not None:
                value = value + outer_mean * pair_cols(outer_cols, k)
            stage[k * ROWS : (k + 1) * ROWS, :] = value
            top = jnp.max(jnp.abs(value), 0, keepdims=True)
            if outer_slot is not None:
                top = top + got_extra[outer_slot, 2 + k : 3 + k, :]
            sent_extra[piece, 2 + k : 3 + k, :] = top
        sent_extra[piece, EXTRA:, :] = tot
        copies[0].start()
        for k in range(half_k):
            value = stage[k * ROWS : (k + 1) * ROWS, :]
            if outer_slot is not None:
                if k % 2 == 0:
                    arriving[1 + k // 2].wait_recv()
                value = value + decoded(outer_slot, k)
            scaled = value * (TOP / jnp.maximum(sent_extra[piece, 2 + k : 3 + k, :], 1e-30))
            sent[piece, k * ROWS : (k + 1) * ROWS, :] = (
                jnp.round(scaled).astype(jnp.int32).astype(jnp.int16)
            )
            if k % 2 == 1 or k == half_k - 1:
                copies[1 + k // 2].start()

    def send_outer(piece):
        @pl.when(jnp.logical_not(inner))
        def _():
            send_sums(piece, None)

    def send_inner(piece, outer_slot):
        @pl.when(inner)
        def _():
            send_sums(piece, outer_slot)

    last = groups - 1
    own_copy(0).wait()
    each(1, g, lambda s: raw_copy(0, s).wait_recv())

    def early_body(step, first_time):
        center_window(step)
        add([0], step, first_time)

    early_body(0, True)

    place = lax.broadcasted_iota(jnp.int32, (kcount, lanes), 1)

    def centered(value, valid):
        return jnp.where(valid, (value - mean).astype(jnp.bfloat16).astype(f32), 0.0)

    def center_body(at, carry):
        return carry + centered(idx_all[at], place < t_dev)

    core_sum = jnp.zeros((kcount, lanes), f32)
    if g <= 4:
        for at in range(g):
            core_sum = center_body(at, core_sum)
    else:
        core_sum = lax.fori_loop(0, g, center_body, core_sum)
    inner_block = centered(idx_all[jnp.where(core == 0, 0, g - 1)], place < t_dev)
    edge = jnp.concatenate([tiles[2 * g], tail[:, : lanes - 128]], 1)
    edge = jnp.where(core == 0, pltpu.roll(edge, t_dev - 128, 1), edge)
    opens = jnp.where(core == 0, t_dev - 64, 0)
    closes = jnp.where(core == 0, t_dev, 62)
    outer_block = centered(edge, (place >= opens) & (place < closes) & (edge < NEAR))

    def part(value, side):
        return jnp.dot(
            value.astype(jnp.bfloat16), chooser[side], preferred_element_type=f32
        )

    by_shift = (
        jnp.sum(core_sum, 1, keepdims=True)
        + part(outer_block, 0)
        - part(inner_block, 1)
    )
    tot_part[...] = jnp.zeros_like(tot_part)
    for k in range(kcount):
        tot_part[k : k + 1, :] = pltpu.roll(
            by_shift[k : k + 1], lax.rem(128 - offset_ref[k], 128), 1
        )

    if g <= 4:
        for step in range(1, g):
            early_body(step, False)
    else:
        each(1, g, lambda s: early_body(s, False))
    total_copy().start()
    split(0, 0)

    total_copy().wait()
    own_tot = tot_part[...] + tot_in[...]
    own_cols = jnp.transpose(own_tot)
    send_outer(0)
    products(1)
    send_sums(1, None)
    send_inner(0, 0)
    products(2)
    send_outer(2)
    send_inner(2, 1)
    products(last)
    near_blocks, far_blocks = sum_copies(1, 2), sum_copies(1, 3)

    def opened(slot, copies, days):
        copies[0].wait_recv()
        far_x = got_extra[slot, 0:1, :]
        cols = jnp.transpose(got_extra[slot, EXTRA:, :])
        return far_x, got_extra[slot, 1:2, :], far_x / days, cols

    near_x, near_sq, near_mean, near_cols = opened(2, near_blocks, group_days)
    for k in range(half_k):
        if k % 2 == 0:
            near_blocks[1 + k // 2].wait_recv()
        far[k * ROWS : (k + 1) * ROWS, :] = decoded(2, k) + near_mean * pair_cols(near_cols, k)
    swap_copy(last, 0).wait_recv()
    far_x, far_sq, far_mean, far_cols = opened(3, far_blocks, 2 * group_days)
    mean_x = (joined_row(last, 0) + near_x + far_x) / total_days
    var_x = (joined_row(last, 1) + near_sq + far_sq) / total_days - mean_x * mean_x
    all_cols = own_cols + near_cols + far_cols
    mask = small[0:1, :]
    mask = mask + pltpu.roll(mask, 64, 1)
    scaling = mask / (total_days * jnp.sqrt(var_x + 1e-06))
    for k in range(half_k):
        at = k * ROWS
        far[at : at + ROWS, :] += (
            joined(last, k)
            + far_mean * pair_cols(far_cols, k)
            - mean_x * pair_cols(all_cols, k)
        )

    def normal(k):
        if k % 2 == 0:
            far_blocks[1 + k // 2].wait_recv()
        value = far[k * ROWS : (k + 1) * ROWS, :] + decoded(3, k)
        scale = jnp.where(low_row, outer[k : k + 1], outer[k + half_k : k + half_k + 1])
        return value * (scaling * scale)

    small_int = lag_ref[...] + MAXLAG
    small[0:1, 0 : lag_ref.shape[1]] = small_int.astype(f32)
    chosen = jnp.broadcast_to(small[0:1, :].astype(jnp.int32), (64, 128))
    kept = lag_ref.shape[1]

    def out_copy(k):
        return pltpu.make_async_copy(out_buf.at[k], out_ref.at[k], out_sem.at[0])

    for k in range(0, half_k, 2):
        upper_rows = normal(k)
        under_rows = normal(k + 1) if k + 1 < half_k else upper_rows
        flat = jnp.transpose(jnp.concatenate([upper_rows, under_rows], 0))
        for side in range(2):
            rows = flat[side * 64 : (side + 1) * 64, :]
            for turn in range(min(2, half_k - k)):
                at = k + turn + side * half_k
                out_buf[at] = jnp.take_along_axis(rows, chosen + 64 * turn, axis=1)[:, :kept]
                out_copy(at).start()
    def drained(ref, sem):
        remote(ref, ref, sem, sem, partner).wait_send()

    drained(packs.at[pl.ds(0, g - 1)], idx_send.at[0])
    drained(tiles.at[pl.ds(0, 2 * g - 1)], tile_send.at[0])
    drained(zin.at[pl.ds(0, groups - 1)], z_send.at[0])
    for piece in range(groups):
        drained(recv.at[piece, pl.ds(0, g - 1)], raw_send.at[piece])
        drained(other.at[piece], swap_send.at[piece])
        if piece < last:
            drained(sent.at[piece], sum_send.at[0, piece])
            drained(sent_extra.at[piece], sum_send.at[1, piece])
    pltpu.make_async_copy(out_buf, out_ref, out_sem.at[0]).wait()


def shards(field, index, lag_list, index_offset, sea_mask):
    t_dev, cells_all = field.shape
    devices = lax.axis_size("tm")
    kcount = index.shape[1]
    lanes = round_up(t_dev, 128)
    groups = GROUPS
    g = devices // 2 // groups
    rows = kcount * ROWS
    half = rows // 2
    sizes = (devices, t_dev, kcount, groups, g)
    dma = pltpu.SemaphoreType.DMA
    f32 = jnp.float32
    maps = pl.pallas_call(
        functools.partial(kernel, sizes),
        out_shape=jax.ShapeDtypeStruct((kcount, 64, lag_list.shape[0]), f32),
        in_specs=[pl.BlockSpec(memory_space=pl.ANY)] * 5,
        out_specs=pl.BlockSpec(memory_space=pl.ANY),
        scratch_shapes=[
            pltpu.VMEM((kcount, t_dev), f32),
            pltpu.VMEM((1, lag_list.shape[0]), jnp.int32),
            pltpu.SMEM((kcount,), jnp.int32),
            pltpu.VMEM((1, sea_mask.shape[0]), jnp.int32),
            pltpu.VMEM((t_dev, cells_all), jnp.bfloat16),
            pltpu.VMEM((kcount, lanes), f32),
            pltpu.VMEM((8, lanes + 128), f32),
            pltpu.VMEM((g, 8, lanes + 128), f32),
            pltpu.VMEM((g, kcount, lanes), f32),
            pltpu.VMEM((2 * g + 1, kcount, 128), f32),
            pltpu.VMEM((kcount, 128), f32),
            pltpu.VMEM((groups, kcount, 128), f32),
            pltpu.VMEM((groups, g, t_dev, 128), jnp.bfloat16),
            pltpu.VMEM((g, kcount * BASE, lanes + 128), f32),
            pltpu.VMEM((g, rows, lanes), jnp.bfloat16),
            pltpu.VMEM((rows + EXTRA, 256), f32),
            pltpu.VMEM((groups, half + EXTRA, 128), f32),
            pltpu.VMEM((groups, half + EXTRA, 128), f32),
            pltpu.VMEM((groups, half + EXTRA, 128), f32),
            pltpu.VMEM((groups, half, 128), jnp.int16),
            pltpu.VMEM((groups, EXTRA + 16, 128), f32),
            pltpu.VMEM((groups, half, 128), jnp.int16),
            pltpu.VMEM((groups, EXTRA + 16, 128), f32),
            pltpu.VMEM((half, 128), f32),
            pltpu.VMEM((half, 128), f32),
            pltpu.VMEM((2, lanes, 128), jnp.bfloat16),
            pltpu.VMEM((kcount, 64, lag_list.shape[0]), f32),
            pltpu.VMEM((8, 128), f32),
            pltpu.VMEM((16, 128), f32),
            pltpu.VMEM((16, 128), f32),
            dma((groups,)),
            dma((groups, g - 1)),
            dma((1,)),
            dma((g - 1,)),
            dma((1,)),
            dma((2 * g - 1,)),
            dma((4,)),
            dma((1,)),
            dma((groups - 1,)),
            dma((groups,)),
            dma((groups, (kcount // 2 + 1) // 2)),
            dma((2, groups - 1)),
            dma(((kcount // 2 + 1) // 2 + 1, groups)),
            dma((groups + 1,)),
            pltpu.SemaphoreType.REGULAR((groups - 2,)),
            dma((1,)),
            dma((4,)),
        ],
        compiler_params=pltpu.CompilerParams(
            collective_id=0, has_side_effects=True, vmem_limit_bytes=60 * 1024 * 1024
        ),
    )(field, index.T, lag_list[None, :], index_offset, sea_mask[None, :])
    return jnp.transpose(maps, (1, 0, 2))


def solution(mesh):
    return jax.shard_map(
        shards,
        mesh=mesh,
        in_specs=(P("tm", None), P("tm", None), P(), P(), P("tm")),
        out_specs=P("tm", None, None),
        check_vma=False,
    )
```

```python
import functools

import jax
import jax.numpy as jnp
from jax import lax
from jax.experimental import pallas as pl
from jax.experimental.pallas import tpu as pltpu
from jax.sharding import PartitionSpec as P

MAXLAG = 30
MAXOFF = 14
REACH = 64
ROWS = 64
BASE = 16
EXTRA = 8
TOP = 32767.0
FAR = 1e30
NEAR = 1e29
GROUPS = 4
MESH = pl.DeviceIdType.MESH


def round_up(value, unit):
    return -(-value // unit) * unit


def kernel(
    sizes,
    field_hbm,
    index_hbm,
    lag_hbm,
    offset_hbm,
    mask_hbm,
    out_ref,
    index_ref,
    lag_ref,
    offset_ref,
    mask_ref,
    field_ref,
    idx_ref,
    pack_ref,
    packs,
    idx_all,
    tiles,
    zmsg,
    zin,
    recv,
    raw_win,
    win,
    acc,
    mine,
    other,
    partner_in,
    sent,
    sent_extra,
    got,
    got_extra,
    far,
    stage,
    chooser,
    out_buf,
    small,
    tot_part,
    tot_in,
    raw_send,
    raw_recv,
    idx_send,
    idx_recv,
    tile_send,
    tile_recv,
    lone_sem,
    z_send,
    z_recv,
    swap_send,
    swap_recv,
    sum_send,
    sum_recv,
    own_sem,
    round_sem,
    out_sem,
    in_sem,
):
    devices, t_dev, kcount, groups, g = sizes
    lanes = idx_ref.shape[1]
    wide = lanes + 128
    half_k = kcount // 2
    spare = [
        ((row - 8) * (lanes // 128) + column, row, column * 128)
        for row in range(8, kcount)
        for column in range(lanes // 128)
    ]
    count = half_k * ROWS
    cells = 128
    me = lax.axis_index("tm")
    core = lax.rem(me, 2)
    chip = lax.div(me, 2)
    h = lax.div(chip, g)
    m = lax.rem(chip, g)
    partner = chip * 2 + (1 - core)
    edge_peer = ((h + 2 * core - 1) * g + m) * 2 + (1 - core)
    has_edge = jnp.where(core == 0, h > 0, h < groups - 1)
    f32 = jnp.float32
    total_days = devices * t_dev * 1.0

    def flipped(value, step, size):
        found, bit = 0, 1
        while bit < size:
            flip = lax.rem(lax.div(value, bit) + lax.div(step, bit), 2)
            found, bit = found + flip * bit, bit * 2
        return found

    def across(step):
        return flipped(m, step, g)

    def device_of(group, member):
        return (group * g + member) * 2 + core

    def remote(src, dst, send, recv_s, device):
        return pltpu.make_async_remote_copy(
            src_ref=src,
            dst_ref=dst,
            send_sem=send,
            recv_sem=recv_s,
            device_id=(device,),
            device_id_type=MESH,
        )

    def block(at):
        return field_ref.at[:, pl.ds(pl.multiple_of(at * cells, cells), cells)]

    inner = jnp.logical_or(h == 1, h == 2)
    upper = lax.div(h, 2)
    beside_h = h + 1 - 2 * lax.rem(h, 2)

    def plane_of(piece):
        if piece == 0:
            return (groups - 1) * (1 - upper)
        if piece == 1:
            return jnp.where(inner, beside_h, 2 - upper)
        return jnp.where(inner, 2 - upper, beside_h) if piece == 2 else h

    def raw_copy(piece, step):
        to = across(step)
        return remote(
            block(plane_of(piece) * g + to),
            recv.at[piece, step],
            raw_send.at[piece],
            raw_recv.at[piece, step - 1],
            device_of(h, to),
        )

    def own_copy(piece):
        return pltpu.make_async_copy(
            block(plane_of(piece) * g + m), recv.at[piece, 0], own_sem.at[piece]
        )

    def idx_copy(step):
        return remote(
            pack_ref,
            packs.at[m],
            idx_send.at[0],
            idx_recv.at[step - 1],
            device_of(h, across(step)),
        )

    def tile_copy(side, step):
        to = (h * g + across(step)) * 2 + (core if side == 0 else 1 - core)
        tile = tiles.at[core * g + m]
        return remote(
            tile, tile, tile_send.at[0], tile_recv.at[side * g + step - 1], to
        )

    def edge_copy():
        return remote(
            tiles.at[jnp.where(core == 0, 0, 2 * g - 1)],
            tiles.at[2 * g],
            lone_sem.at[0],
            lone_sem.at[1],
            edge_peer,
        )

    def total_copy():
        return remote(tot_part, tot_in, lone_sem.at[2], lone_sem.at[3], partner)

    def z_copy(step):
        return remote(
            zmsg,
            zin.at[step],
            z_send.at[0],
            z_recv.at[step - 1],
            device_of(flipped(h, step, groups), m),
        )

    chunks = (half_k + 1) // 2

    def swap_copy(piece, chunk):
        begin = EXTRA + 2 * chunk * ROWS if chunk else 0
        end = EXTRA + min(2 * chunk + 2, half_k) * ROWS
        rows = pl.ds(begin, end - begin)
        return remote(
            other.at[piece, rows],
            partner_in.at[piece, rows],
            swap_send.at[piece],
            swap_recv.at[piece, chunk],
            partner,
        )

    def slot_of(piece):
        return jnp.where(inner, (3, 2, 3)[piece], piece)

    def receiver(piece):
        if piece == 1:
            return device_of(beside_h, m)
        return device_of(jnp.where(inner, plane_of(piece), beside_h), m)

    def sum_copies(piece, slot):
        copies = [
            remote(
                sent_extra.at[piece],
                got_extra.at[slot],
                sum_send.at[1, piece],
                sum_recv.at[chunks, slot],
                receiver(piece),
            )
        ]
        for chunk in range(chunks):
            rows = pl.ds(2 * chunk * ROWS, min(2, half_k - 2 * chunk) * ROWS)
            copies.append(
                remote(
                    sent.at[piece, rows],
                    got.at[slot, rows],
                    sum_send.at[0, piece],
                    sum_recv.at[chunk, slot],
                    receiver(piece),
                )
            )
        return copies

    def each(low_step, high_step, act):
        def body(step, carry):
            act(step)
            return carry

        lax.fori_loop(low_step, high_step, body, 0)

    load = pltpu.make_async_copy(field_hbm, field_ref, own_sem.at[groups])
    inputs = [
        pltpu.make_async_copy(src, dst, in_sem.at[at])
        for at, (src, dst) in enumerate(
            (
                (index_hbm, index_ref),
                (lag_hbm, lag_ref),
                (offset_hbm, offset_ref),
                (mask_hbm, mask_ref),
            )
        )
    ]
    barrier = pltpu.get_barrier_semaphore()

    def tell(sem, device):
        pl.semaphore_signal(sem, inc=1, device_id=(device,), device_id_type=MESH)

    def tell_line(sem):
        @pl.when(h > 0)
        def _():
            tell(sem, device_of(h - 1, m))

        @pl.when(h < groups - 1)
        def _():
            tell(sem, device_of(h + 1, m))

    beside = jnp.where(h > 0, 1, 0) + jnp.where(h < groups - 1, 1, 0)
    tell_line(barrier)

    @pl.when(has_edge)
    def _():
        tell(barrier, edge_peer)

    each(1, 2 * g, lambda s: tell(barrier, (h * g + across(lax.div(s, 2))) * 2 + lax.rem(core + s, 2)))
    inputs[0].start()
    load.start()
    for copy in inputs[1:]:
        copy.start()
    idx_ref[...] = jnp.zeros_like(idx_ref)
    other[...] = jnp.zeros_like(other)
    sent_extra[...] = jnp.zeros_like(sent_extra)
    small[...] = jnp.zeros_like(small)
    inputs[0].wait()
    idx_ref[0:kcount, 0:t_dev] = index_ref[...]
    lane = lax.broadcasted_iota(jnp.int32, (kcount, 128), 1)
    series = idx_ref[...]
    tile = jnp.where(
        lane < 64, series[:, :128], pltpu.roll(series, (128 - t_dev) % lanes, 1)[:, :128]
    )
    tile = jnp.where(lane == 62, jnp.sum(series, 1, keepdims=True), tile)
    tile = jnp.where(lane == 63, jnp.sum(series * series, 1, keepdims=True), tile)
    tiles[core * g + m] = tile
    idx_all[m] = series
    pack_ref[:, :lanes] = series[:8]
    pack_ref[:, lanes:] = jnp.zeros((8, 128), f32)
    for at, row, column in spare:
        pack_ref[at : at + 1, lanes:] = series[row : row + 1, column : column + 128]

    @pl.when(jnp.logical_not(has_edge))
    def _():
        tiles[2 * g] = jnp.full((kcount, 128), FAR, f32)

    pl.semaphore_wait(barrier, 2 * g - 1 + beside + jnp.where(has_edge, 1, 0))
    tell_line(round_sem.at[0])

    for side in range(2):
        each(1 - side, g, lambda s, side=side: tile_copy(side, s).start())
    each(1, g, lambda s: idx_copy(s).start())
    load.wait()
    for copy in inputs[1:]:
        copy.wait()
    small[0:1, 0 : cells // 2] = mask_ref[...].astype(f32)
    for piece in range(groups):
        own_copy(piece).start()
        each(1, g, lambda s, piece=piece: raw_copy(piece, s).start())
    for turn in range(groups - 2):
        if turn > 0:
            tell_line(round_sem.at[turn])
        pl.semaphore_wait(round_sem.at[turn], beside)
    for side in range(2):
        each(1 - side, g, lambda s, side=side: tile_copy(side, s).wait_recv())

    @pl.when(has_edge)
    def _():
        edge_copy().start()

    zero_tile = jnp.zeros((kcount, 128), f32)
    zmsg[...] = lax.fori_loop(0, 2 * g, lambda at, carry: carry + tiles[at], zero_tile)
    each(1, groups, lambda s: z_copy(s).start())

    def unpack(step):
        member = across(step)
        idx_copy(step).wait_recv()
        idx_all[member, 0:8, :] = packs[member, :, :lanes]
        for at, row, column in spare:
            idx_all[member, row : row + 1, column : column + 128] = packs[
                member, at : at + 1, lanes:
            ]

    each(1, g, unpack)

    spot = lax.broadcasted_iota(jnp.int32, (kcount, wide), 1)
    wing = jnp.zeros((kcount, 128), f32)
    tail = jnp.zeros((kcount, wide - 128), f32)

    def tile_at(order):
        inside = lax.rem(order, 2) * g + lax.div(order, 2)
        outside = jnp.logical_or(order < 0, order >= 2 * g)
        return tiles[jnp.where(outside, 2 * g, inside)]

    def window(member):
        order = member * 2 + core
        step = flipped(m, member, g)
        here = jnp.concatenate([idx_all[member], wing], 1)
        before = jnp.concatenate([tile_at(order - 1), tail], 1)
        after = jnp.concatenate([tile_at(order + 1), tail], 1)
        left = pltpu.roll(before, wide - REACH, 1)
        mid = pltpu.roll(here, REACH, 1)
        right = pltpu.roll(after, REACH + t_dev, 1)
        ext = jnp.where(spot < REACH, left, jnp.where(spot < REACH + t_dev, mid, right))
        for k in range(kcount):
            line = pltpu.roll(ext[k : k + 1], wide - REACH - MAXLAG + offset_ref[k], 1)
            line = jnp.broadcast_to(line, (BASE, wide))
            raw_win[step, k * BASE : (k + 1) * BASE, :] = pltpu.roll(
                line, 0, 1, stride=1, stride_axis=0
            )

    each(0, g - 1, lambda at: window(jnp.where(core == 0, g - 1 - at, at)))

    @pl.when(has_edge)
    def _():
        edge_copy().wait()

    window(jnp.where(core == 0, 0, g - 1))
    day = lax.broadcasted_iota(jnp.int32, (lanes, 128), 0)
    shift = lax.broadcasted_iota(jnp.int32, (lanes, 128), 1) - MAXLAG
    late = jnp.where((day >= t_dev - shift) & (day < t_dev), 1.0, 0.0)
    early = jnp.where(day < -shift, 1.0, 0.0)
    chooser[0] = jnp.where(core == 0, late, early).astype(jnp.bfloat16)
    chooser[1] = jnp.where(core == 0, early, late).astype(jnp.bfloat16)
    each(1, groups, lambda s: z_copy(s).wait_recv())
    stats = zmsg[...]
    for s in range(1, groups):
        stats = stats + zin[s]
    mean = stats[:, 62:63] / total_days
    var = stats[:, 63:64] / total_days - mean * mean
    outer = 1.0 / jnp.sqrt(var + 1e-06)

    def center_window(step):
        for k in range(kcount):
            value = raw_win[step, k * BASE : (k + 1) * BASE, :]
            value = jnp.where(value < NEAR, value - mean[k : k + 1], 0.0).astype(jnp.bfloat16)
            for turn in range(0, ROWS, BASE):
                turned = value if turn == 0 else pltpu.roll(value, turn, 1)
                win[step, k * ROWS + turn : k * ROWS + turn + BASE, :] = turned[:, :lanes]

    low = lax.broadcasted_iota(jnp.int32, (ROWS, 128), 1) < 64
    low_row = lax.broadcasted_iota(jnp.int32, (1, 128), 1) < 64

    def pair_cols(cols, k):
        return jnp.where(low, cols[0:ROWS, k : k + 1], cols[0:ROWS, k + half_k : k + half_k + 1])

    def halves(first_half, second_half, is_low):
        turned_first = pltpu.roll(first_half, 64, 1)
        turned_second = pltpu.roll(second_half, 64, 1)
        zeroth = jnp.where(is_low, first_half, turned_second)
        oneth = jnp.where(is_low, turned_first, second_half)
        return jnp.where(core == 0, zeroth, oneth), jnp.where(core == 0, oneth, zeroth)

    group_days = 2 * g * t_dev * 1.0
    sums_at = 2 * count

    def add(pieces, step, first_time):
        width = 128 * len(pieces)
        value = jnp.concatenate([recv[piece, step] for piece in pieces], 1)
        wide_value = value.astype(f32)
        sums = jnp.sum(wide_value, 0, keepdims=True)
        squares = jnp.sum(wide_value * wide_value, 0, keepdims=True)
        found = jnp.dot(win[step, :, :t_dev], value, preferred_element_type=f32)
        if first_time:
            acc[0:sums_at, :width] = found
            acc[sums_at : sums_at + 1, :width] = sums
            acc[sums_at + 1 : sums_at + 2, :width] = squares
        else:
            acc[0:sums_at, :width] += found
            acc[sums_at : sums_at + 1, :width] += sums
            acc[sums_at + 1 : sums_at + 2, :width] += squares

    def split(piece, column):
        column = slice(column * 128, column * 128 + 128)
        for row in range(2):
            value = acc[sums_at + row : sums_at + row + 1, column]
            kept, given = halves(value, value, low_row)
            mine[piece, row : row + 1, :] = kept
            other[piece, row : row + 1, :] = given
        for k in range(half_k):
            at = k * ROWS
            kept, given = halves(
                acc[at : at + ROWS, column], acc[count + at : count + at + ROWS, column], low
            )
            mine[piece, EXTRA + at : EXTRA + at + ROWS, :] = kept
            other[piece, EXTRA + at : EXTRA + at + ROWS, :] = given
            if k % 2 == 1 or k == half_k - 1:
                swap_copy(piece, k // 2).start()

    def products(piece):
        own_copy(piece).wait()
        add([piece], 0, True)

        def body(turn, carry):
            step = turn
            raw_copy(piece, step).wait_recv()
            add([piece], step, False)
            return carry

        lax.fori_loop(1, g, body, 0)
        split(piece, 0)

    def joined(piece, k):
        at = EXTRA + k * ROWS
        if k % 2 == 0 and k > 0:
            swap_copy(piece, k // 2).wait_recv()
        return mine[piece, at : at + ROWS, :] + partner_in[piece, at : at + ROWS, :]

    def joined_row(piece, row):
        at = row
        return mine[piece, at : at + 1, :] + partner_in[piece, at : at + 1, :]

    def decoded(slot, k):
        coded = got[slot, k * ROWS : (k + 1) * ROWS, :].astype(jnp.int32).astype(f32)
        return coded * (got_extra[slot, 2 + k : 3 + k, :] * (1.0 / TOP))

    def send_sums(piece, outer_slot):
        swap_copy(piece, 0).wait_recv()
        sx, sq = joined_row(piece, 0), joined_row(piece, 1)
        tot, cols, days = own_tot, own_cols, group_days
        copies = sum_copies(piece, slot_of(piece))
        if outer_slot is not None:
            arriving = sum_copies(1, outer_slot)
            arriving[0].wait_recv()
            outer_x = got_extra[outer_slot, 0:1, :]
            outer_mean = outer_x / group_days
            sx, sq = sx + outer_x, sq + got_extra[outer_slot, 1:2, :]
            outer_tot = got_extra[outer_slot, EXTRA:, :]
            outer_cols = jnp.transpose(outer_tot)
            tot, cols, days = tot + outer_tot, cols + outer_cols, 2 * group_days
        sent_extra[piece, 0:1, :] = sx
        sent_extra[piece, 1:2, :] = sq
        local_mean = sx / days
        for k in range(half_k):
            value = joined(piece, k) - local_mean * pair_cols(cols, k)
            if outer_slot is not None:
                value = value + outer_mean * pair_cols(outer_cols, k)
            stage[k * ROWS : (k + 1) * ROWS, :] = value
            top = jnp.max(jnp.abs(value), 0, keepdims=True)
            if outer_slot is not None:
                top = top + got_extra[outer_slot, 2 + k : 3 + k, :]
            sent_extra[piece, 2 + k : 3 + k, :] = top
        sent_extra[piece, EXTRA:, :] = tot
        copies[0].start()
        for k in range(half_k):
            value = stage[k * ROWS : (k + 1) * ROWS, :]
            if outer_slot is not None:
                if k % 2 == 0:
                    arriving[1 + k // 2].wait_recv()
                value = value + decoded(outer_slot, k)
            scaled = value * (TOP / jnp.maximum(sent_extra[piece, 2 + k : 3 + k, :], 1e-30))
            sent[piece, k * ROWS : (k + 1) * ROWS, :] = (
                jnp.round(scaled).astype(jnp.int32).astype(jnp.int16)
            )
            if k % 2 == 1 or k == half_k - 1:
                copies[1 + k // 2].start()

    def send_outer(piece):
        @pl.when(jnp.logical_not(inner))
        def _():
            send_sums(piece, None)

    def send_inner(piece, outer_slot):
        @pl.when(inner)
        def _():
            send_sums(piece, outer_slot)

    last = groups - 1
    own_copy(0).wait()
    each(1, g, lambda s: raw_copy(0, s).wait_recv())

    def early_body(step, first_time):
        center_window(step)
        add([0], step, first_time)

    early_body(0, True)

    place = lax.broadcasted_iota(jnp.int32, (kcount, lanes), 1)

    def centered(value, valid):
        return jnp.where(valid, (value - mean).astype(jnp.bfloat16).astype(f32), 0.0)

    def center_body(at, carry):
        return carry + centered(idx_all[at], place < t_dev)

    core_sum = jnp.zeros((kcount, lanes), f32)
    if g <= 4:
        for at in range(g):
            core_sum = center_body(at, core_sum)
    else:
        core_sum = lax.fori_loop(0, g, center_body, core_sum)
    inner_block = centered(idx_all[jnp.where(core == 0, 0, g - 1)], place < t_dev)
    edge = jnp.concatenate([tiles[2 * g], tail[:, : lanes - 128]], 1)
    edge = jnp.where(core == 0, pltpu.roll(edge, t_dev - 128, 1), edge)
    opens = jnp.where(core == 0, t_dev - 64, 0)
    closes = jnp.where(core == 0, t_dev, 62)
    outer_block = centered(edge, (place >= opens) & (place < closes) & (edge < NEAR))

    def part(value, side):
        return jnp.dot(
            value.astype(jnp.bfloat16), chooser[side], preferred_element_type=f32
        )

    by_shift = (
        jnp.sum(core_sum, 1, keepdims=True)
        + part(outer_block, 0)
        - part(inner_block, 1)
    )
    tot_part[...] = jnp.zeros_like(tot_part)
    for k in range(kcount):
        tot_part[k : k + 1, :] = pltpu.roll(
            by_shift[k : k + 1], lax.rem(128 - offset_ref[k], 128), 1
        )

    if g <= 4:
        for step in range(1, g):
            early_body(step, False)
    else:
        each(1, g, lambda s: early_body(s, False))
    total_copy().start()
    split(0, 0)

    total_copy().wait()
    own_tot = tot_part[...] + tot_in[...]
    own_cols = jnp.transpose(own_tot)
    send_outer(0)
    products(1)
    send_sums(1, None)
    send_inner(0, 0)
    products(2)
    send_outer(2)
    send_inner(2, 1)
    products(last)
    near_blocks, far_blocks = sum_copies(1, 2), sum_copies(1, 3)

    def opened(slot, copies, days):
        copies[0].wait_recv()
        far_x = got_extra[slot, 0:1, :]
        cols = jnp.transpose(got_extra[slot, EXTRA:, :])
        return far_x, got_extra[slot, 1:2, :], far_x / days, cols

    near_x, near_sq, near_mean, near_cols = opened(2, near_blocks, group_days)
    for k in range(half_k):
        if k % 2 == 0:
            near_blocks[1 + k // 2].wait_recv()
        far[k * ROWS : (k + 1) * ROWS, :] = decoded(2, k) + near_mean * pair_cols(near_cols, k)
    swap_copy(last, 0).wait_recv()
    far_x, far_sq, far_mean, far_cols = opened(3, far_blocks, 2 * group_days)
    mean_x = (joined_row(last, 0) + near_x + far_x) / total_days
    var_x = (joined_row(last, 1) + near_sq + far_sq) / total_days - mean_x * mean_x
    all_cols = own_cols + near_cols + far_cols
    mask = small[0:1, :]
    mask = mask + pltpu.roll(mask, 64, 1)
    scaling = mask / (total_days * jnp.sqrt(var_x + 1e-06))
    for k in range(half_k):
        at = k * ROWS
        far[at : at + ROWS, :] += (
            joined(last, k)
            + far_mean * pair_cols(far_cols, k)
            - mean_x * pair_cols(all_cols, k)
        )

    def normal(k):
        if k % 2 == 0:
            far_blocks[1 + k // 2].wait_recv()
        value = far[k * ROWS : (k + 1) * ROWS, :] + decoded(3, k)
        scale = jnp.where(low_row, outer[k : k + 1], outer[k + half_k : k + half_k + 1])
        return value * (scaling * scale)

    small_int = lag_ref[...] + MAXLAG
    small[0:1, 0 : lag_ref.shape[1]] = small_int.astype(f32)
    chosen = jnp.broadcast_to(small[0:1, :].astype(jnp.int32), (64, 128))
    kept = lag_ref.shape[1]

    def out_copy(k):
        return pltpu.make_async_copy(out_buf.at[k], out_ref.at[k], out_sem.at[0])

    for k in range(0, half_k, 2):
        upper_rows = normal(k)
        under_rows = normal(k + 1) if k + 1 < half_k else upper_rows
        flat = jnp.transpose(jnp.concatenate([upper_rows, under_rows], 0))
        for side in range(2):
            rows = flat[side * 64 : (side + 1) * 64, :]
            for turn in range(min(2, half_k - k)):
                at = k + turn + side * half_k
                out_buf[at] = jnp.take_along_axis(rows, chosen + 64 * turn, axis=1)[:, :kept]
                out_copy(at).start()
    def drained(ref, sem):
        remote(ref, ref, sem, sem, partner).wait_send()

    drained(packs.at[pl.ds(0, g - 1)], idx_send.at[0])
    drained(tiles.at[pl.ds(0, 2 * g - 1)], tile_send.at[0])
    drained(zin.at[pl.ds(0, groups - 1)], z_send.at[0])
    for piece in range(groups):
        drained(recv.at[piece, pl.ds(0, g - 1)], raw_send.at[piece])
        drained(other.at[piece], swap_send.at[piece])
        if piece < last:
            drained(sent.at[piece], sum_send.at[0, piece])
            drained(sent_extra.at[piece], sum_send.at[1, piece])
    pltpu.make_async_copy(out_buf, out_ref, out_sem.at[0]).wait()


def shards(field, index, lag_list, index_offset, sea_mask):
    t_dev, cells_all = field.shape
    devices = lax.axis_size("tm")
    kcount = index.shape[1]
    lanes = round_up(t_dev, 128)
    groups = GROUPS
    g = devices // 2 // groups
    rows = kcount * ROWS
    half = rows // 2
    sizes = (devices, t_dev, kcount, groups, g)
    dma = pltpu.SemaphoreType.DMA
    f32 = jnp.float32
    maps = pl.pallas_call(
        functools.partial(kernel, sizes),
        out_shape=jax.ShapeDtypeStruct((kcount, 64, lag_list.shape[0]), f32),
        in_specs=[pl.BlockSpec(memory_space=pl.ANY)] * 5,
        out_specs=pl.BlockSpec(memory_space=pl.ANY),
        scratch_shapes=[
            pltpu.VMEM((kcount, t_dev), f32),
            pltpu.VMEM((1, lag_list.shape[0]), jnp.int32),
            pltpu.SMEM((kcount,), jnp.int32),
            pltpu.VMEM((1, sea_mask.shape[0]), jnp.int32),
            pltpu.VMEM((t_dev, cells_all), jnp.bfloat16),
            pltpu.VMEM((kcount, lanes), f32),
            pltpu.VMEM((8, lanes + 128), f32),
            pltpu.VMEM((g, 8, lanes + 128), f32),
            pltpu.VMEM((g, kcount, lanes), f32),
            pltpu.VMEM((2 * g + 1, kcount, 128), f32),
            pltpu.VMEM((kcount, 128), f32),
            pltpu.VMEM((groups, kcount, 128), f32),
            pltpu.VMEM((groups, g, t_dev, 128), jnp.bfloat16),
            pltpu.VMEM((g, kcount * BASE, lanes + 128), f32),
            pltpu.VMEM((g, rows, lanes), jnp.bfloat16),
            pltpu.VMEM((rows + EXTRA, 256), f32),
            pltpu.VMEM((groups, half + EXTRA, 128), f32),
            pltpu.VMEM((groups, half + EXTRA, 128), f32),
            pltpu.VMEM((groups, half + EXTRA, 128), f32),
            pltpu.VMEM((groups, half, 128), jnp.int16),
            pltpu.VMEM((groups, EXTRA + 16, 128), f32),
            pltpu.VMEM((groups, half, 128), jnp.int16),
            pltpu.VMEM((groups, EXTRA + 16, 128), f32),
            pltpu.VMEM((half, 128), f32),
            pltpu.VMEM((half, 128), f32),
            pltpu.VMEM((2, lanes, 128), jnp.bfloat16),
            pltpu.VMEM((kcount, 64, lag_list.shape[0]), f32),
            pltpu.VMEM((8, 128), f32),
            pltpu.VMEM((16, 128), f32),
            pltpu.VMEM((16, 128), f32),
            dma((groups,)),
            dma((groups, g - 1)),
            dma((1,)),
            dma((g - 1,)),
            dma((1,)),
            dma((2 * g - 1,)),
            dma((4,)),
            dma((1,)),
            dma((groups - 1,)),
            dma((groups,)),
            dma((groups, (kcount // 2 + 1) // 2)),
            dma((2, groups - 1)),
            dma(((kcount // 2 + 1) // 2 + 1, groups)),
            dma((groups + 1,)),
            pltpu.SemaphoreType.REGULAR((groups - 2,)),
            dma((1,)),
            dma((4,)),
        ],
        compiler_params=pltpu.CompilerParams(
            collective_id=0, has_side_effects=True, vmem_limit_bytes=60 * 1024 * 1024
        ),
    )(field, index.T, lag_list[None, :], index_offset, sea_mask[None, :])
    return jnp.transpose(maps, (1, 0, 2))


def solution(mesh):
    return jax.shard_map(
        shards,
        mesh=mesh,
        in_specs=(P("tm", None), P("tm", None), P(), P(), P("tm")),
        out_specs=P("tm", None, None),
        check_vma=False,
    )
```
